256 devices in a mesh: dp: 8 (over y, core), head: 2 (over z_lo), kv: 16 (over z_hi, x).
Axes of the slice: x: 4, y: 4, z: 8 (z_hi: 4, z_lo: 2; z = z_hi * 2 + z_lo), core: 2. Of those that a mesh axis runs over, the one named last changes fastest.
Arguments:
- teacher_query: bfloat16 [8, 4096, 3584], P('dp', 'kv', 'head'), may hold values from -96 to 96
- teacher_key: bfloat16 [8, 4096, 512], P('dp', 'kv', 'head'), may hold values from -8 to 8
- student_query: bfloat16 [8, 4096, 1792], P('dp', 'kv', 'head'), may hold values from -96 to 96
- student_key: bfloat16 [8, 4096, 256], P('dp', 'kv', 'head'), may hold values from -8 to 8
- pair_table: int32 [14, 2], replicated, may hold values from 0 to 27, as said below
Outputs:
- kl: float32 [8, 14, 4096], P('dp', 'head', 'kv')
- head_loss: float32 [14], P('head')
The draws below stay inside these ranges and needn't reach their ends.
Inputs may be any that keep to these rules, and one draw needn't show every extreme that they name: `pair_table`: each of the 28 teacher heads appears exactly once in the table.
All inputs are finite; a program needn't handle non-finite values.
Results may differ from the reference program's by a relative error of at most 0.0003.
Values may be sent and summed in bfloat16 or wider, within the bound.
No kernel may reach another device: no remote copies, remote signals or barrier semaphores. Data moves between devices by JAX's collectives and lax.ppermute only.
A program may use at most 64 MiB of HBM per device.

```python
import math
import jax
import jax.numpy as jnp
from jax import lax

HT = 28
KVT = 4
DH = 128
HS = 14
KVS = 2
L = 4096
SEQS = 8


def key_field(key, heads):
    shape = (SEQS, L, heads, DH)
    row_scale = jnp.exp(jax.random.uniform(jax.random.fold_in(key, 1), (SEQS, L, heads, 1), jnp.float32, math.log(0.5), math.log(2.0)))
    base = jnp.clip(jax.random.normal(key, shape, jnp.float32), -4.0, 4.0)
    return base * row_scale


def query_field(key, heads):
    shape = (SEQS, L, heads, DH)
    row_scale = jnp.exp(jax.random.uniform(jax.random.fold_in(key, 1), (SEQS, L, heads, 1), jnp.float32, math.log(0.3), math.log(3.0)))
    return jnp.clip(jax.random.normal(key, shape, jnp.float32), -5.0, 5.0) * row_scale


def draw_teacher_key(key, part):
    keys = key_field(jax.random.fold_in(key, 11), KVT)
    return keys.reshape(SEQS, L, KVT * DH).astype(jnp.bfloat16)


def draw_student_key(key, part):
    keys = key_field(jax.random.fold_in(key, 12), KVS)
    return keys.reshape(SEQS, L, KVS * DH).astype(jnp.bfloat16)


def draw_teacher_query(key, part):
    queries = query_field(jax.random.fold_in(key, 13), HT)
    return queries.reshape(SEQS, L, HT * DH).astype(jnp.bfloat16)


def draw_student_query(key, part):
    queries = query_field(jax.random.fold_in(key, 14), HS)
    return queries.reshape(SEQS, L, HS * DH).astype(jnp.bfloat16)


def draw_pair_table(key, part):
    order = jax.random.permutation(jax.random.fold_in(key, 15), HT)
    return order.astype(jnp.int32).reshape(HS, 2)


def setup_inputs(seed: int = 0) -> dict:
    streams_of = jax.random.split(jax.random.key(seed), 6)
    teacher_query = draw_teacher_query(jax.random.fold_in(streams_of[5], 71), 0)
    teacher_key = draw_teacher_key(jax.random.fold_in(streams_of[5], 71), 0)
    student_query = draw_student_query(jax.random.fold_in(streams_of[5], 71), 0)
    student_key = draw_student_key(jax.random.fold_in(streams_of[5], 71), 0)
    pair_table = draw_pair_table(jax.random.fold_in(streams_of[5], 71), 0)
    return dict(teacher_query=teacher_query, teacher_key=teacher_key, student_query=student_query, student_key=student_key, pair_table=pair_table)


masked_value = -1e+30

def masked_logits(query_rows, key_rows, causal_mask):
    scale = 1.0 / math.sqrt(DH)
    product = jnp.dot(query_rows.astype(jnp.float32), key_rows.astype(jnp.float32).T, precision=lax.Precision.HIGHEST, preferred_element_type=jnp.float32) * scale
    return jnp.where(causal_mask, product, masked_value)

def log_total(logits, causal_mask):
    row_max = lax.optimization_barrier(jnp.max(logits, axis=-1))
    weights = jnp.where(causal_mask, jnp.exp(logits - row_max[:, None]), 0.0)
    return row_max + jnp.log(lax.optimization_barrier(jnp.sum(weights, axis=-1)))

def reference(teacher_query, teacher_key, student_query, student_key, pair_table):
    teacher_q = teacher_query.reshape(SEQS, L, HT, DH)
    teacher_k = teacher_key.reshape(SEQS, L, KVT, DH)
    student_q = student_query.reshape(SEQS, L, HS, DH)
    student_k = student_key.reshape(SEQS, L, KVS, DH)
    group_teacher = HT // KVT
    group_student = HS // KVS
    positions = jnp.arange(L, dtype=jnp.int32)
    causal_mask = positions[None, :] <= positions[:, None]

    def one_item(flat_index):
        sequence = flat_index // HS
        student = flat_index % HS
        s_logits = masked_logits(student_q[sequence, :, student], student_k[sequence, :, student // group_student], causal_mask)
        s_lse = log_total(s_logits, causal_mask)
        total = jnp.zeros((L,), jnp.float32)
        for column in range(2):
            teacher = pair_table[student, column]
            t_logits = masked_logits(teacher_q[sequence, :, teacher], teacher_k[sequence, :, teacher // group_teacher], causal_mask)
            t_lse = log_total(t_logits, causal_mask)
            probs = jnp.where(causal_mask, jnp.exp(t_logits - t_lse[:, None]), 0.0)
            total = total + (lax.optimization_barrier(jnp.sum(probs * (t_logits - s_logits), axis=-1)) - t_lse + s_lse)
        return total
    kl = lax.map(one_item, jnp.arange(SEQS * HS, dtype=jnp.int32)).reshape(SEQS, HS, L)
    head_loss = lax.optimization_barrier(jnp.sum(kl, axis=(0, 2))) / (SEQS * L)
    return (kl, head_loss)
```

```python
import functools
import math

import jax
import jax.numpy as jnp
from jax import lax
from jax.experimental import pallas as pl
from jax.experimental.pallas import tpu as pltpu
from jax.sharding import Mesh
from jax.sharding import PartitionSpec as P

HT = 28
KVT = 4
DH = 128
HS = 14
KVS = 2
ROWS = 256
PAIRS = 14
STUDENTS = 7
HEADS = PAIRS + STUDENTS
KV = ("kv_0", "kv_1")
DP = ("dp_0", "dp_1")
LANE = 128
SUB = 8
MASKED = -1e30
LN2 = math.log(2.0)
KAPPA = 1.0 / (LN2 * math.sqrt(DH))


def prepare_kernel(sel, own, other, student, out):
    def put(slot, q):
        q = q.astype(jnp.float32) * KAPPA
        high = q.astype(jnp.bfloat16)
        low = (q - high.astype(jnp.float32)).astype(jnp.bfloat16)
        out[slot, :DH, :] = jnp.transpose(high.astype(jnp.float32)).astype(jnp.bfloat16)
        out[slot, DH:, :] = jnp.transpose(low.astype(jnp.float32)).astype(jnp.bfloat16)

    for s in range(STUDENTS):
        put(PAIRS + s, student[:, s * DH : (s + 1) * DH])
    for p in range(PAIRS):
        lanes = pl.ds(pl.multiple_of(sel[1, p] * DH, DH), DH)

        @pl.when(sel[0, p] == 0)
        def _():
            put(p, own[:, lanes])

        @pl.when(sel[0, p] != 0)
        def _():
            put(p, other[:, lanes])


def prepare(sel, own, other, student):
    vmem = pl.BlockSpec(memory_space=pltpu.VMEM)
    return pl.pallas_call(
        prepare_kernel,
        out_shape=jax.ShapeDtypeStruct((HEADS, 2 * DH, ROWS), jnp.bfloat16),
        in_specs=[pl.BlockSpec(memory_space=pltpu.SMEM), vmem, vmem, vmem],
        out_specs=vmem,
        name="prepare",
    )(sel, own, other, student)


def attend_kernel(n_groups, sizes, info, qt, *refs):
    groups = refs[:n_groups]
    out = refs[n_groups]
    keys, tm, tl, tc, sm, sl, sems = refs[n_groups + 1 :]
    copies = []
    at = 0
    for g in range(n_groups):
        copies.append(
            pltpu.make_async_copy(groups[g], keys.at[pl.ds(at, sizes[g])], sems.at[g])
        )
        at += sizes[g]
    for c in copies:
        c.start()
    for ref in (tm, sm):
        ref[...] = jnp.full_like(ref, MASKED)
    for ref in (tl, tc, sl):
        ref[...] = jnp.zeros_like(ref)
    for c in copies:
        c.wait()
    row_block = info[0, 0]

    def update(logits, mask, m_ref, l_ref, index):
        if mask is not None:
            logits = jnp.where(mask, logits, MASKED)
        folded = logits.reshape(ROWS // SUB, SUB, ROWS)
        old = m_ref[index]
        new = jnp.maximum(old, jnp.max(folded, axis=0))
        weights = jnp.exp2(folded - new[None])
        rescale = jnp.exp2(old - new)
        m_ref[index] = new
        l_ref[index] = l_ref[index] * rescale + jnp.sum(weights, axis=0)
        return weights, rescale

    def block(own_slot, other_slot, masked):
        mask = None
        if masked:
            key_pos = lax.broadcasted_iota(jnp.int32, (ROWS, ROWS), 0)
            row_pos = lax.broadcasted_iota(jnp.int32, (ROWS, ROWS), 1)
            mask = key_pos <= row_pos
        student_keys = keys[own_slot, :, 2 * DH :]
        student_keys = jnp.concatenate([student_keys, student_keys], axis=1)
        for s in range(STUDENTS):
            zs = jnp.dot(student_keys, qt[PAIRS + s], preferred_element_type=jnp.float32)
            update(zs, mask, sm, sl, s)
            for c in range(2):
                p = 2 * s + c
                slot = jnp.where(info[1, p] == 0, own_slot, other_slot)
                lanes = pl.ds(pl.multiple_of(info[2, p] * DH, DH), DH)
                teacher_keys = keys[slot, :, lanes]
                teacher_keys = jnp.concatenate([teacher_keys, teacher_keys], axis=1)
                zt = jnp.dot(teacher_keys, qt[p], preferred_element_type=jnp.float32)
                weights, rescale = update(zt, mask, tm, tl, p)
                gap = (zt - zs).reshape(ROWS // SUB, SUB, ROWS)
                tc[p] = tc[p] * rescale + jnp.sum(weights * gap, axis=0)

    def step(i, carry):
        position = info[3, i]
        own_slot = info[4, i]
        other_slot = info[5, i]

        @pl.when(position < row_block)
        def _():
            block(own_slot, other_slot, False)

        @pl.when(position == row_block)
        def _():
            block(own_slot, other_slot, True)

        return carry

    lax.fori_loop(0, 16, step, 0)

    def merged(m8, l8):
        top = jnp.max(m8, axis=0, keepdims=True)
        factor = jnp.exp2(m8 - top)
        total = jnp.sum(l8 * factor, axis=0, keepdims=True)
        return factor, total, LN2 * top + jnp.log(total)

    for s in range(STUDENTS):
        _, _, s_lse = merged(sm[s], sl[s])
        value = 2.0 * s_lse
        for c in range(2):
            p = 2 * s + c
            factor, total, t_lse = merged(tm[p], tl[p])
            cross = jnp.sum(tc[p] * factor, axis=0, keepdims=True)
            value = value + (LN2 * cross / total - t_lse)
        out[s : s + 1, :] = value


def attend(info, qt, groups):
    sizes = tuple(g.shape[0] for g in groups)
    state = lambda n: pltpu.VMEM((n, SUB, ROWS), jnp.float32)
    return pl.pallas_call(
        functools.partial(attend_kernel, len(groups), sizes),
        out_shape=jax.ShapeDtypeStruct((STUDENTS, ROWS), jnp.float32),
        in_specs=[pl.BlockSpec(memory_space=pltpu.SMEM), pl.BlockSpec(memory_space=pltpu.VMEM)]
        + [pl.BlockSpec(memory_space=pl.ANY)] * len(groups),
        out_specs=pl.BlockSpec(memory_space=pltpu.VMEM),
        scratch_shapes=[
            pltpu.VMEM((sum(sizes), ROWS, 3 * DH), jnp.bfloat16),
            state(PAIRS),
            state(PAIRS),
            state(PAIRS),
            state(STUDENTS),
            state(STUDENTS),
            pltpu.SemaphoreType.DMA((len(groups),)),
        ],
        compiler_params=pltpu.CompilerParams(vmem_limit_bytes=40 * 1024 * 1024),
        name="attend",
    )(info, qt, *groups)


def shift(n, by):
    return [(i, (i + by) % n) for i in range(n)]


def z_place(ring):
    ring %= 8
    return (ring % 2) * 4 + ring // 2


def z_shift(by):
    return [(z_place(i), z_place(i + by)) for i in range(8)]


def per_device(teacher_query, teacher_key, student_query, student_key, pair_table):
    head = lax.axis_index("head")
    z_hi = lax.axis_index("kv_0")
    x = lax.axis_index("kv_1")
    other_query = lax.ppermute(teacher_query, "head", [(0, 1), (1, 0)])
    own_keys = jnp.concatenate([teacher_key, student_key], axis=2)

    ring = {0: own_keys}
    up = down = own_keys
    for step in range(1, 5):
        up = lax.ppermute(up, ("head", "kv_0"), z_shift(1))
        ring[step] = up
        if step < 4:
            down = lax.ppermute(down, ("head", "kv_0"), z_shift(-1))
            ring[8 - step] = down
    column = jnp.concatenate([ring[o] for o in range(8)], axis=0)
    left = lax.ppermute(column, "kv_1", shift(4, 1))
    right = lax.ppermute(column, "kv_1", shift(4, -1))
    far_a = lax.ppermute(left[:4], "kv_1", shift(4, 1))
    far_b = lax.ppermute(right[4:], "kv_1", shift(4, -1))
    groups = [column, left, right, far_a, far_b]

    my_pairs = lax.dynamic_slice_in_dim(pair_table, head * STUDENTS, STUDENTS, 0).reshape(-1)
    sel = jnp.stack([(my_pairs // PAIRS != head).astype(jnp.int32), my_pairs % PAIRS])
    kv_head = my_pairs // (HT // KVT)
    pad = jnp.zeros((2,), jnp.int32)
    xs = jnp.repeat(jnp.arange(4, dtype=jnp.int32), 4)
    m = jnp.tile(jnp.arange(4, dtype=jnp.int32), 4)
    x_of = jnp.mod(x + jnp.array([0, -1, 1, 2], jnp.int32)[xs], 4)
    position = jnp.mod(z_hi - m, 4) * 4 + x_of
    own_slot = xs * 8 + 2 * m
    other_slot = xs * 8 + jnp.mod(2 * m - 1 + 2 * head, 8)
    info = jnp.stack(
        [
            jnp.full((16,), z_hi * 4 + x, jnp.int32),
            jnp.concatenate([(kv_head // 2 != head).astype(jnp.int32), pad]),
            jnp.concatenate([kv_head % 2, pad]),
            position,
            own_slot,
            other_slot,
        ]
    )
    qt = prepare(sel, teacher_query[0], other_query[0], student_query[0])
    kl = attend(info, qt, groups)

    sums = jnp.pad(jnp.sum(kl, axis=1), (0, LANE - STUDENTS))
    everyone = ("dp_0", "dp_1", "kv_0", "kv_1")
    count = lax.axis_size(everyone)
    terms = lax.all_to_all(
        jnp.broadcast_to(sums, (count, LANE)), everyone, 0, 0, tiled=True
    )
    head_loss = jnp.sum(terms, axis=0)[:STUDENTS] / (count * ROWS)
    return (kl[None], head_loss)


def solution(mesh):
    split = Mesh(
        mesh.devices.reshape(4, 2, mesh.shape["head"], 4, 4),
        ("dp_0", "dp_1", "head", "kv_0", "kv_1"),
    )
    in_specs = (P(DP, KV, "head"), P(DP, KV, "head"), P(DP, KV, "head"), P(DP, KV, "head"), P())
    out_specs = (P(DP, "head", KV), P("head"))
    return jax.shard_map(
        per_device, mesh=split, in_specs=in_specs, out_specs=out_specs, check_vma=False
    )
```

```python
import functools
import math

import jax
import jax.numpy as jnp
from jax import lax
from jax.experimental import pallas as pl
from jax.experimental.pallas import tpu as pltpu
from jax.sharding import Mesh
from jax.sharding import PartitionSpec as P

HT = 28
KVT = 4
DH = 128
HS = 14
KVS = 2
ROWS = 256
PAIRS = 14
STUDENTS = 7
HEADS = PAIRS + STUDENTS
KV = ("kv_0", "kv_1")
DP = ("dp_0", "dp_1")
LANE = 128
SUB = 8
MASKED = -1e30
LN2 = math.log(2.0)
KAPPA = 1.0 / (LN2 * math.sqrt(DH))


def prepare_kernel(sel, own, other, student, out):
    def put(slot, q):
        q = q.astype(jnp.float32) * KAPPA
        high = q.astype(jnp.bfloat16)
        low = (q - high.astype(jnp.float32)).astype(jnp.bfloat16)
        out[slot, :DH, :] = jnp.transpose(high.astype(jnp.float32)).astype(jnp.bfloat16)
        out[slot, DH:, :] = jnp.transpose(low.astype(jnp.float32)).astype(jnp.bfloat16)

    for s in range(STUDENTS):
        put(PAIRS + s, student[:, s * DH : (s + 1) * DH])
    for p in range(PAIRS):
        lanes = pl.ds(pl.multiple_of(sel[1, p] * DH, DH), DH)

        @pl.when(sel[0, p] == 0)
        def _():
            put(p, own[:, lanes])

        @pl.when(sel[0, p] != 0)
        def _():
            put(p, other[:, lanes])


def prepare(sel, own, other, student):
    vmem = pl.BlockSpec(memory_space=pltpu.VMEM)
    return pl.pallas_call(
        prepare_kernel,
        out_shape=jax.ShapeDtypeStruct((HEADS, 2 * DH, ROWS), jnp.bfloat16),
        in_specs=[pl.BlockSpec(memory_space=pltpu.SMEM), vmem, vmem, vmem],
        out_specs=vmem,
        name="prepare",
    )(sel, own, other, student)


STATE = 3 * PAIRS + 2 * STUDENTS
TL, TC, SM, SL = PAIRS, 2 * PAIRS, 3 * PAIRS, 3 * PAIRS + STUDENTS
HALF = ROWS // 2
PIECES = 5


def attend_kernel(first, last, info, qt, *refs):
    parts = refs[: 2 * PIECES]
    refs = refs[2 * PIECES :]
    if not first:
        before, *refs = refs
    out, keys, *refs = refs
    if last:
        state, sems = refs
    else:
        state = out
        (sems,) = refs
    row_block = info[0, 0]
    needed = info[0, 1] != 0

    def copies():
        for side in range(2):
            for n in range(PIECES):
                slot = min(n, 3)
                rows = pl.ds(0, ROWS) if n < 3 else pl.ds((n - 3) * HALF, HALF)
                yield pltpu.make_async_copy(
                    parts[side * PIECES + n], keys.at[side, slot, rows], sems.at[side, n]
                )

    @pl.when(needed)
    def _():
        for c in copies():
            c.start()

    if first:
        for part, value in ((0, MASKED), (TL, 0.0), (TC, 0.0)):
            state[part : part + PAIRS] = jnp.full((PAIRS, SUB, ROWS), value, jnp.float32)
        for part, value in ((SM, MASKED), (SL, 0.0)):
            state[part : part + STUDENTS] = jnp.full((STUDENTS, SUB, ROWS), value, jnp.float32)
    else:
        state[...] = before[...]

    def update(logits, mask, m_index, l_index):
        if mask is not None:
            logits = jnp.where(mask, logits, MASKED)
        folded = logits.reshape(ROWS // SUB, SUB, ROWS)
        old = state[m_index]
        new = jnp.maximum(old, jnp.max(folded, axis=0))
        weights = jnp.exp2(folded - new[None])
        rescale = jnp.exp2(old - new)
        state[m_index] = new
        state[l_index] = state[l_index] * rescale + jnp.sum(weights, axis=0)
        return weights, rescale

    def block(slot, masked):
        mask = None
        if masked:
            key_pos = lax.broadcasted_iota(jnp.int32, (ROWS, ROWS), 0)
            row_pos = lax.broadcasted_iota(jnp.int32, (ROWS, ROWS), 1)
            mask = key_pos <= row_pos
        student_keys = keys[0, slot, :, 2 * DH :]
        student_keys = jnp.concatenate([student_keys, student_keys], axis=1)
        for s in range(STUDENTS):
            zs = jnp.dot(student_keys, qt[PAIRS + s], preferred_element_type=jnp.float32)
            update(zs, mask, SM + s, SL + s)
            for c in range(2):
                p = 2 * s + c
                lanes = pl.ds(pl.multiple_of(info[2, p] * DH, DH), DH)
                teacher_keys = keys[info[1, p], slot, :, lanes]
                teacher_keys = jnp.concatenate([teacher_keys, teacher_keys], axis=1)
                zt = jnp.dot(teacher_keys, qt[p], preferred_element_type=jnp.float32)
                weights, rescale = update(zt, mask, p, TL + p)
                gap = (zt - zs).reshape(ROWS // SUB, SUB, ROWS)
                state[TC + p] = state[TC + p] * rescale + jnp.sum(weights * gap, axis=0)

    def step(slot, carry):
        position = info[3, slot]

        @pl.when(position < row_block)
        def _():
            block(slot, False)

        if first:

            @pl.when(position == row_block)
            def _():
                block(slot, True)

        return carry

    @pl.when(needed)
    def _():
        for c in copies():
            c.wait()
        lax.fori_loop(0, 4, step, 0)

    if not last:
        return

    def merged(m8, l8):
        top = jnp.max(m8, axis=0, keepdims=True)
        factor = jnp.exp2(m8 - top)
        total = jnp.sum(l8 * factor, axis=0, keepdims=True)
        return factor, total, LN2 * top + jnp.log(total)

    for s in range(STUDENTS):
        _, _, s_lse = merged(state[SM + s], state[SL + s])
        value = 2.0 * s_lse
        for c in range(2):
            p = 2 * s + c
            factor, total, t_lse = merged(state[p], state[TL + p])
            cross = jnp.sum(state[TC + p] * factor, axis=0, keepdims=True)
            value = value + (LN2 * cross / total - t_lse)
        out[s : s + 1, :] = value


def attend(info, qt, parts, state, last):
    first = state is None
    vmem = pl.BlockSpec(memory_space=pltpu.VMEM)
    operands = [info, qt, *parts] + ([] if first else [state])
    state_shape = (STATE, SUB, ROWS)
    scratch = [pltpu.VMEM((2, 4, ROWS, 3 * DH), jnp.bfloat16)]
    if last:
        scratch.append(pltpu.VMEM(state_shape, jnp.float32))
    scratch.append(pltpu.SemaphoreType.DMA((2, PIECES)))
    return pl.pallas_call(
        functools.partial(attend_kernel, first, last),
        out_shape=jax.ShapeDtypeStruct((STUDENTS, ROWS) if last else state_shape, jnp.float32),
        in_specs=[pl.BlockSpec(memory_space=pltpu.SMEM), vmem]
        + [pl.BlockSpec(memory_space=pl.ANY)] * len(parts)
        + ([] if first else [vmem]),
        out_specs=vmem,
        scratch_shapes=scratch,
        compiler_params=pltpu.CompilerParams(vmem_limit_bytes=24 * 1024 * 1024),
        cost_estimate=pl.CostEstimate(
            flops=4 * HEADS * 2 * ROWS * ROWS * 2 * DH,
            bytes_accessed=8 * ROWS * 3 * DH * 2,
            transcendentals=4 * HEADS * ROWS * ROWS,
        ),
        name="attend",
    )(*operands)


CORE = "dp_1"


def per_device(teacher_query, teacher_key, student_query, student_key, pair_table):
    core = lax.axis_index(CORE)
    head = lax.axis_index("head")
    z_hi = lax.axis_index("kv_0")
    x = lax.axis_index("kv_1")
    stays = core == head

    def swap(a):
        return lax.ppermute(a, (CORE, "head"), [(1, 2), (2, 1)])

    def swapped(a):
        return jnp.where(stays, a, swap(a))

    def across(a, chunks):
        pairs = [(c * 4 + z, (1 - c) * 4 + z) for c in range(2) for z in chunks]
        return lax.ppermute(a, (CORE, "kv_0"), pairs)

    def along_x(a, by, chunks):
        pairs = [(z * 4 + i, z * 4 + (i + by) % 4) for z in chunks for i in range(4)]
        return lax.ppermute(a, KV, pairs)

    def along_z(a, pairs):
        return lax.ppermute(a, "kv_0", pairs)

    def gathered(a, chunks):
        left = along_x(a, 1, chunks)
        right = along_x(a, -1, chunks)
        far_a = along_x(left[:HALF], 1, chunks)
        far_b = along_x(right[HALF:], -1, chunks)
        mine = [a, left, right, far_a, far_b]
        return mine + [across(m, chunks) for m in mine]

    keys = swapped(jnp.concatenate([teacher_key[0], student_key[0]], axis=1))
    student = swapped(student_query[0])
    own = swapped(teacher_query[0])
    other = across(own, range(4))

    one_back = along_z(keys, [(0, 1), (1, 2), (2, 3)])
    wrapped = along_z(keys, [(0, 3)])
    two_back = along_z(one_back, [(1, 2), (2, 3)])

    side = core
    my_pairs = lax.dynamic_slice_in_dim(pair_table, side * STUDENTS, STUDENTS, 0).reshape(-1)
    sel = jnp.stack([(my_pairs // PAIRS != side).astype(jnp.int32), my_pairs % PAIRS])
    kv_head = my_pairs // (HT // KVT)
    pad = jnp.zeros((2,), jnp.int32)
    x_of = jnp.mod(x + jnp.array([0, -1, 1, 2], jnp.int32), 4)

    def info(chunk, needed):
        return jnp.stack(
            [
                jnp.pad(jnp.stack([z_hi * 4 + x, needed.astype(jnp.int32)]), (0, 14)),
                jnp.concatenate([(kv_head // 2 != side).astype(jnp.int32), pad]),
                jnp.concatenate([kv_head % 2, pad]),
                jnp.pad(chunk * 4 + x_of, (0, 12)),
            ]
        )

    qt = prepare(sel, own, other, student)
    state = attend(info(z_hi, z_hi >= 0), qt, gathered(keys, range(4)), None, False)
    state = attend(info(z_hi - 1, z_hi >= 1), qt, gathered(one_back, (1, 2, 3)), state, False)
    state = attend(info(z_hi - 3, z_hi == 3), qt, gathered(wrapped, (3,)), state, False)
    kl = attend(info(z_hi - 2, z_hi >= 2), qt, gathered(two_back, (2, 3)), state, True)
    kl = swapped(kl)

    sums = jnp.pad(jnp.sum(kl, axis=1), (0, LANE - STUDENTS))
    everyone = ("dp_0", "dp_1", "kv_0", "kv_1")
    count = lax.axis_size(everyone)
    terms = lax.all_to_all(
        jnp.broadcast_to(sums, (count, LANE)), everyone, 0, 0, tiled=True
    )
    head_loss = jnp.sum(terms, axis=0)[:STUDENTS] / (count * ROWS)
    return (kl[None], head_loss)


def solution(mesh):
    split = Mesh(
        mesh.devices.reshape(4, 2, mesh.shape["head"], 4, 4),
        ("dp_0", "dp_1", "head", "kv_0", "kv_1"),
    )
    in_specs = (P(DP, KV, "head"), P(DP, KV, "head"), P(DP, KV, "head"), P(DP, KV, "head"), P())
    out_specs = (P(DP, "head", KV), P("head"))
    return jax.shard_map(
        per_device, mesh=split, in_specs=in_specs, out_specs=out_specs, check_vma=False
    )
```

```python
import functools
import math

import jax
import jax.numpy as jnp
from jax import lax
from jax.experimental import pallas as pl
from jax.experimental.pallas import tpu as pltpu
from jax.sharding import Mesh
from jax.sharding import PartitionSpec as P

HT = 28
KVT = 4
DH = 128
HS = 14
KVS = 2
ROWS = 256
PAIRS = 14
STUDENTS = 7
HEADS = PAIRS + STUDENTS
KV = ("kv_0", "kv_1")
DP = ("dp_0", "dp_1")
LANE = 128
SUB = 8
MASKED = -1e30
LN2 = math.log(2.0)
KAPPA = 1.0 / (LN2 * math.sqrt(DH))


def prepare_kernel(sel, own, other, student, out):
    def put(slot, q):
        q = q.astype(jnp.float32) * KAPPA
        high = q.astype(jnp.bfloat16)
        low = (q - high.astype(jnp.float32)).astype(jnp.bfloat16)
        out[slot, :DH, :] = jnp.transpose(high.astype(jnp.float32)).astype(jnp.bfloat16)
        out[slot, DH:, :] = jnp.transpose(low.astype(jnp.float32)).astype(jnp.bfloat16)

    for s in range(STUDENTS):
        put(PAIRS + s, student[:, s * DH : (s + 1) * DH])
    for p in range(PAIRS):
        lanes = pl.ds(pl.multiple_of(sel[1, p] * DH, DH), DH)

        @pl.when(sel[0, p] == 0)
        def _():
            put(p, own[:, lanes])

        @pl.when(sel[0, p] != 0)
        def _():
            put(p, other[:, lanes])


def prepare(sel, own, other, student):
    vmem = pl.BlockSpec(memory_space=pltpu.VMEM)
    return pl.pallas_call(
        prepare_kernel,
        out_shape=jax.ShapeDtypeStruct((HEADS, 2 * DH, ROWS), jnp.bfloat16),
        in_specs=[pl.BlockSpec(memory_space=pltpu.SMEM), vmem, vmem, vmem],
        out_specs=vmem,
        name="prepare",
    )(sel, own, other, student)


STATE = 3 * PAIRS + 2 * STUDENTS
TL, TC, SM, SL = PAIRS, 2 * PAIRS, 3 * PAIRS, 3 * PAIRS + STUDENTS
OWN = 3
COLUMN = 4 * OWN + 4 * 2


def split_kernel(teacher, student, out):
    out[0] = teacher[:, :DH]
    out[1] = teacher[:, DH:]
    out[2] = student[...]


def split_heads(teacher, student):
    return pl.pallas_call(
        split_kernel,
        out_shape=jax.ShapeDtypeStruct((OWN, ROWS, DH), jnp.bfloat16),
        in_specs=[pl.BlockSpec(memory_space=pltpu.VMEM)] * 2,
        out_specs=pl.BlockSpec(memory_space=pltpu.VMEM),
        name="split_heads",
    )(teacher, student)


def column_kernel(side, *refs):
    ring, out, sems = refs[:8], refs[8], refs[9]

    def move(head):
        copies = []
        for m in range(4):
            own = ring[2 * m]
            other = ring[(2 * m - 1 + 2 * head) % 8]
            copies.append(
                pltpu.make_async_copy(own, out.at[pl.ds(OWN * m, OWN)], sems.at[m])
            )
            copies.append(
                pltpu.make_async_copy(
                    other.at[pl.ds(0, 2)], out.at[pl.ds(4 * OWN + 2 * m, 2)], sems.at[4 + m]
                )
            )
        for c in copies:
            c.start()
        for c in copies:
            c.wait()

    for head in range(2):

        @pl.when(side[0, 0] == head)
        def _():
            move(head)


def column_of(side, ring):
    return pl.pallas_call(
        column_kernel,
        out_shape=jax.ShapeDtypeStruct((COLUMN, ROWS, DH), jnp.bfloat16),
        in_specs=[pl.BlockSpec(memory_space=pltpu.SMEM)]
        + [pl.BlockSpec(memory_space=pl.ANY)] * 8,
        out_specs=pl.BlockSpec(memory_space=pltpu.VMEM),
        scratch_shapes=[pltpu.SemaphoreType.DMA((8,))],
        name="column",
    )(side, *ring)


def attend_kernel(first, last, counts, info, qt, *refs):
    groups = refs[: len(counts)]
    refs = refs[len(counts) :]
    if not first:
        before, *refs = refs
    out, keys, *refs = refs
    if last:
        state, sems = refs
    else:
        state = out
        (sems,) = refs
    row_block = info[0, 0]
    copies = []
    at = 0
    for g, n in enumerate(counts):
        copies.append(pltpu.make_async_copy(groups[g], keys.at[pl.ds(at, n)], sems.at[g]))
        at += n
    columns = at // COLUMN
    for c in copies:
        c.start()

    if first:
        for part, value in ((0, MASKED), (TL, 0.0), (TC, 0.0)):
            state[part : part + PAIRS] = jnp.full((PAIRS, SUB, ROWS), value, jnp.float32)
        for part, value in ((SM, MASKED), (SL, 0.0)):
            state[part : part + STUDENTS] = jnp.full((STUDENTS, SUB, ROWS), value, jnp.float32)
    else:
        state[...] = before[...]
    for c in copies:
        c.wait()

    def update(logits, mask, m_index, l_index):
        if mask is not None:
            logits = jnp.where(mask, logits, MASKED)
        folded = logits.reshape(ROWS // SUB, SUB, ROWS)
        old = state[m_index]
        new = jnp.maximum(old, jnp.max(folded, axis=0))
        weights = jnp.exp2(folded - new[None])
        rescale = jnp.exp2(old - new)
        state[m_index] = new
        state[l_index] = state[l_index] * rescale + jnp.sum(weights, axis=0)
        return weights, rescale

    def block(base, m, masked):
        mask = None
        if masked:
            key_pos = lax.broadcasted_iota(jnp.int32, (ROWS, ROWS), 0)
            row_pos = lax.broadcasted_iota(jnp.int32, (ROWS, ROWS), 1)
            mask = key_pos <= row_pos
        student_keys = keys[base + OWN * m + 2]
        student_keys = jnp.concatenate([student_keys, student_keys], axis=1)
        for s in range(STUDENTS):
            zs = jnp.dot(student_keys, qt[PAIRS + s], preferred_element_type=jnp.float32)
            update(zs, mask, SM + s, SL + s)
            for c in range(2):
                p = 2 * s + c
                teacher_keys = keys[base + info[1, p] + info[2, p] * m]
                teacher_keys = jnp.concatenate([teacher_keys, teacher_keys], axis=1)
                zt = jnp.dot(teacher_keys, qt[p], preferred_element_type=jnp.float32)
                weights, rescale = update(zt, mask, p, TL + p)
                gap = (zt - zs).reshape(ROWS // SUB, SUB, ROWS)
                state[TC + p] = state[TC + p] * rescale + jnp.sum(weights * gap, axis=0)

    def step(i, carry):
        position = info[3, i]
        base = (i // 4) * COLUMN
        m = lax.rem(i, 4)

        @pl.when(position < row_block)
        def _():
            block(base, m, False)

        if first:

            @pl.when(position == row_block)
            def _():
                block(base, m, True)

        return carry

    lax.fori_loop(0, 4 * columns, step, 0)

    if not last:
        return

    def merged(m8, l8):
        top = jnp.max(m8, axis=0, keepdims=True)
        factor = jnp.exp2(m8 - top)
        total = jnp.sum(l8 * factor, axis=0, keepdims=True)
        return factor, total, LN2 * top + jnp.log(total)

    for s in range(STUDENTS):
        _, _, s_lse = merged(state[SM + s], state[SL + s])
        value = 2.0 * s_lse
        for c in range(2):
            p = 2 * s + c
            factor, total, t_lse = merged(state[p], state[TL + p])
            cross = jnp.sum(state[TC + p] * factor, axis=0, keepdims=True)
            value = value + (LN2 * cross / total - t_lse)
        out[s : s + 1, :] = value


def attend(info, qt, groups, state, last):
    first = state is None
    vmem = pl.BlockSpec(memory_space=pltpu.VMEM)
    operands = [info, qt, *groups] + ([] if first else [state])
    state_shape = (STATE, SUB, ROWS)
    counts = tuple(g.shape[0] for g in groups)
    blocks = 4 * sum(counts) // COLUMN
    scratch = [pltpu.VMEM((sum(counts), ROWS, DH), jnp.bfloat16)]
    if last:
        scratch.append(pltpu.VMEM(state_shape, jnp.float32))
    scratch.append(pltpu.SemaphoreType.DMA((len(groups),)))
    return pl.pallas_call(
        functools.partial(attend_kernel, first, last, counts),
        out_shape=jax.ShapeDtypeStruct((STUDENTS, ROWS) if last else state_shape, jnp.float32),
        in_specs=[pl.BlockSpec(memory_space=pltpu.SMEM), vmem]
        + [pl.BlockSpec(memory_space=pl.ANY)] * len(groups)
        + ([] if first else [vmem]),
        out_specs=vmem,
        scratch_shapes=scratch,
        compiler_params=pltpu.CompilerParams(vmem_limit_bytes=24 * 1024 * 1024),
        cost_estimate=pl.CostEstimate(
            flops=blocks * HEADS * 2 * ROWS * ROWS * 2 * DH,
            bytes_accessed=blocks * ROWS * 5 * DH * 2,
            transcendentals=blocks * HEADS * ROWS * ROWS,
        ),
        name="attend",
    )(*operands)


def shift(n, by):
    return [(i, (i + by) % n) for i in range(n)]


def z_place(ring):
    ring %= 8
    return (ring % 2) * 4 + ring // 2


def z_shift(by):
    return [(z_place(i), z_place(i + by)) for i in range(8)]


def per_device(teacher_query, teacher_key, student_query, student_key, pair_table):
    head = lax.axis_index("head")
    z_hi = lax.axis_index("kv_0")
    x = lax.axis_index("kv_1")

    own_keys = split_heads(teacher_key[0], student_key[0])
    ring = {0: own_keys}
    up = down = own_keys
    for step in range(1, 5):
        up = lax.ppermute(up, ("head", "kv_0"), z_shift(1))
        ring[step] = up
        if step < 4:
            down = lax.ppermute(down, ("head", "kv_0"), z_shift(-1))
            ring[8 - step] = down
    column = column_of(head[None, None], [ring[o] for o in range(8)])
    left = lax.ppermute(column, "kv_1", shift(4, 1))
    right = lax.ppermute(column, "kv_1", shift(4, -1))
    late_query, _ = lax.optimization_barrier((teacher_query[0], ring[4]))
    other_query = lax.ppermute(late_query, "head", [(0, 1), (1, 0)])

    my_pairs = lax.dynamic_slice_in_dim(pair_table, head * STUDENTS, STUDENTS, 0).reshape(-1)
    sel = jnp.stack([(my_pairs // PAIRS != head).astype(jnp.int32), my_pairs % PAIRS])
    kv_head = my_pairs // (HT // KVT)
    pad = jnp.zeros((2,), jnp.int32)
    elsewhere = kv_head // 2 != head
    slot = jnp.where(elsewhere, 4 * OWN, 0) + kv_head % 2
    stride = jnp.where(elsewhere, 2, OWN)
    m = jnp.arange(4, dtype=jnp.int32)

    def info(*offsets):
        position = [jnp.mod(z_hi - m, 4) * 4 + jnp.mod(x + o, 4) for o in offsets]
        position = jnp.concatenate(position)
        return jnp.stack(
            [
                jnp.full((16,), z_hi * 4 + x, jnp.int32),
                jnp.concatenate([slot, pad]),
                jnp.concatenate([stride, pad]),
                jnp.pad(position, (0, 16 - position.shape[0])),
            ]
        )

    qt = prepare(sel, teacher_query[0], other_query, student_query[0])
    state = attend(info(0), qt, [column], None, False)
    left, right, state = lax.optimization_barrier((left, right, state))
    half = COLUMN // 2
    far_a = lax.ppermute(left[:half], "kv_1", shift(4, 1))
    far_b = lax.ppermute(right[half:], "kv_1", shift(4, -1))
    state = attend(info(-1, 1), qt, [left, right], state, False)
    kl = attend(info(2), qt, [far_a, far_b], state, True)

    sums = jnp.pad(jnp.sum(kl, axis=1), (0, LANE - STUDENTS))
    everyone = ("dp_0", "dp_1", "kv_0", "kv_1")
    count = lax.axis_size(everyone)
    terms = lax.all_to_all(
        jnp.broadcast_to(sums, (count, LANE)), everyone, 0, 0, tiled=True
    )
    head_loss = jnp.sum(terms, axis=0)[:STUDENTS] / (count * ROWS)
    return (kl[None], head_loss)


def solution(mesh):
    split = Mesh(
        mesh.devices.reshape(4, 2, mesh.shape["head"], 4, 4),
        ("dp_0", "dp_1", "head", "kv_0", "kv_1"),
    )
    in_specs = (P(DP, KV, "head"), P(DP, KV, "head"), P(DP, KV, "head"), P(DP, KV, "head"), P())
    out_specs = (P(DP, "head", KV), P("head"))
    return jax.shard_map(
        per_device, mesh=split, in_specs=in_specs, out_specs=out_specs, check_vma=False
    )
```

```python
import functools
import math

import jax
import jax.numpy as jnp
from jax import lax
from jax.experimental import pallas as pl
from jax.experimental.pallas import tpu as pltpu
from jax.sharding import Mesh
from jax.sharding import PartitionSpec as P


HT = 28
KVT = 4
DH = 128
ROWS = 256
PAIRS = 14
STUDENTS = 7
HEADS = PAIRS + STUDENTS
GROUP = HT // KVT
KV = ("kv_0", "kv_1")
DP = ("dp_0", "dp_1")
LANE = 128
SUB = 8
MASKED = -1e30
LN2 = math.log(2.0)
KAPPA = 1.0 / (LN2 * math.sqrt(DH))
STATE = 3 * PAIRS + 2 * STUDENTS
TL, TC, SM, SL = PAIRS, 2 * PAIRS, 3 * PAIRS, 3 * PAIRS + STUDENTS
OWN = 3
OTHER = 2
CHUNK = OWN + OTHER
REST = 3 * CHUNK
SENT = 9
MIB = 1024 * 1024
SMEM = pl.BlockSpec(memory_space=pltpu.SMEM)
VMEM = pl.BlockSpec(memory_space=pltpu.VMEM)
ANY = pl.BlockSpec(memory_space=pl.ANY)


def heads_of(n):
    return jax.ShapeDtypeStruct((n, ROWS, DH), jnp.bfloat16)


def small(limit):
    return pltpu.CompilerParams(vmem_limit_bytes=limit * MIB)


def run_all(copies):
    for c in copies:
        c.start()
    for c in copies:
        c.wait()


def split_kernel(teacher, student, out):
    out[0] = teacher[:, :DH]
    out[1] = teacher[:, DH:]
    out[2] = student[...]


def split_heads(teacher, student):
    return pl.pallas_call(
        split_kernel,
        out_shape=heads_of(OWN),
        in_specs=[VMEM, VMEM],
        out_specs=VMEM,
        compiler_params=small(2),
        name="split_heads",
    )(teacher, student)


def queries_kernel(place, table, query, sent, more, sems):
    head = place[0, 0]
    theirs = (1 - head) * STUDENTS

    def each(act):
        rank = jnp.int32(0)
        for p in range(PAIRS):
            teacher = table[theirs + p // 2, p % 2]
            mine = lax.div(teacher, PAIRS) == head
            lanes = pl.ds(pl.multiple_of(lax.rem(teacher, PAIRS) * DH, DH), DH)

            @pl.when(jnp.logical_and(mine, rank < SENT))
            def _():
                act(pltpu.make_async_copy(query.at[:, lanes], sent.at[rank], sems.at[p]))

            @pl.when(jnp.logical_and(mine, rank >= SENT))
            def _():
                act(pltpu.make_async_copy(query.at[:, lanes], more.at[rank - SENT], sems.at[p]))

            rank = rank + mine.astype(jnp.int32)

    each(lambda c: c.start())
    each(lambda c: c.wait())


def queries_for_other(place, table, query):
    return pl.pallas_call(
        queries_kernel,
        out_shape=(heads_of(SENT), heads_of(PAIRS - SENT)),
        in_specs=[SMEM, SMEM, ANY],
        out_specs=(VMEM, VMEM),
        scratch_shapes=[pltpu.SemaphoreType.DMA((PAIRS,))],
        compiler_params=small(4),
        name="queries_for_other",
    )(place, table, query)


def own_chunk_kernel(place, own, ring_1, ring_7, out, sems):
    for head, pair in enumerate((ring_7, ring_1)):

        @pl.when(place[0, 0] == head)
        def _():
            run_all(
                [
                    pltpu.make_async_copy(own, out.at[pl.ds(0, OWN)], sems.at[0]),
                    pltpu.make_async_copy(
                        pair.at[pl.ds(0, OTHER)], out.at[pl.ds(OWN, OTHER)], sems.at[1]
                    ),
                ]
            )


def own_chunk(place, own, ring_1, ring_7):
    return pl.pallas_call(
        own_chunk_kernel,
        out_shape=heads_of(CHUNK),
        in_specs=[SMEM, ANY, ANY, ANY],
        out_specs=VMEM,
        scratch_shapes=[pltpu.SemaphoreType.DMA((2,))],
        compiler_params=small(2),
        name="own_chunk",
    )(place, own, ring_1, ring_7)


def rest_kernel(place, *refs):
    ring, out, sems = refs[:7], refs[7], refs[8]
    for head in range(2):

        @pl.when(place[0, 0] == head)
        def _():
            copies = []
            for m in range(1, 4):
                own = ring[2 * m - 1]
                other = ring[(2 * m - 1 + 2 * head) - 1]
                copies.append(
                    pltpu.make_async_copy(
                        own, out.at[pl.ds(OWN * (m - 1), OWN)], sems.at[m - 1]
                    )
                )
                copies.append(
                    pltpu.make_async_copy(
                        other.at[pl.ds(0, OTHER)],
                        out.at[pl.ds(3 * OWN + OTHER * (m - 1), OTHER)],
                        sems.at[m + 2],
                    )
                )
            run_all(copies)


def rest_of(place, ring):
    return pl.pallas_call(
        rest_kernel,
        out_shape=heads_of(REST),
        in_specs=[SMEM] + [ANY] * 7,
        out_specs=VMEM,
        scratch_shapes=[pltpu.SemaphoreType.DMA((6,))],
        compiler_params=small(4),
        name="rest_of",
    )(place, *ring)


def scaled(q):
    q = q.astype(jnp.float32) * KAPPA
    high = q.astype(jnp.bfloat16)
    low = (q - high.astype(jnp.float32)).astype(jnp.bfloat16)
    return jnp.concatenate([high, low], axis=1)


def fill_queries(place, table, own, sent, more, student, rows):
    head = place[0, 0]
    for s in range(STUDENTS):
        rows[PAIRS + s] = scaled(student[:, s * DH : (s + 1) * DH])
    rank = jnp.int32(0)
    for p in range(PAIRS):
        teacher = table[head * STUDENTS + p // 2, p % 2]
        mine = lax.div(teacher, PAIRS) == head
        lanes = pl.ds(pl.multiple_of(lax.rem(teacher, PAIRS) * DH, DH), DH)

        @pl.when(mine)
        def _():
            rows[p] = scaled(own[:, lanes])

        @pl.when(jnp.logical_and(jnp.logical_not(mine), rank < SENT))
        def _():
            rows[p] = scaled(sent[rank])

        @pl.when(jnp.logical_and(jnp.logical_not(mine), rank >= SENT))
        def _():
            rows[p] = scaled(more[rank - SENT])

        rank = rank + 1 - mine.astype(jnp.int32)


def attend_kernel(first, last, counts, blocks, place, table, plan, *refs):
    refs = list(refs)
    take = lambda n: [refs.pop(0) for _ in range(n)]
    groups = take(len(counts))
    if first:
        own, sent, more, student = take(4)
        state, rows = take(2)
    else:
        rows, before = take(2)
        if last:
            out, sums = take(2)
        else:
            (state,) = take(1)
    (keys,) = take(1)
    if last:
        (state,) = take(1)
    (sems,) = refs
    head, z_hi, x = place[0, 0], place[0, 1], place[0, 2]
    row_block = z_hi * 4 + x

    copies = []
    at = 0
    for g, n in enumerate(counts):
        copies.append(pltpu.make_async_copy(groups[g], keys.at[pl.ds(at, n)], sems.at[g]))
        at += n
    for c in copies:
        c.start()
    if first:
        for part, value in ((0, MASKED), (TL, 0.0), (TC, 0.0)):
            state[part : part + PAIRS] = jnp.full((PAIRS, SUB, ROWS), value, jnp.float32)
        for part, value in ((SM, MASKED), (SL, 0.0)):
            state[part : part + STUDENTS] = jnp.full((STUDENTS, SUB, ROWS), value, jnp.float32)
        fill_queries(place, table, own, sent, more, student, rows)
    else:
        state[...] = before[...]
    for c in copies:
        c.wait()

    def product(k, p):
        return lax.dot_general(
            jnp.concatenate([k, k], axis=1),
            rows[p],
            (((1,), (1,)), ((), ())),
            preferred_element_type=jnp.float32,
        )

    def update(logits, mask, m_index, l_index):
        if mask is not None:
            logits = jnp.where(mask, logits, MASKED)
        folded = logits.reshape(ROWS // SUB, SUB, ROWS)
        old = state[m_index]
        new = jnp.maximum(old, jnp.max(folded, axis=0))
        weights = jnp.exp2(folded - new[None])
        rescale = jnp.exp2(old - new)
        state[m_index] = new
        state[l_index] = state[l_index] * rescale + jnp.sum(weights, axis=0)
        return weights, rescale

    def block(own_at, other_at, masked):
        mask = None
        if masked:
            key_pos = lax.broadcasted_iota(jnp.int32, (ROWS, ROWS), 0)
            row_pos = lax.broadcasted_iota(jnp.int32, (ROWS, ROWS), 1)
            mask = key_pos <= row_pos
        student_keys = keys[own_at + 2]
        for s in range(STUDENTS):
            zs = product(student_keys, PAIRS + s)
            update(zs, mask, SM + s, SL + s)
            for c in range(2):
                p = 2 * s + c
                kv_head = lax.div(table[head * STUDENTS + s, c], GROUP)
                base = jnp.where(lax.div(kv_head, 2) == head, own_at, other_at)
                zt = product(keys[base + lax.rem(kv_head, 2)], p)
                weights, rescale = update(zt, mask, p, TL + p)
                gap = (zt - zs).reshape(ROWS // SUB, SUB, ROWS)
                state[TC + p] = state[TC + p] * rescale + jnp.sum(weights * gap, axis=0)

    def step(i, carry):
        chunk = lax.bitwise_and(z_hi - plan[0, i], 3)
        position = chunk * 4 + lax.bitwise_and(x + plan[1, i], 3)

        @pl.when(position < row_block)
        def _():
            block(plan[2, i], plan[3, i], False)

        if first:

            @pl.when(position == row_block)
            def _():
                block(plan[2, i], plan[3, i], True)

        return carry

    lax.fori_loop(0, blocks, step, 0)

    if not last:
        return

    def merged(m8, l8):
        top = jnp.max(m8, axis=0, keepdims=True)
        factor = jnp.exp2(m8 - top)
        total = jnp.sum(l8 * factor, axis=0, keepdims=True)
        return factor, total, LN2 * top + jnp.log(total)

    lane = lax.broadcasted_iota(jnp.int32, (1, LANE), 1)
    line = jnp.zeros((1, LANE), jnp.float32)
    for s in range(STUDENTS):
        _, _, s_lse = merged(state[SM + s], state[SL + s])
        value = 2.0 * s_lse
        for c in range(2):
            p = 2 * s + c
            factor, total, t_lse = merged(state[p], state[TL + p])
            cross = jnp.sum(state[TC + p] * factor, axis=0, keepdims=True)
            value = value + (LN2 * cross / total - t_lse)
        out[s : s + 1, :] = value
        line = jnp.where(lane == s, jnp.sum(value, axis=1, keepdims=True), line)
    sums[...] = jnp.broadcast_to(line, sums.shape)


def attend(place, table, plan, groups, queries=None, rows=None, state=None, copies_out=0):
    first = queries is not None
    last = copies_out > 0
    counts = tuple(g.shape[0] for g in groups)
    blocks = plan.shape[1]
    state_shape = jax.ShapeDtypeStruct((STATE, SUB, ROWS), jnp.float32)
    rows_shape = jax.ShapeDtypeStruct((HEADS, ROWS, 2 * DH), jnp.bfloat16)
    if first:
        extra, out_shape = list(queries), (state_shape, rows_shape)
    elif last:
        extra = [rows, state]
        out_shape = (
            jax.ShapeDtypeStruct((STUDENTS, ROWS), jnp.float32),
            jax.ShapeDtypeStruct((copies_out, LANE), jnp.float32),
        )
    else:
        extra, out_shape = [rows, state], state_shape
    scratch = [pltpu.VMEM((sum(counts), ROWS, DH), jnp.bfloat16)]
    if last:
        scratch.append(pltpu.VMEM(state_shape.shape, jnp.float32))
    scratch.append(pltpu.SemaphoreType.DMA((len(groups),)))
    return pl.pallas_call(
        functools.partial(attend_kernel, first, last, counts, blocks),
        out_shape=out_shape,
        in_specs=[SMEM] * 3 + [ANY] * len(groups) + [VMEM] * len(extra),
        out_specs=jax.tree.map(lambda _: VMEM, out_shape),
        scratch_shapes=scratch,
        compiler_params=small(24),
        cost_estimate=pl.CostEstimate(
            flops=blocks * HEADS * 2 * ROWS * ROWS * 2 * DH,
            bytes_accessed=blocks * ROWS * CHUNK * DH * 2,
            transcendentals=blocks * HEADS * ROWS * ROWS,
        ),
        name="attend",
    )(place, table, plan, *groups, *extra)


def shift(n, by):
    return [(i, (i + by) % n) for i in range(n)]


def z_place(ring):
    ring %= 8
    return (ring % 2) * 4 + ring // 2


def z_shift(by):
    return [(z_place(i), z_place(i + by)) for i in range(8)]


def plan_of(blocks):
    return jnp.array([list(row) for row in zip(*blocks)], jnp.int32)


def rest_blocks(by, base):
    return [
        (m, by, base + OWN * (m - 1), base + 3 * OWN + OTHER * (m - 1)) for m in range(1, 4)
    ]


def program(teacher_query, teacher_key, student_query, student_key, pair_table):
    head = lax.axis_index("head")
    place = jnp.stack([head, lax.axis_index("kv_0"), lax.axis_index("kv_1")])[None]

    along_x = lambda a, by: lax.ppermute(a, "kv_1", shift(4, by))
    along_z = lambda a, by: lax.ppermute(a, ("head", "kv_0"), z_shift(by))
    other_side = [(0, 1), (1, 0)]

    ring = {0: split_heads(teacher_key[0], student_key[0])}
    ring[1] = along_z(ring[0], 1)
    ring[7] = along_z(ring[0], -1)
    sent, more = queries_for_other(place, pair_table, teacher_query[0])
    sent, ring[1], ring[7] = lax.optimization_barrier((sent, ring[1], ring[7]))
    sent = lax.ppermute(sent, "head", other_side)
    mine = own_chunk(place, ring[0], ring[1], ring[7])
    near = [mine, along_x(mine, 1), along_x(mine, -1), along_x(mine, 2)]
    for step in range(2, 5):
        ring[step] = along_z(ring[step - 1], 1)
        if step < 4:
            ring[8 - step] = along_z(ring[9 - step], -1)
    my_pairs = lax.dynamic_slice_in_dim(pair_table, head * STUDENTS, STUDENTS, 0)
    count = jnp.sum((my_pairs // PAIRS != head).astype(jnp.int32))
    more = lax.cond(
        count > SENT, lambda q: lax.ppermute(q, "head", other_side), lambda q: q, more
    )

    rest = rest_of(place, [ring[o] for o in range(1, 8)])
    left, right = along_x(rest, 1), along_x(rest, -1)
    near_plan = [(0, by, CHUNK * n, CHUNK * n + OWN) for n, by in enumerate((0, -1, 1, 2))]
    state, rows = attend(
        place,
        pair_table,
        plan_of(near_plan + rest_blocks(0, 4 * CHUNK)),
        near + [rest],
        queries=(teacher_query[0], sent, more, student_query[0]),
    )
    left, right, state = lax.optimization_barrier((left, right, state))
    cut = (REST + 1) // 2
    far = [along_x(left[:cut], 1), along_x(right[cut:], -1)]
    state = attend(
        place,
        pair_table,
        plan_of(rest_blocks(-1, 0) + rest_blocks(1, REST)),
        [left, right],
        rows=rows,
        state=state,
    )
    everyone = ("dp_0", "dp_1", "kv_0", "kv_1")
    devices = lax.axis_size(everyone)
    kl, sums = attend(
        place,
        pair_table,
        plan_of(rest_blocks(2, 0)),
        far,
        rows=rows,
        state=state,
        copies_out=devices,
    )
    terms = lax.all_to_all(sums, everyone, 0, 0, tiled=True)
    head_loss = jnp.sum(terms, axis=0)[:STUDENTS] / (devices * ROWS)
    return (kl[None], head_loss)


def solution(mesh):
    split = Mesh(
        mesh.devices.reshape(4, 2, mesh.shape["head"], 4, 4),
        ("dp_0", "dp_1", "head", "kv_0", "kv_1"),
    )
    in_specs = (P(DP, KV, "head"), P(DP, KV, "head"), P(DP, KV, "head"), P(DP, KV, "head"), P())
    out_specs = (P(DP, "head", KV), P("head"))
    return jax.shard_map(
        program, mesh=split, in_specs=in_specs, out_specs=out_specs, check_vma=False
    )
```

```python
import functools
import math

import jax
import jax.numpy as jnp
from jax import lax
from jax.experimental import pallas as pl
from jax.experimental.pallas import tpu as pltpu
from jax.sharding import Mesh
from jax.sharding import PartitionSpec as P


HT = 28
KVT = 4
DH = 128
ROWS = 256
PAIRS = 14
STUDENTS = 7
HEADS = PAIRS + STUDENTS
GROUP = HT // KVT
KV = ("kv_0", "kv_1")
DP = ("dp_0", "dp_1")
LANE = 128
SUB = 8
MASKED = -1e30
LN2 = math.log(2.0)
KAPPA = 1.0 / (LN2 * math.sqrt(DH))
STATE = 3 * PAIRS + 2 * STUDENTS
TL, TC, SM, SL = PAIRS, 2 * PAIRS, 3 * PAIRS, 3 * PAIRS + STUDENTS
OWN = 3
OTHER = 2
CHUNK = OWN + OTHER
SENT = 9
MIB = 1024 * 1024
SMEM = pl.BlockSpec(memory_space=pltpu.SMEM)
VMEM = pl.BlockSpec(memory_space=pltpu.VMEM)
ANY = pl.BlockSpec(memory_space=pl.ANY)
HBM = pl.BlockSpec(memory_space=pltpu.HBM)


def heads_of(n):
    return jax.ShapeDtypeStruct((n, ROWS, DH), jnp.bfloat16)


def small(limit):
    return pltpu.CompilerParams(vmem_limit_bytes=limit * MIB)


def run_all(copies):
    for c in copies:
        c.start()
    for c in copies:
        c.wait()


def split_kernel(teacher, student, out, sems):
    run_all(
        [
            pltpu.make_async_copy(teacher.at[:, pl.ds(0, DH)], out.at[0], sems.at[0]),
            pltpu.make_async_copy(teacher.at[:, pl.ds(DH, DH)], out.at[1], sems.at[1]),
            pltpu.make_async_copy(student, out.at[2], sems.at[2]),
        ]
    )


def split_heads(teacher, student):
    return pl.pallas_call(
        split_kernel,
        out_shape=heads_of(OWN),
        in_specs=[HBM, HBM],
        out_specs=VMEM,
        scratch_shapes=[pltpu.SemaphoreType.DMA((3,))],
        compiler_params=small(2),
        name="split_heads",
    )(teacher, student)


def queries_kernel(place, table, query, sent, more, count, sems):
    head = place[0, 0]
    theirs = (1 - head) * STUDENTS

    def each(act):
        rank = jnp.int32(0)
        for p in range(PAIRS):
            teacher = table[theirs + p // 2, p % 2]
            mine = lax.div(teacher, PAIRS) == head
            lanes = pl.ds(pl.multiple_of(lax.rem(teacher, PAIRS) * DH, DH), DH)

            @pl.when(jnp.logical_and(mine, rank < SENT))
            def _():
                act(pltpu.make_async_copy(query.at[:, lanes], sent.at[rank], sems.at[p]))

            @pl.when(jnp.logical_and(mine, rank >= SENT))
            def _():
                act(pltpu.make_async_copy(query.at[:, lanes], more.at[rank - SENT], sems.at[p]))

            rank = rank + mine.astype(jnp.int32)
        return rank

    count[0, 0] = each(lambda c: c.start())
    each(lambda c: c.wait())


def queries_for_other(place, table, query):
    return pl.pallas_call(
        queries_kernel,
        out_shape=(
            heads_of(SENT),
            heads_of(PAIRS - SENT),
            jax.ShapeDtypeStruct((1, 1), jnp.int32),
        ),
        in_specs=[SMEM, SMEM, HBM],
        out_specs=(VMEM, VMEM, SMEM),
        scratch_shapes=[pltpu.SemaphoreType.DMA((PAIRS,))],
        compiler_params=small(4),
        name="queries_for_other",
    )(place, table, query)


def own_chunk_kernel(place, own, ring_1, ring_7, out, sems):
    for head, pair in enumerate((ring_7, ring_1)):

        @pl.when(place[0, 0] == head)
        def _():
            run_all(
                [
                    pltpu.make_async_copy(own, out.at[pl.ds(0, OWN)], sems.at[0]),
                    pltpu.make_async_copy(
                        pair.at[pl.ds(0, OTHER)], out.at[pl.ds(OWN, OTHER)], sems.at[1]
                    ),
                ]
            )


def own_chunk(place, own, ring_1, ring_7):
    return pl.pallas_call(
        own_chunk_kernel,
        out_shape=heads_of(CHUNK),
        in_specs=[SMEM, ANY, ANY, ANY],
        out_specs=VMEM,
        scratch_shapes=[pltpu.SemaphoreType.DMA((2,))],
        compiler_params=small(2),
        name="own_chunk",
    )(place, own, ring_1, ring_7)


def rest_kernel(chunks, place, *refs):
    ring, out, sems = refs[:-2], refs[-2], refs[-1]
    for head in range(2):

        @pl.when(place[0, 0] == head)
        def _():
            copies = []
            for n in range(chunks):
                own, other = ring[3 * n], ring[3 * n + 1 + head]
                copies.append(
                    pltpu.make_async_copy(own, out.at[pl.ds(CHUNK * n, OWN)], sems.at[n, 0])
                )
                copies.append(
                    pltpu.make_async_copy(
                        other.at[pl.ds(0, OTHER)],
                        out.at[pl.ds(CHUNK * n + OWN, OTHER)],
                        sems.at[n, 1],
                    )
                )
            run_all(copies)


def rest_of(place, ring, chunks):
    parts = [ring[o] for m in chunks for o in (2 * m, 2 * m - 1, (2 * m + 1) % 8)]
    return pl.pallas_call(
        functools.partial(rest_kernel, len(chunks)),
        out_shape=heads_of(CHUNK * len(chunks)),
        in_specs=[SMEM] + [ANY] * len(parts),
        out_specs=VMEM,
        scratch_shapes=[pltpu.SemaphoreType.DMA((len(chunks), 2))],
        compiler_params=small(4),
        name="rest_of",
    )(place, *parts)


def scaled(q):
    q = q.astype(jnp.float32) * KAPPA
    high = q.astype(jnp.bfloat16)
    low = (q - high.astype(jnp.float32)).astype(jnp.bfloat16)
    return jnp.concatenate([high, low], axis=1)


def fill_queries(place, table, own, sent, more, student, rows):
    head = place[0, 0]
    for s in range(STUDENTS):
        rows[PAIRS + s] = scaled(student[:, s * DH : (s + 1) * DH])
    rank = jnp.int32(0)
    for p in range(PAIRS):
        teacher = table[head * STUDENTS + p // 2, p % 2]
        mine = lax.div(teacher, PAIRS) == head
        lanes = pl.ds(pl.multiple_of(lax.rem(teacher, PAIRS) * DH, DH), DH)

        @pl.when(mine)
        def _():
            rows[p] = scaled(own[:, lanes])

        @pl.when(jnp.logical_and(jnp.logical_not(mine), rank < SENT))
        def _():
            rows[p] = scaled(sent[rank])

        @pl.when(jnp.logical_and(jnp.logical_not(mine), rank >= SENT))
        def _():
            rows[p] = scaled(more[rank - SENT])

        rank = rank + 1 - mine.astype(jnp.int32)


def attend_kernel(first, last, counts, blocks, place, table, plan, *refs):
    refs = list(refs)
    take = lambda n: [refs.pop(0) for _ in range(n)]
    groups = take(len(counts))
    if first:
        own, sent, more, student = take(4)
        state, rows = take(2)
    else:
        rows, before = take(2)
        if last:
            out, sums = take(2)
        else:
            (state,) = take(1)
    (keys,) = take(1)
    if first:
        own_vmem, student_vmem = take(2)
    if last:
        (state,) = take(1)
    (sems,) = refs
    head, z_hi, x = place[0, 0], place[0, 1], place[0, 2]
    row_block = z_hi * 4 + x

    copies, arrivals = [], []
    at = 0
    for g, n in enumerate(counts):
        copies.append(pltpu.make_async_copy(groups[g], keys.at[pl.ds(at, n)], sems.at[g]))
        arrivals.append((at // CHUNK, copies[-1]))
        at += n
    if first:
        inputs = [
            pltpu.make_async_copy(own, own_vmem, sems.at[len(counts)]),
            pltpu.make_async_copy(student, student_vmem, sems.at[len(counts) + 1]),
        ]
        for c in inputs:
            c.start()
    for c in copies:
        c.start()
    if first:
        for part, value in ((0, MASKED), (TL, 0.0), (TC, 0.0)):
            state[part : part + PAIRS] = jnp.full((PAIRS, SUB, ROWS), value, jnp.float32)
        for part, value in ((SM, MASKED), (SL, 0.0)):
            state[part : part + STUDENTS] = jnp.full((STUDENTS, SUB, ROWS), value, jnp.float32)
        for c in inputs:
            c.wait()
        fill_queries(place, table, own_vmem, sent, more, student_vmem, rows)
    else:
        state[...] = before[...]

    def product(k, p):
        return lax.dot_general(
            jnp.concatenate([k, k], axis=1),
            rows[p],
            (((1,), (1,)), ((), ())),
            preferred_element_type=jnp.float32,
        )

    def update(logits, mask, m_index, l_index):
        if mask is not None:
            logits = jnp.where(mask, logits, MASKED)
        folded = logits.reshape(ROWS // SUB, SUB, ROWS)
        old = state[m_index]
        new = jnp.maximum(old, jnp.max(folded, axis=0))
        weights = jnp.exp2(folded - new[None])
        rescale = jnp.exp2(old - new)
        state[m_index] = new
        state[l_index] = state[l_index] * rescale + jnp.sum(weights, axis=0)
        return weights, rescale

    def block(own_at, other_at, masked):
        mask = None
        if masked:
            key_pos = lax.broadcasted_iota(jnp.int32, (ROWS, ROWS), 0)
            row_pos = lax.broadcasted_iota(jnp.int32, (ROWS, ROWS), 1)
            mask = key_pos <= row_pos
        student_keys = keys[own_at + 2]
        for s in range(STUDENTS):
            zs = product(student_keys, PAIRS + s)
            update(zs, mask, SM + s, SL + s)
            for c in range(2):
                p = 2 * s + c
                kv_head = lax.div(table[head * STUDENTS + s, c], GROUP)
                base = jnp.where(lax.div(kv_head, 2) == head, own_at, other_at)
                zt = product(keys[base + lax.rem(kv_head, 2)], p)
                weights, rescale = update(zt, mask, p, TL + p)
                gap = (zt - zs).reshape(ROWS // SUB, SUB, ROWS)
                state[TC + p] = state[TC + p] * rescale + jnp.sum(weights * gap, axis=0)

    def step(i, carry):
        for at_block, c in arrivals:

            @pl.when(i == at_block)
            def _():
                c.wait()

        chunk = lax.bitwise_and(z_hi - plan[0, i], 3)
        position = chunk * 4 + lax.bitwise_and(x + plan[1, i], 3)

        @pl.when(position < row_block)
        def _():
            block(CHUNK * i, CHUNK * i + OWN, False)

        if first:

            @pl.when(position == row_block)
            def _():
                block(CHUNK * i, CHUNK * i + OWN, True)

        return carry

    lax.fori_loop(0, blocks, step, 0)

    if not last:
        return

    def merged(m8, l8):
        top = jnp.max(m8, axis=0, keepdims=True)
        factor = jnp.exp2(m8 - top)
        total = jnp.sum(l8 * factor, axis=0, keepdims=True)
        return factor, total, LN2 * top + jnp.log(total)

    lane = lax.broadcasted_iota(jnp.int32, (1, LANE), 1)
    line = jnp.zeros((1, LANE), jnp.float32)
    for s in range(STUDENTS):
        _, _, s_lse = merged(state[SM + s], state[SL + s])
        value = 2.0 * s_lse
        for c in range(2):
            p = 2 * s + c
            factor, total, t_lse = merged(state[p], state[TL + p])
            cross = jnp.sum(state[TC + p] * factor, axis=0, keepdims=True)
            value = value + (LN2 * cross / total - t_lse)
        out[s : s + 1, :] = value
        line = jnp.where(lane == s, jnp.sum(value, axis=1, keepdims=True), line)
    sums[...] = jnp.broadcast_to(line, sums.shape)


def attend(place, table, plan, groups, queries=None, rows=None, state=None, copies_out=0):
    first = queries is not None
    last = copies_out > 0
    counts = tuple(g.shape[0] for g in groups)
    blocks = plan.shape[1]
    state_shape = jax.ShapeDtypeStruct((STATE, SUB, ROWS), jnp.float32)
    rows_shape = jax.ShapeDtypeStruct((HEADS, ROWS, 2 * DH), jnp.bfloat16)
    if first:
        extra, out_shape = list(queries), (state_shape, rows_shape)
    elif last:
        extra = [rows, state]
        out_shape = (
            jax.ShapeDtypeStruct((STUDENTS, ROWS), jnp.float32),
            jax.ShapeDtypeStruct((copies_out, LANE), jnp.float32),
        )
    else:
        extra, out_shape = [rows, state], state_shape
    extra_specs = [HBM, VMEM, VMEM, HBM] if first else [VMEM, VMEM]
    scratch = [pltpu.VMEM((sum(counts), ROWS, DH), jnp.bfloat16)]
    if first:
        scratch.append(pltpu.VMEM((ROWS, PAIRS * DH), jnp.bfloat16))
        scratch.append(pltpu.VMEM((ROWS, STUDENTS * DH), jnp.bfloat16))
    if last:
        scratch.append(pltpu.VMEM(state_shape.shape, jnp.float32))
    scratch.append(pltpu.SemaphoreType.DMA((len(groups) + 2,)))
    return pl.pallas_call(
        functools.partial(attend_kernel, first, last, counts, blocks),
        out_shape=out_shape,
        in_specs=[SMEM] * 3 + [ANY] * len(groups) + extra_specs,
        out_specs=jax.tree.map(lambda _: VMEM, out_shape),
        scratch_shapes=scratch,
        compiler_params=small(24),
        cost_estimate=pl.CostEstimate(
            flops=blocks * HEADS * 2 * ROWS * ROWS * 2 * DH,
            bytes_accessed=blocks * ROWS * CHUNK * DH * 2,
            transcendentals=blocks * HEADS * ROWS * ROWS,
        ),
        name="attend",
    )(place, table, plan, *groups, *extra)


def shift(n, by):
    return [(i, (i + by) % n) for i in range(n)]


def z_place(ring):
    ring %= 8
    return (ring % 2) * 4 + ring // 2


def z_shift(by):
    return [(z_place(i), z_place(i + by)) for i in range(8)]


def plan_of(blocks):
    return jnp.array([list(row) for row in zip(*blocks)], jnp.int32)


def program(teacher_query, teacher_key, student_query, student_key, pair_table):
    head = lax.axis_index("head")
    place = jnp.stack([head, lax.axis_index("kv_0"), lax.axis_index("kv_1")])[None]

    along_x = lambda a, by: lax.ppermute(a, "kv_1", shift(4, by))
    along_z = lambda a, by: lax.ppermute(a, ("head", "kv_0"), z_shift(by))
    other_side = [(0, 1), (1, 0)]

    ring = {0: split_heads(teacher_key[0], student_key[0])}
    sent, more, count = queries_for_other(place, pair_table, teacher_query[0])
    ring[1] = along_z(ring[0], 1)
    ring[7] = along_z(ring[0], -1)
    sent = lax.ppermute(sent, "head", other_side)
    mine = own_chunk(place, ring[0], ring[1], ring[7])
    near_a = along_x(mine, 1)
    near_b = along_x(mine, -1)
    near_c = along_x(near_a[:OTHER], 1)
    near_d = along_x(near_b[OTHER:], -1)
    for step in range(2, 5):
        ring[step] = along_z(ring[step - 1], 1)
        if step < 4:
            ring[8 - step] = along_z(ring[9 - step], -1)
    more = lax.cond(
        count[0, 0] > SENT, lambda q: lax.ppermute(q, "head", other_side), lambda q: q, more
    )

    rest_13 = rest_of(place, ring, (1, 3))
    left_13 = along_x(rest_13, 1)
    right_13 = along_x(rest_13, -1)
    rest_2 = rest_of(place, ring, (2,))
    left_2 = along_x(rest_2, 1)
    right_2 = along_x(rest_2, -1)
    state, rows = attend(
        place,
        pair_table,
        plan_of([(0, 0), (0, -1), (0, 1), (0, 2), (1, 0), (3, 0), (2, 0)]),
        [mine, near_a, near_b, near_c, near_d, rest_13, rest_2],
        queries=(teacher_query[0], sent, more, student_query[0]),
    )
    left_13, right_13, left_2, right_2, state = lax.optimization_barrier(
        (left_13, right_13, left_2, right_2, state)
    )
    far_1 = along_x(left_13[:CHUNK], 1)
    far_3 = along_x(right_13[CHUNK:], -1)
    far_2 = along_x(left_2, 1)
    state = attend(
        place,
        pair_table,
        plan_of([(1, -1), (3, -1), (1, 1), (3, 1), (2, -1), (2, 1)]),
        [left_13, right_13, left_2, right_2],
        rows=rows,
        state=state,
    )
    everyone = ("dp_0", "dp_1", "kv_0", "kv_1")
    devices = lax.axis_size(everyone)
    kl, sums = attend(
        place,
        pair_table,
        plan_of([(1, 2), (3, 2), (2, 2)]),
        [far_1, far_3, far_2],
        rows=rows,
        state=state,
        copies_out=devices,
    )
    terms = lax.all_to_all(sums, everyone, 0, 0, tiled=True)
    head_loss = jnp.sum(terms, axis=0)[:STUDENTS] / (devices * ROWS)
    return (kl[None], head_loss)


def solution(mesh):
    split = Mesh(
        mesh.devices.reshape(4, 2, mesh.shape["head"], 4, 4),
        ("dp_0", "dp_1", "head", "kv_0", "kv_1"),
    )
    in_specs = (P(DP, KV, "head"), P(DP, KV, "head"), P(DP, KV, "head"), P(DP, KV, "head"), P())
    out_specs = (P(DP, "head", KV), P("head"))
    return jax.shard_map(
        program, mesh=split, in_specs=in_specs, out_specs=out_specs, check_vma=False
    )
```

```python
import functools
import math

import jax
import jax.numpy as jnp
from jax import lax
from jax.experimental import pallas as pl
from jax.experimental.pallas import tpu as pltpu
from jax.sharding import Mesh
from jax.sharding import PartitionSpec as P


HT = 28
KVT = 4
DH = 128
ROWS = 256
PAIRS = 14
STUDENTS = 7
HEADS = PAIRS + STUDENTS
GROUP = HT // KVT
KV = ("kv_0", "kv_1")
DP = ("dp_0", "dp_1")
LANE = 128
SUB = 8
MASKED = -1e30
LN2 = math.log(2.0)
KAPPA = 1.0 / (LN2 * math.sqrt(DH))
STATE = 3 * PAIRS + 2 * STUDENTS
TL, TC, SM, SL = PAIRS, 2 * PAIRS, 3 * PAIRS, 3 * PAIRS + STUDENTS
OWN = 3
OTHER = 2
CHUNK = OWN + OTHER
PIECES = (2, 2, 2, 3)
SENT = sum(PIECES)
MIB = 1024 * 1024
SMEM = pl.BlockSpec(memory_space=pltpu.SMEM)
VMEM = pl.BlockSpec(memory_space=pltpu.VMEM)
ANY = pl.BlockSpec(memory_space=pl.ANY)
HBM = pl.BlockSpec(memory_space=pltpu.HBM)


def heads_of(n):
    return jax.ShapeDtypeStruct((n, ROWS, DH), jnp.bfloat16)


def small(limit):
    return pltpu.CompilerParams(vmem_limit_bytes=limit * MIB)


def run_all(copies):
    for c in copies:
        c.start()
    for c in copies:
        c.wait()


def split_kernel(teacher, student, out, sems):
    run_all(
        [
            pltpu.make_async_copy(teacher.at[:, pl.ds(0, DH)], out.at[0], sems.at[0]),
            pltpu.make_async_copy(teacher.at[:, pl.ds(DH, DH)], out.at[1], sems.at[1]),
            pltpu.make_async_copy(student, out.at[2], sems.at[2]),
        ]
    )


def split_heads(teacher, student):
    return pl.pallas_call(
        split_kernel,
        out_shape=heads_of(OWN),
        in_specs=[HBM, HBM],
        out_specs=VMEM,
        scratch_shapes=[pltpu.SemaphoreType.DMA((3,))],
        compiler_params=small(2),
        name="split_heads",
    )(teacher, student)


def queries_kernel(place, table, query, sent, count, sems):
    head = place[0, 0]
    theirs = (1 - head) * STUDENTS

    def each(act):
        rank = jnp.int32(0)
        for p in range(PAIRS):
            teacher = table[theirs + p // 2, p % 2]
            mine = lax.div(teacher, PAIRS) == head
            lanes = pl.ds(pl.multiple_of(lax.rem(teacher, PAIRS) * DH, DH), DH)

            @pl.when(mine)
            def _():
                act(pltpu.make_async_copy(query.at[:, lanes], sent.at[rank], sems.at[p]))

            rank = rank + mine.astype(jnp.int32)
        return rank

    count[0, 0] = each(lambda c: c.start())
    each(lambda c: c.wait())


def queries_for_other(place, table, query):
    return pl.pallas_call(
        queries_kernel,
        out_shape=(heads_of(PAIRS), jax.ShapeDtypeStruct((1, 1), jnp.int32)),
        in_specs=[SMEM, SMEM, ANY],
        out_specs=(VMEM, SMEM),
        scratch_shapes=[pltpu.SemaphoreType.DMA((PAIRS,))],
        compiler_params=small(4),
        name="queries_for_other",
    )(place, table, query)


def own_chunk_kernel(place, own, ring_1, ring_7, out, sems):
    for head, pair in enumerate((ring_7, ring_1)):

        @pl.when(place[0, 0] == head)
        def _():
            run_all(
                [
                    pltpu.make_async_copy(own, out.at[pl.ds(0, OWN)], sems.at[0]),
                    pltpu.make_async_copy(
                        pair.at[pl.ds(0, OTHER)], out.at[pl.ds(OWN, OTHER)], sems.at[1]
                    ),
                ]
            )


def own_chunk(place, own, ring_1, ring_7):
    return pl.pallas_call(
        own_chunk_kernel,
        out_shape=heads_of(CHUNK),
        in_specs=[SMEM, ANY, ANY, ANY],
        out_specs=VMEM,
        scratch_shapes=[pltpu.SemaphoreType.DMA((2,))],
        compiler_params=small(2),
        name="own_chunk",
    )(place, own, ring_1, ring_7)


def rest_kernel(chunks, place, *refs):
    ring, out, sems = refs[:-2], refs[-2], refs[-1]
    for head in range(2):

        @pl.when(place[0, 0] == head)
        def _():
            copies = []
            for n in range(chunks):
                own, other = ring[3 * n], ring[3 * n + 1 + head]
                copies.append(
                    pltpu.make_async_copy(own, out.at[pl.ds(CHUNK * n, OWN)], sems.at[n, 0])
                )
                copies.append(
                    pltpu.make_async_copy(
                        other.at[pl.ds(0, OTHER)],
                        out.at[pl.ds(CHUNK * n + OWN, OTHER)],
                        sems.at[n, 1],
                    )
                )
            run_all(copies)


def rest_of(place, ring, chunks):
    parts = [ring[o] for m in chunks for o in (2 * m, 2 * m - 1, (2 * m + 1) % 8)]
    return pl.pallas_call(
        functools.partial(rest_kernel, len(chunks)),
        out_shape=heads_of(CHUNK * len(chunks)),
        in_specs=[SMEM] + [ANY] * len(parts),
        out_specs=VMEM,
        scratch_shapes=[pltpu.SemaphoreType.DMA((len(chunks), 2))],
        compiler_params=small(4),
        name="rest_of",
    )(place, *parts)


def scaled(q):
    q = q.astype(jnp.float32) * KAPPA
    high = q.astype(jnp.bfloat16)
    low = (q - high.astype(jnp.float32)).astype(jnp.bfloat16)
    return jnp.concatenate([high, low], axis=1)


def prepare_kernel(place, table, own, student, rows):
    head = place[0, 0]
    for s in range(STUDENTS):
        rows[PAIRS + s] = scaled(student[:, s * DH : (s + 1) * DH])
    for p in range(PAIRS):
        teacher = table[head * STUDENTS + p // 2, p % 2]
        lanes = pl.ds(pl.multiple_of(lax.rem(teacher, PAIRS) * DH, DH), DH)

        @pl.when(lax.div(teacher, PAIRS) == head)
        def _():
            rows[p] = scaled(own[:, lanes])


def prepare(place, table, own, student):
    return pl.pallas_call(
        prepare_kernel,
        out_shape=jax.ShapeDtypeStruct((HEADS, ROWS, 2 * DH), jnp.bfloat16),
        in_specs=[SMEM, SMEM, VMEM, VMEM],
        out_specs=VMEM,
        compiler_params=small(8),
        cost_estimate=pl.CostEstimate(
            flops=HEADS * ROWS * DH * 64, bytes_accessed=HEADS * ROWS * DH * 6, transcendentals=0
        ),
        name="prepare",
    )(place, table, own, student)


def fill_received(place, table, received, rows):
    head = place[0, 0]
    rank = jnp.int32(0)
    for p in range(PAIRS):
        mine = lax.div(table[head * STUDENTS + p // 2, p % 2], PAIRS) == head

        @pl.when(jnp.logical_not(mine))
        def _():
            rows[p] = scaled(received[rank])

        rank = rank + 1 - mine.astype(jnp.int32)


def attend_kernel(first, last, counts, blocks, place, table, plan, *refs):
    refs = list(refs)
    take = lambda n: [refs.pop(0) for _ in range(n)]
    groups = take(len(counts))
    if first:
        pieces = take(len(PIECES) + 1)
        take(1)
        state, rows = take(2)
    else:
        rows, before = take(2)
        if last:
            out, sums = take(2)
        else:
            (state,) = take(1)
    (keys,) = take(1)
    if first:
        (received,) = take(1)
    if last:
        (state,) = take(1)
    (sems,) = refs
    head, z_hi, x = place[0, 0], place[0, 1], place[0, 2]
    row_block = z_hi * 4 + x

    copies, arrivals = [], []
    at = 0
    for g, n in enumerate(counts):
        copies.append(pltpu.make_async_copy(groups[g], keys.at[pl.ds(at, n)], sems.at[g]))
        arrivals.append((at // CHUNK, copies[-1]))
        at += n
    if first:
        inputs = []
        rank = 0
        for n, piece in enumerate(pieces):
            length = piece.shape[0]
            inputs.append(
                pltpu.make_async_copy(
                    piece, received.at[pl.ds(rank, length)], sems.at[len(counts) + n]
                )
            )
            rank += length
        for c in inputs:
            c.start()
    for c in copies:
        c.start()
    if first:
        for part, value in ((0, MASKED), (TL, 0.0), (TC, 0.0)):
            state[part : part + PAIRS] = jnp.full((PAIRS, SUB, ROWS), value, jnp.float32)
        for part, value in ((SM, MASKED), (SL, 0.0)):
            state[part : part + STUDENTS] = jnp.full((STUDENTS, SUB, ROWS), value, jnp.float32)
        for c in inputs:
            c.wait()
        fill_received(place, table, received, rows)
    else:
        state[...] = before[...]

    def product(k, p):
        return lax.dot_general(
            jnp.concatenate([k, k], axis=1),
            rows[p],
            (((1,), (1,)), ((), ())),
            preferred_element_type=jnp.float32,
        )

    def update(logits, mask, m_index, l_index):
        if mask is not None:
            logits = jnp.where(mask, logits, MASKED)
        folded = logits.reshape(ROWS // SUB, SUB, ROWS)
        old = state[m_index]
        new = jnp.maximum(old, jnp.max(folded, axis=0))
        weights = jnp.exp2(folded - new[None])
        rescale = jnp.exp2(old - new)
        state[m_index] = new
        state[l_index] = state[l_index] * rescale + jnp.sum(weights, axis=0)
        return weights, rescale

    def block(own_at, other_at, masked):
        mask = None
        if masked:
            key_pos = lax.broadcasted_iota(jnp.int32, (ROWS, ROWS), 0)
            row_pos = lax.broadcasted_iota(jnp.int32, (ROWS, ROWS), 1)
            mask = key_pos <= row_pos
        student_keys = keys[own_at + 2]
        for s in range(STUDENTS):
            zs = product(student_keys, PAIRS + s)
            update(zs, mask, SM + s, SL + s)
            for c in range(2):
                p = 2 * s + c
                kv_head = lax.div(table[head * STUDENTS + s, c], GROUP)
                base = jnp.where(lax.div(kv_head, 2) == head, own_at, other_at)
                zt = product(keys[base + lax.rem(kv_head, 2)], p)
                weights, rescale = update(zt, mask, p, TL + p)
                gap = (zt - zs).reshape(ROWS // SUB, SUB, ROWS)
                state[TC + p] = state[TC + p] * rescale + jnp.sum(weights * gap, axis=0)

    def step(i, carry):
        for at_block, c in arrivals:

            @pl.when(i == at_block)
            def _():
                c.wait()

        chunk = lax.bitwise_and(z_hi - plan[0, i], 3)
        position = chunk * 4 + lax.bitwise_and(x + plan[1, i], 3)

        @pl.when(position < row_block)
        def _():
            block(CHUNK * i, CHUNK * i + OWN, False)

        if first:

            @pl.when(position == row_block)
            def _():
                block(CHUNK * i, CHUNK * i + OWN, True)

        return carry

    lax.fori_loop(0, blocks, step, 0)

    if not last:
        return

    def merged(m8, l8):
        top = jnp.max(m8, axis=0, keepdims=True)
        factor = jnp.exp2(m8 - top)
        total = jnp.sum(l8 * factor, axis=0, keepdims=True)
        return factor, total, LN2 * top + jnp.log(total)

    lane = lax.broadcasted_iota(jnp.int32, (1, LANE), 1)
    line = jnp.zeros((1, LANE), jnp.float32)
    for s in range(STUDENTS):
        _, _, s_lse = merged(state[SM + s], state[SL + s])
        value = 2.0 * s_lse
        for c in range(2):
            p = 2 * s + c
            factor, total, t_lse = merged(state[p], state[TL + p])
            cross = jnp.sum(state[TC + p] * factor, axis=0, keepdims=True)
            value = value + (LN2 * cross / total - t_lse)
        out[s : s + 1, :] = value
        line = jnp.where(lane == s, jnp.sum(value, axis=1, keepdims=True), line)
    sums[...] = jnp.broadcast_to(line, sums.shape)


def attend(place, table, plan, groups, rows, queries=None, state=None, copies_out=0):
    first = queries is not None
    last = copies_out > 0
    counts = tuple(g.shape[0] for g in groups)
    blocks = plan.shape[1]
    state_shape = jax.ShapeDtypeStruct((STATE, SUB, ROWS), jnp.float32)
    rows_shape = jax.ShapeDtypeStruct((HEADS, ROWS, 2 * DH), jnp.bfloat16)
    if first:
        extra, out_shape = [*queries, rows], (state_shape, rows_shape)
    elif last:
        extra = [rows, state]
        out_shape = (
            jax.ShapeDtypeStruct((STUDENTS, ROWS), jnp.float32),
            jax.ShapeDtypeStruct((copies_out, LANE), jnp.float32),
        )
    else:
        extra, out_shape = [rows, state], state_shape
    extra_specs = [ANY] * (len(PIECES) + 1) + [VMEM] if first else [VMEM, VMEM]
    scratch = [pltpu.VMEM((sum(counts), ROWS, DH), jnp.bfloat16)]
    if first:
        scratch.append(pltpu.VMEM((PAIRS, ROWS, DH), jnp.bfloat16))
    if last:
        scratch.append(pltpu.VMEM(state_shape.shape, jnp.float32))
    scratch.append(pltpu.SemaphoreType.DMA((len(groups) + len(PIECES) + 1,)))
    return pl.pallas_call(
        functools.partial(attend_kernel, first, last, counts, blocks),
        out_shape=out_shape,
        in_specs=[SMEM] * 3 + [ANY] * len(groups) + extra_specs,
        out_specs=jax.tree.map(lambda _: VMEM, out_shape),
        scratch_shapes=scratch,
        input_output_aliases={3 + len(groups) + len(extra) - 1: 1} if first else {},
        compiler_params=small(24),
        cost_estimate=pl.CostEstimate(
            flops=blocks * HEADS * 2 * ROWS * ROWS * 2 * DH,
            bytes_accessed=blocks * ROWS * CHUNK * DH * 2,
            transcendentals=blocks * HEADS * ROWS * ROWS,
        ),
        name="attend",
    )(place, table, plan, *groups, *extra)


def shift(n, by):
    return [(i, (i + by) % n) for i in range(n)]


def z_place(ring):
    ring %= 8
    return (ring % 2) * 4 + ring // 2


def z_shift(by):
    return [(z_place(i), z_place(i + by)) for i in range(8)]


def plan_of(blocks):
    return jnp.array([list(row) for row in zip(*blocks)], jnp.int32)


def program(teacher_query, teacher_key, student_query, student_key, pair_table):
    head = lax.axis_index("head")
    place = jnp.stack([head, lax.axis_index("kv_0"), lax.axis_index("kv_1")])[None]

    along_x = lambda a, by: lax.ppermute(a, "kv_1", shift(4, by))
    along_z = lambda a, by: lax.ppermute(a, ("head", "kv_0"), z_shift(by))
    other_side = [(0, 1), (1, 0)]

    ring = {0: split_heads(teacher_key[0], student_key[0])}
    chosen, count = queries_for_other(place, pair_table, teacher_query[0])
    ring[1] = along_z(ring[0], 1)
    ring[7] = along_z(ring[0], -1)
    pieces, rank = [], 0
    for length in PIECES:
        piece = chosen[rank : rank + length]
        pieces.append(lax.ppermute(piece, "head", other_side))
        rank += length
    more = lax.cond(
        count[0, 0] > SENT,
        lambda q: lax.ppermute(q, "head", other_side),
        lambda q: q,
        chosen[SENT:],
    )
    more, ring[1], ring[7] = lax.optimization_barrier((more, ring[1], ring[7]))
    rows = prepare(place, pair_table, teacher_query[0], student_query[0])
    mine = own_chunk(place, ring[0], ring[1], ring[7])
    near_a = along_x(mine, 1)
    near_b = along_x(mine, -1)
    near_c = along_x(near_a[:OTHER], 1)
    near_d = along_x(near_b[OTHER:], -1)
    for step in range(2, 5):
        ring[step] = along_z(ring[step - 1], 1)
        if step < 4:
            ring[8 - step] = along_z(ring[9 - step], -1)

    rest_13 = rest_of(place, ring, (1, 3))
    left_13 = along_x(rest_13, 1)
    right_13 = along_x(rest_13, -1)
    rest_2 = rest_of(place, ring, (2,))
    left_2 = along_x(rest_2, 1)
    right_2 = along_x(rest_2, -1)
    state, rows = attend(
        place,
        pair_table,
        plan_of([(0, 0), (0, -1), (0, 1), (0, 2), (1, 0), (3, 0), (2, 0)]),
        [mine, near_a, near_b, near_c, near_d, rest_13, rest_2],
        rows,
        queries=(*pieces, more),
    )
    left_13, right_13, left_2, right_2, state = lax.optimization_barrier(
        (left_13, right_13, left_2, right_2, state)
    )
    far_1 = along_x(left_13[:CHUNK], 1)
    far_3 = along_x(right_13[CHUNK:], -1)
    far_2 = along_x(left_2, 1)
    state = attend(
        place,
        pair_table,
        plan_of([(1, -1), (3, -1), (1, 1), (3, 1), (2, -1), (2, 1)]),
        [left_13, right_13, left_2, right_2],
        rows,
        state=state,
    )
    everyone = ("dp_0", "dp_1", "kv_0", "kv_1")
    devices = lax.axis_size(everyone)
    kl, sums = attend(
        place,
        pair_table,
        plan_of([(1, 2), (3, 2), (2, 2)]),
        [far_1, far_3, far_2],
        rows,
        state=state,
        copies_out=devices,
    )
    terms = lax.all_to_all(sums, everyone, 0, 0, tiled=True)
    head_loss = jnp.sum(terms, axis=0)[:STUDENTS] / (devices * ROWS)
    return (kl[None], head_loss)


def solution(mesh):
    split = Mesh(
        mesh.devices.reshape(4, 2, mesh.shape["head"], 4, 4),
        ("dp_0", "dp_1", "head", "kv_0", "kv_1"),
    )
    in_specs = (P(DP, KV, "head"), P(DP, KV, "head"), P(DP, KV, "head"), P(DP, KV, "head"), P())
    out_specs = (P(DP, "head", KV), P("head"))
    return jax.shard_map(
        program, mesh=split, in_specs=in_specs, out_specs=out_specs, check_vma=False
    )
```

```python
import functools
import math

import jax
import jax.numpy as jnp
from jax import lax
from jax.experimental import pallas as pl
from jax.experimental.pallas import tpu as pltpu
from jax.sharding import Mesh
from jax.sharding import PartitionSpec as P


HT = 28
KVT = 4
DH = 128
ROWS = 256
PAIRS = 14
STUDENTS = 7
HEADS = PAIRS + STUDENTS
GROUP = HT // KVT
KV = ("kv_0", "kv_1")
DP = ("dp_0", "dp_1")
LANE = 128
SUB = 8
MASKED = -1e30
LARGE = 2.0**100
LN2 = math.log(2.0)
KAPPA = 1.0 / (LN2 * math.sqrt(DH))
STATE = 3 * PAIRS + 2 * STUDENTS
TL, TC, SM, SL = PAIRS, 2 * PAIRS, 3 * PAIRS, 3 * PAIRS + STUDENTS
OWN = 3
OTHER = 2
CHUNK = OWN + OTHER
PIECES = (2, 2, 2, 3)
SENT = sum(PIECES)
MIB = 1024 * 1024
SMEM = pl.BlockSpec(memory_space=pltpu.SMEM)
VMEM = pl.BlockSpec(memory_space=pltpu.VMEM)
ANY = pl.BlockSpec(memory_space=pl.ANY)
HBM = pl.BlockSpec(memory_space=pltpu.HBM)


def heads_of(n):
    return jax.ShapeDtypeStruct((n, ROWS, DH), jnp.bfloat16)


def small(limit):
    return pltpu.CompilerParams(vmem_limit_bytes=limit * MIB)


def run_all(copies):
    for c in copies:
        c.start()
    for c in copies:
        c.wait()


def split_kernel(teacher, student, out, sems):
    run_all(
        [
            pltpu.make_async_copy(teacher.at[:, pl.ds(0, DH)], out.at[0], sems.at[0]),
            pltpu.make_async_copy(teacher.at[:, pl.ds(DH, DH)], out.at[1], sems.at[1]),
            pltpu.make_async_copy(student, out.at[2], sems.at[2]),
        ]
    )


def split_heads(teacher, student):
    return pl.pallas_call(
        split_kernel,
        out_shape=heads_of(OWN),
        in_specs=[HBM, HBM],
        out_specs=VMEM,
        scratch_shapes=[pltpu.SemaphoreType.DMA((3,))],
        compiler_params=small(2),
        name="split_heads",
    )(teacher, student)


def queries_kernel(place, table, query, sent, count, sems):
    head = place[0, 0]
    theirs = (1 - head) * STUDENTS

    def each(act):
        rank = jnp.int32(0)
        for p in range(PAIRS):
            teacher = table[theirs + p // 2, p % 2]
            mine = lax.div(teacher, PAIRS) == head
            lanes = pl.ds(pl.multiple_of(lax.rem(teacher, PAIRS) * DH, DH), DH)

            @pl.when(mine)
            def _():
                act(pltpu.make_async_copy(query.at[:, lanes], sent.at[rank], sems.at[p]))

            rank = rank + mine.astype(jnp.int32)
        return rank

    count[0, 0] = each(lambda c: c.start())
    each(lambda c: c.wait())


def queries_for_other(place, table, query):
    return pl.pallas_call(
        queries_kernel,
        out_shape=(heads_of(PAIRS), jax.ShapeDtypeStruct((1, 1), jnp.int32)),
        in_specs=[SMEM, SMEM, ANY],
        out_specs=(VMEM, SMEM),
        scratch_shapes=[pltpu.SemaphoreType.DMA((PAIRS,))],
        compiler_params=small(4),
        name="queries_for_other",
    )(place, table, query)


def own_chunk_kernel(place, own, ring_1, ring_7, out, sems):
    for head, pair in enumerate((ring_7, ring_1)):

        @pl.when(place[0, 0] == head)
        def _():
            run_all(
                [
                    pltpu.make_async_copy(own, out.at[pl.ds(0, OWN)], sems.at[0]),
                    pltpu.make_async_copy(
                        pair.at[pl.ds(0, OTHER)], out.at[pl.ds(OWN, OTHER)], sems.at[1]
                    ),
                ]
            )


def own_chunk(place, own, ring_1, ring_7):
    return pl.pallas_call(
        own_chunk_kernel,
        out_shape=heads_of(CHUNK),
        in_specs=[SMEM, ANY, ANY, ANY],
        out_specs=VMEM,
        scratch_shapes=[pltpu.SemaphoreType.DMA((2,))],
        compiler_params=small(2),
        name="own_chunk",
    )(place, own, ring_1, ring_7)


def rest_kernel(chunks, place, *refs):
    ring, out, sems = refs[:-2], refs[-2], refs[-1]
    for head in range(2):

        @pl.when(place[0, 0] == head)
        def _():
            copies = []
            for n in range(chunks):
                own, other = ring[3 * n], ring[3 * n + 1 + head]
                copies.append(
                    pltpu.make_async_copy(own, out.at[pl.ds(CHUNK * n, OWN)], sems.at[n, 0])
                )
                copies.append(
                    pltpu.make_async_copy(
                        other.at[pl.ds(0, OTHER)],
                        out.at[pl.ds(CHUNK * n + OWN, OTHER)],
                        sems.at[n, 1],
                    )
                )
            run_all(copies)


def rest_of(place, ring, chunks):
    parts = [ring[o] for m in chunks for o in (2 * m, 2 * m - 1, (2 * m + 1) % 8)]
    return pl.pallas_call(
        functools.partial(rest_kernel, len(chunks)),
        out_shape=heads_of(CHUNK * len(chunks)),
        in_specs=[SMEM] + [ANY] * len(parts),
        out_specs=VMEM,
        scratch_shapes=[pltpu.SemaphoreType.DMA((len(chunks), 2))],
        compiler_params=small(4),
        name="rest_of",
    )(place, *parts)


def scaled(q):
    q = q.astype(jnp.float32) * KAPPA
    high = q.astype(jnp.bfloat16)
    low = (q - high.astype(jnp.float32)).astype(jnp.bfloat16)
    return jnp.concatenate([high, low], axis=1)


def prepare_kernel(place, table, own, student, rows):
    head = place[0, 0]
    for s in range(STUDENTS):
        rows[PAIRS + s] = scaled(student[:, s * DH : (s + 1) * DH])
    for p in range(PAIRS):
        teacher = table[head * STUDENTS + p // 2, p % 2]
        lanes = pl.ds(pl.multiple_of(lax.rem(teacher, PAIRS) * DH, DH), DH)

        @pl.when(lax.div(teacher, PAIRS) == head)
        def _():
            rows[p] = scaled(own[:, lanes])


def prepare(place, table, own, student):
    return pl.pallas_call(
        prepare_kernel,
        out_shape=jax.ShapeDtypeStruct((HEADS, ROWS, 2 * DH), jnp.bfloat16),
        in_specs=[SMEM, SMEM, VMEM, VMEM],
        out_specs=VMEM,
        compiler_params=small(8),
        cost_estimate=pl.CostEstimate(
            flops=HEADS * ROWS * DH * 64, bytes_accessed=HEADS * ROWS * DH * 6, transcendentals=0
        ),
        name="prepare",
    )(place, table, own, student)


def fill_received(place, table, received, rows):
    head = place[0, 0]
    rank = jnp.int32(0)
    for p in range(PAIRS):
        mine = lax.div(table[head * STUDENTS + p // 2, p % 2], PAIRS) == head

        @pl.when(jnp.logical_not(mine))
        def _():
            rows[p] = scaled(received[rank])

        rank = rank + 1 - mine.astype(jnp.int32)


def attend_kernel(first, last, counts, blocks, place, table, plan, *refs):
    refs = list(refs)
    take = lambda n: [refs.pop(0) for _ in range(n)]
    groups = take(len(counts))
    if first:
        pieces = take(len(PIECES) + 1)
        take(1)
        state, rows = take(2)
    else:
        rows, before = take(2)
        if last:
            out, sums = take(2)
        else:
            (state,) = take(1)
    (keys,) = take(1)
    if first:
        received, entry = take(2)
    if last:
        (state,) = take(1)
    offsets, sems = refs
    head, z_hi, x = place[0, 0], place[0, 1], place[0, 2]
    row_block = z_hi * 4 + x

    copies, arrivals = [], []
    at = 0
    for g, n in enumerate(counts):
        copies.append(pltpu.make_async_copy(groups[g], keys.at[pl.ds(at, n)], sems.at[g]))
        arrivals.append((at // CHUNK, copies[-1]))
        at += n
    if first:
        inputs = []
        rank = 0
        for n, piece in enumerate(pieces):
            length = piece.shape[0]
            inputs.append(
                pltpu.make_async_copy(
                    piece, received.at[pl.ds(rank, length)], sems.at[len(counts) + n]
                )
            )
            rank += length
        for c in inputs:
            c.start()
    for c in copies:
        c.start()
    if first:
        for c in inputs:
            c.wait()
        fill_received(place, table, received, rows)
    else:
        entry = before
        state[...] = before[...]

    for p in range(PAIRS):
        kv_head = lax.div(table[head * STUDENTS + p // 2, p % 2], GROUP)
        side = jnp.where(lax.div(kv_head, 2) == head, 0, OWN)
        offsets[p] = side + lax.rem(kv_head, 2)

    def product(k, p):
        return lax.dot_general(
            jnp.concatenate([k, k], axis=1),
            rows[p],
            (((1,), (1,)), ((), ())),
            preferred_element_type=jnp.float32,
        )

    def folded(a):
        return a.reshape(ROWS // SUB, SUB, ROWS)

    def own_block():
        key_pos = lax.broadcasted_iota(jnp.int32, (ROWS, ROWS), 0)
        row_pos = lax.broadcasted_iota(jnp.int32, (ROWS, ROWS), 1)
        mask = key_pos <= row_pos

        def begin(logits, m_index, l_index):
            logits = jnp.where(mask, logits, MASKED)
            top = jnp.max(logits, axis=0, keepdims=True)
            weights = folded(jnp.exp2(logits - top))
            state[m_index] = jnp.broadcast_to(top, (SUB, ROWS))
            state[l_index] = jnp.sum(weights, axis=0)
            return weights

        for s in range(STUDENTS):
            zs = product(keys[2], PAIRS + s)
            begin(zs, SM + s, SL + s)
            for c in range(2):
                p = 2 * s + c
                zt = product(keys[offsets[p]], p)
                weights = begin(zt, p, TL + p)
                state[TC + p] = jnp.sum(weights * folded(zt - zs), axis=0)

    def block(base):
        def add(logits, m_index, l_index):
            weights = jnp.exp2(folded(logits) - state[m_index][None])
            state[l_index] = state[l_index] + jnp.sum(weights, axis=0)
            return weights

        student_keys = keys[base + 2]
        for s in range(STUDENTS):
            zs = product(student_keys, PAIRS + s)
            add(zs, SM + s, SL + s)
            for c in range(2):
                p = 2 * s + c
                zt = product(keys[base + offsets[p]], p)
                weights = add(zt, p, TL + p)
                state[TC + p] = state[TC + p] + jnp.sum(weights * folded(zt - zs), axis=0)

    def exact_block(base):
        def add(logits, m_index, l_index):
            logits = folded(logits)
            old = state[m_index]
            new = jnp.maximum(old, jnp.max(logits, axis=0))
            weights = jnp.exp2(logits - new[None])
            rescale = jnp.exp2(old - new)
            state[m_index] = new
            state[l_index] = state[l_index] * rescale + jnp.sum(weights, axis=0)
            return weights, rescale

        def student(s, carry):
            zs = product(keys[base + 2], PAIRS + s)
            add(zs, SM + s, SL + s)
            for c in range(2):
                p = 2 * s + c
                zt = product(keys[base + offsets[p]], p)
                weights, rescale = add(zt, p, TL + p)
                cross = jnp.sum(weights * folded(zt - zs), axis=0)
                state[TC + p] = state[TC + p] * rescale + cross
            return carry

        lax.fori_loop(0, STUDENTS, student, 0)

    def visible(i):
        chunk = lax.bitwise_and(z_hi - plan[0, i], 3)
        return chunk * 4 + lax.bitwise_and(x + plan[1, i], 3) < row_block

    def step(i, carry):
        for at_block, c in arrivals:

            @pl.when(i == at_block)
            def _():
                c.wait()

        @pl.when(visible(i))
        def _():
            block(CHUNK * i)

        return carry

    def exact_step(i, carry):
        @pl.when(visible(i))
        def _():
            exact_block(CHUNK * i)

        return carry

    if first:
        arrivals[0][1].wait()
        arrivals = arrivals[1:]
        own_block()
        entry[...] = state[...]
    lax.fori_loop(int(first), blocks, step, 0)

    largest = jnp.maximum(
        jnp.max(state[TL : TL + PAIRS]), jnp.max(state[SL : SL + STUDENTS])
    )

    @pl.when(largest > LARGE)
    def _():
        state[...] = entry[...]
        lax.fori_loop(int(first), blocks, exact_step, 0)

    if not last:
        return

    def merged(m8, l8):
        top = jnp.max(m8, axis=0, keepdims=True)
        factor = jnp.exp2(m8 - top)
        total = jnp.sum(l8 * factor, axis=0, keepdims=True)
        return factor, total, LN2 * top + jnp.log(total)

    lane = lax.broadcasted_iota(jnp.int32, (1, LANE), 1)
    line = jnp.zeros((1, LANE), jnp.float32)
    for s in range(STUDENTS):
        _, _, s_lse = merged(state[SM + s], state[SL + s])
        value = 2.0 * s_lse
        for c in range(2):
            p = 2 * s + c
            factor, total, t_lse = merged(state[p], state[TL + p])
            cross = jnp.sum(state[TC + p] * factor, axis=0, keepdims=True)
            value = value + (LN2 * cross / total - t_lse)
        out[s : s + 1, :] = value
        line = jnp.where(lane == s, jnp.sum(value, axis=1, keepdims=True), line)
    sums[...] = jnp.broadcast_to(line, sums.shape)


def attend(place, table, plan, groups, rows, queries=None, state=None, copies_out=0):
    first = queries is not None
    last = copies_out > 0
    counts = tuple(g.shape[0] for g in groups)
    blocks = plan.shape[1]
    state_shape = jax.ShapeDtypeStruct((STATE, SUB, ROWS), jnp.float32)
    rows_shape = jax.ShapeDtypeStruct((HEADS, ROWS, 2 * DH), jnp.bfloat16)
    if first:
        extra, out_shape = [*queries, rows], (state_shape, rows_shape)
    elif last:
        extra = [rows, state]
        out_shape = (
            jax.ShapeDtypeStruct((STUDENTS, ROWS), jnp.float32),
            jax.ShapeDtypeStruct((copies_out, LANE), jnp.float32),
        )
    else:
        extra, out_shape = [rows, state], state_shape
    extra_specs = [ANY] * (len(PIECES) + 1) + [VMEM] if first else [VMEM, VMEM]
    scratch = [pltpu.VMEM((sum(counts), ROWS, DH), jnp.bfloat16)]
    if first:
        scratch.append(pltpu.VMEM((PAIRS, ROWS, DH), jnp.bfloat16))
        scratch.append(pltpu.VMEM(state_shape.shape, jnp.float32))
    if last:
        scratch.append(pltpu.VMEM(state_shape.shape, jnp.float32))
    scratch.append(pltpu.SMEM((PAIRS,), jnp.int32))
    scratch.append(pltpu.SemaphoreType.DMA((len(groups) + len(PIECES) + 1,)))
    return pl.pallas_call(
        functools.partial(attend_kernel, first, last, counts, blocks),
        out_shape=out_shape,
        in_specs=[SMEM] * 3 + [ANY] * len(groups) + extra_specs,
        out_specs=jax.tree.map(lambda _: VMEM, out_shape),
        scratch_shapes=scratch,
        input_output_aliases={3 + len(groups) + len(extra) - 1: 1} if first else {},
        compiler_params=small(24),
        cost_estimate=pl.CostEstimate(
            flops=blocks * HEADS * 2 * ROWS * ROWS * 2 * DH,
            bytes_accessed=blocks * ROWS * CHUNK * DH * 2,
            transcendentals=blocks * HEADS * ROWS * ROWS,
        ),
        name="attend",
    )(place, table, plan, *groups, *extra)


def shift(n, by):
    return [(i, (i + by) % n) for i in range(n)]


def z_place(ring):
    ring %= 8
    return (ring % 2) * 4 + ring // 2


def z_shift(by):
    return [(z_place(i), z_place(i + by)) for i in range(8)]


def plan_of(blocks):
    return jnp.array([list(row) for row in zip(*blocks)], jnp.int32)


def program(teacher_query, teacher_key, student_query, student_key, pair_table):
    head = lax.axis_index("head")
    place = jnp.stack([head, lax.axis_index("kv_0"), lax.axis_index("kv_1")])[None]

    along_x = lambda a, by: lax.ppermute(a, "kv_1", shift(4, by))
    along_z = lambda a, by: lax.ppermute(a, ("head", "kv_0"), z_shift(by))
    other_side = [(0, 1), (1, 0)]

    ring = {0: split_heads(teacher_key[0], student_key[0])}
    chosen, count = queries_for_other(place, pair_table, teacher_query[0])
    ring[1] = along_z(ring[0], 1)
    ring[7] = along_z(ring[0], -1)
    pieces, rank = [], 0
    for length in PIECES:
        piece = chosen[rank : rank + length]
        pieces.append(lax.ppermute(piece, "head", other_side))
        rank += length
    more = lax.cond(
        count[0, 0] > SENT,
        lambda q: lax.ppermute(q, "head", other_side),
        lambda q: q,
        chosen[SENT:],
    )
    more, ring[1], ring[7] = lax.optimization_barrier((more, ring[1], ring[7]))
    rows = prepare(place, pair_table, teacher_query[0], student_query[0])
    mine = own_chunk(place, ring[0], ring[1], ring[7])
    near_a = along_x(mine, 1)
    near_b = along_x(mine, -1)
    near_c = along_x(near_a[:OTHER], 1)
    near_d = along_x(near_b[OTHER:], -1)
    for step in range(2, 5):
        ring[step] = along_z(ring[step - 1], 1)
        if step < 4:
            ring[8 - step] = along_z(ring[9 - step], -1)

    rest_13 = rest_of(place, ring, (1, 3))
    left_13 = along_x(rest_13, 1)
    right_13 = along_x(rest_13, -1)
    rest_2 = rest_of(place, ring, (2,))
    left_2 = along_x(rest_2, 1)
    right_2 = along_x(rest_2, -1)
    state, rows = attend(
        place,
        pair_table,
        plan_of([(0, 0), (0, -1), (0, 1), (0, 2), (1, 0), (3, 0), (2, 0)]),
        [mine, near_a, near_b, near_c, near_d, rest_13, rest_2],
        rows,
        queries=(*pieces, more),
    )
    left_13, right_13, left_2, right_2, state = lax.optimization_barrier(
        (left_13, right_13, left_2, right_2, state)
    )
    far_1 = along_x(left_13[:CHUNK], 1)
    far_3 = along_x(right_13[CHUNK:], -1)
    far_2 = along_x(left_2, 1)
    state = attend(
        place,
        pair_table,
        plan_of([(1, -1), (3, -1), (1, 1), (3, 1), (2, -1), (2, 1)]),
        [left_13, right_13, left_2, right_2],
        rows,
        state=state,
    )
    everyone = ("dp_0", "dp_1", "kv_0", "kv_1")
    devices = lax.axis_size(everyone)
    kl, sums = attend(
        place,
        pair_table,
        plan_of([(1, 2), (3, 2), (2, 2)]),
        [far_1, far_3, far_2],
        rows,
        state=state,
        copies_out=devices,
    )
    terms = lax.all_to_all(sums, everyone, 0, 0, tiled=True)
    head_loss = jnp.sum(terms, axis=0)[:STUDENTS] / (devices * ROWS)
    return (kl[None], head_loss)


def solution(mesh):
    split = Mesh(
        mesh.devices.reshape(4, 2, mesh.shape["head"], 4, 4),
        ("dp_0", "dp_1", "head", "kv_0", "kv_1"),
    )
    in_specs = (P(DP, KV, "head"), P(DP, KV, "head"), P(DP, KV, "head"), P(DP, KV, "head"), P())
    out_specs = (P(DP, "head", KV), P("head"))
    return jax.shard_map(
        program, mesh=split, in_specs=in_specs, out_specs=out_specs, check_vma=False
    )
```

```python
import functools
import math

import jax
import jax.numpy as jnp
from jax import lax
from jax.experimental import pallas as pl
from jax.experimental.pallas import tpu as pltpu
from jax.sharding import Mesh
from jax.sharding import PartitionSpec as P


HT = 28
KVT = 4
DH = 128
ROWS = 256
PAIRS = 14
STUDENTS = 7
HEADS = PAIRS + STUDENTS
GROUP = HT // KVT
KV = ("kv_0", "kv_1")
DP = ("dp_0", "dp_1")
LANE = 128
SUB = 8
MASKED = -1e30
LARGE = 2.0**100
LN2 = math.log(2.0)
KAPPA = 1.0 / (LN2 * math.sqrt(DH))
STATE = 3 * PAIRS + 2 * STUDENTS
TL, TC, SM, SL = PAIRS, 2 * PAIRS, 3 * PAIRS, 3 * PAIRS + STUDENTS
OWN = 3
OTHER = 2
CHUNK = OWN + OTHER
PIECES = (3, 3, 3)
SENT = sum(PIECES)
MIB = 1024 * 1024
SMEM = pl.BlockSpec(memory_space=pltpu.SMEM)
VMEM = pl.BlockSpec(memory_space=pltpu.VMEM)
ANY = pl.BlockSpec(memory_space=pl.ANY)
HBM = pl.BlockSpec(memory_space=pltpu.HBM)


def heads_of(n):
    return jax.ShapeDtypeStruct((n, ROWS, DH), jnp.bfloat16)


def small(limit):
    return pltpu.CompilerParams(vmem_limit_bytes=limit * MIB)


def run_all(copies):
    for c in copies:
        c.start()
    for c in copies:
        c.wait()


def split_kernel(teacher, student, out, sems):
    run_all(
        [
            pltpu.make_async_copy(teacher.at[:, pl.ds(0, DH)], out.at[0], sems.at[0]),
            pltpu.make_async_copy(teacher.at[:, pl.ds(DH, DH)], out.at[1], sems.at[1]),
            pltpu.make_async_copy(student, out.at[2], sems.at[2]),
        ]
    )


def split_heads(teacher, student):
    return pl.pallas_call(
        split_kernel,
        out_shape=heads_of(OWN),
        in_specs=[HBM, HBM],
        out_specs=VMEM,
        scratch_shapes=[pltpu.SemaphoreType.DMA((3,))],
        compiler_params=small(2),
        name="split_heads",
    )(teacher, student)


def queries_kernel(place, table, query, *refs):
    pieces, (count, sent, sems) = refs[:-3], refs[-3:]
    head = place[0, 0]
    theirs = (1 - head) * STUDENTS

    def each(act):
        rank = jnp.int32(0)
        for p in range(PAIRS):
            teacher = table[p % 2, theirs + p // 2]
            mine = lax.div(teacher, PAIRS) == head
            lanes = pl.ds(pl.multiple_of(lax.rem(teacher, PAIRS) * DH, DH), DH)

            @pl.when(mine)
            def _():
                act(pltpu.make_async_copy(query.at[:, lanes], sent.at[rank], sems.at[p]))

            rank = rank + mine.astype(jnp.int32)
        return rank

    count[0, 0] = each(lambda c: c.start())
    each(lambda c: c.wait())
    rank = 0
    for piece in pieces:
        piece[...] = sent[rank : rank + piece.shape[0]]
        rank += piece.shape[0]


def queries_for_other(place, table, query):
    return pl.pallas_call(
        queries_kernel,
        out_shape=(
            *(heads_of(n) for n in (*PIECES, PAIRS - SENT)),
            jax.ShapeDtypeStruct((1, 1), jnp.int32),
        ),
        in_specs=[SMEM, SMEM, ANY],
        out_specs=(*[VMEM] * (len(PIECES) + 1), SMEM),
        scratch_shapes=[
            pltpu.VMEM((PAIRS, ROWS, DH), jnp.bfloat16),
            pltpu.SemaphoreType.DMA((PAIRS,)),
        ],
        compiler_params=small(4),
        name="queries_for_other",
    )(place, table, query)


def chunks_kernel(place, *refs):
    ring, out = refs[:-1], refs[-1]
    for head in range(2):

        @pl.when(place[0, 0] == head)
        def _():
            for n in range(len(ring) // 3):
                own, other = ring[3 * n], ring[3 * n + 1 + head]
                out[CHUNK * n : CHUNK * n + OWN] = own[...]
                out[CHUNK * n + OWN : CHUNK * (n + 1)] = other[:OTHER]


def chunks_of(place, ring, chunks):
    parts = [ring[o % 8] for m in chunks for o in (2 * m, 2 * m - 1, 2 * m + 1)]
    return pl.pallas_call(
        chunks_kernel,
        out_shape=heads_of(CHUNK * len(chunks)),
        in_specs=[SMEM] + [VMEM] * len(parts),
        out_specs=VMEM,
        compiler_params=small(4),
        name="chunks_of",
    )(place, *parts)


def scaled(q):
    q = q.astype(jnp.float32) * KAPPA
    high = q.astype(jnp.bfloat16)
    low = (q - high.astype(jnp.float32)).astype(jnp.bfloat16)
    return jnp.concatenate([high, low], axis=1)


def prepare_kernel(place, table, own, student, rows):
    head = place[0, 0]
    for s in range(STUDENTS):
        rows[PAIRS + s] = scaled(student[:, s * DH : (s + 1) * DH])
    for p in range(PAIRS):
        teacher = table[p % 2, head * STUDENTS + p // 2]
        lanes = pl.ds(pl.multiple_of(lax.rem(teacher, PAIRS) * DH, DH), DH)

        @pl.when(lax.div(teacher, PAIRS) == head)
        def _():
            rows[p] = scaled(own[:, lanes])


def prepare(place, table, own, student):
    return pl.pallas_call(
        prepare_kernel,
        out_shape=jax.ShapeDtypeStruct((HEADS, ROWS, 2 * DH), jnp.bfloat16),
        in_specs=[SMEM, SMEM, VMEM, VMEM],
        out_specs=VMEM,
        compiler_params=small(8),
        cost_estimate=pl.CostEstimate(
            flops=HEADS * ROWS * DH * 64, bytes_accessed=HEADS * ROWS * DH * 6, transcendentals=0
        ),
        name="prepare",
    )(place, table, own, student)


def fill_received(place, table, received, rows):
    head = place[0, 0]
    rank = jnp.int32(0)
    for p in range(PAIRS):
        mine = lax.div(table[p % 2, head * STUDENTS + p // 2], PAIRS) == head

        @pl.when(jnp.logical_not(mine))
        def _():
            rows[p] = scaled(received[rank])

        rank = rank + 1 - mine.astype(jnp.int32)


def attend_kernel(first, last, counts, blocks, place, table, plan, *refs):
    refs = list(refs)
    take = lambda n: [refs.pop(0) for _ in range(n)]
    groups = take(len(counts))
    if first:
        pieces = take(len(PIECES) + 1)
        take(1)
        state, rows = take(2)
    else:
        rows, before = take(2)
        if last:
            out, sums = take(2)
        else:
            (state,) = take(1)
    (keys,) = take(1)
    if first:
        received, entry = take(2)
    if last:
        (state,) = take(1)
    offsets, sems = refs
    head, z_hi, x = place[0, 0], place[0, 1], place[0, 2]
    row_block = z_hi * 4 + x

    copies, arrivals = [], []
    at = 0
    for g, n in enumerate(counts):
        copies.append(pltpu.make_async_copy(groups[g], keys.at[pl.ds(at, n)], sems.at[g]))
        arrivals.append((at // CHUNK, copies[-1]))
        at += n
    if first:
        inputs = []
        rank = 0
        for n, piece in enumerate(pieces):
            length = piece.shape[0]
            inputs.append(
                pltpu.make_async_copy(
                    piece, received.at[pl.ds(rank, length)], sems.at[len(counts) + n]
                )
            )
            rank += length
        for c in inputs:
            c.start()
    for c in copies:
        c.start()
    if first:
        for c in inputs:
            c.wait()
        fill_received(place, table, received, rows)
    else:
        entry = before
        state[...] = before[...]

    for p in range(PAIRS):
        kv_head = lax.div(table[p % 2, head * STUDENTS + p // 2], GROUP)
        side = jnp.where(lax.div(kv_head, 2) == head, 0, OWN)
        offsets[p] = side + lax.rem(kv_head, 2)

    def product(k, p):
        return lax.dot_general(
            jnp.concatenate([k, k], axis=1),
            rows[p],
            (((1,), (1,)), ((), ())),
            preferred_element_type=jnp.float32,
        )

    def folded(a):
        return a.reshape(ROWS // SUB, SUB, ROWS)

    def own_block():
        key_pos = lax.broadcasted_iota(jnp.int32, (ROWS, ROWS), 0)
        row_pos = lax.broadcasted_iota(jnp.int32, (ROWS, ROWS), 1)
        mask = key_pos <= row_pos

        def begin(logits, m_index, l_index):
            logits = jnp.where(mask, logits, MASKED)
            top = jnp.max(logits, axis=0, keepdims=True)
            weights = folded(jnp.exp2(logits - top))
            state[m_index] = jnp.broadcast_to(top, (SUB, ROWS))
            state[l_index] = jnp.sum(weights, axis=0)
            return weights

        for s in range(STUDENTS):
            zs = product(keys[2], PAIRS + s)
            begin(zs, SM + s, SL + s)
            for c in range(2):
                p = 2 * s + c
                zt = product(keys[offsets[p]], p)
                weights = begin(zt, p, TL + p)
                state[TC + p] = jnp.sum(weights * folded(zt - zs), axis=0)

    def block(base):
        def add(logits, m_index, l_index):
            weights = jnp.exp2(folded(logits) - state[m_index][None])
            state[l_index] = state[l_index] + jnp.sum(weights, axis=0)
            return weights

        student_keys = keys[base + 2]
        for s in range(STUDENTS):
            zs = product(student_keys, PAIRS + s)
            add(zs, SM + s, SL + s)
            for c in range(2):
                p = 2 * s + c
                zt = product(keys[base + offsets[p]], p)
                weights = add(zt, p, TL + p)
                state[TC + p] = state[TC + p] + jnp.sum(weights * folded(zt - zs), axis=0)

    def exact_block(base):
        def add(logits, m_index, l_index):
            logits = folded(logits)
            old = state[m_index]
            new = jnp.maximum(old, jnp.max(logits, axis=0))
            weights = jnp.exp2(logits - new[None])
            rescale = jnp.exp2(old - new)
            state[m_index] = new
            state[l_index] = state[l_index] * rescale + jnp.sum(weights, axis=0)
            return weights, rescale

        def student(s, carry):
            zs = product(keys[base + 2], PAIRS + s)
            add(zs, SM + s, SL + s)
            for c in range(2):
                p = 2 * s + c
                zt = product(keys[base + offsets[p]], p)
                weights, rescale = add(zt, p, TL + p)
                cross = jnp.sum(weights * folded(zt - zs), axis=0)
                state[TC + p] = state[TC + p] * rescale + cross
            return carry

        lax.fori_loop(0, STUDENTS, student, 0)

    def visible(i):
        chunk = lax.bitwise_and(z_hi - plan[0, i], 3)
        return chunk * 4 + lax.bitwise_and(x + plan[1, i], 3) < row_block

    def step(i, carry):
        for at_block, c in arrivals:

            @pl.when(i == at_block)
            def _():
                c.wait()

        @pl.when(visible(i))
        def _():
            block(CHUNK * i)

        return carry

    def exact_step(i, carry):
        @pl.when(visible(i))
        def _():
            exact_block(CHUNK * i)

        return carry

    if first:
        arrivals[0][1].wait()
        arrivals = arrivals[1:]
        own_block()
        entry[...] = state[...]
    lax.fori_loop(int(first), blocks, step, 0)

    largest = jnp.maximum(
        jnp.max(state[TL : TL + PAIRS]), jnp.max(state[SL : SL + STUDENTS])
    )

    @pl.when(largest > LARGE)
    def _():
        state[...] = entry[...]
        lax.fori_loop(int(first), blocks, exact_step, 0)

    if not last:
        return

    def merged(m8, l8):
        top = jnp.max(m8, axis=0, keepdims=True)
        factor = jnp.exp2(m8 - top)
        total = jnp.sum(l8 * factor, axis=0, keepdims=True)
        return factor, total, LN2 * top + jnp.log(total)

    lane = lax.broadcasted_iota(jnp.int32, (1, LANE), 1)
    line = jnp.zeros((1, LANE), jnp.float32)
    for s in range(STUDENTS):
        _, _, s_lse = merged(state[SM + s], state[SL + s])
        value = 2.0 * s_lse
        for c in range(2):
            p = 2 * s + c
            factor, total, t_lse = merged(state[p], state[TL + p])
            cross = jnp.sum(state[TC + p] * factor, axis=0, keepdims=True)
            value = value + (LN2 * cross / total - t_lse)
        out[s : s + 1, :] = value
        line = jnp.where(lane == s, jnp.sum(value, axis=1, keepdims=True), line)
    sums[...] = jnp.broadcast_to(line, sums.shape)


def attend(place, table, plan, groups, rows, queries=None, state=None, copies_out=0):
    first = queries is not None
    last = copies_out > 0
    counts = tuple(g.shape[0] for g in groups)
    blocks = plan.shape[1]
    state_shape = jax.ShapeDtypeStruct((STATE, SUB, ROWS), jnp.float32)
    rows_shape = jax.ShapeDtypeStruct((HEADS, ROWS, 2 * DH), jnp.bfloat16)
    if first:
        extra, out_shape = [*queries, rows], (state_shape, rows_shape)
    elif last:
        extra = [rows, state]
        out_shape = (
            jax.ShapeDtypeStruct((STUDENTS, ROWS), jnp.float32),
            jax.ShapeDtypeStruct((copies_out, LANE), jnp.float32),
        )
    else:
        extra, out_shape = [rows, state], state_shape
    extra_specs = [ANY] * (len(PIECES) + 1) + [VMEM] if first else [VMEM, VMEM]
    scratch = [pltpu.VMEM((sum(counts), ROWS, DH), jnp.bfloat16)]
    if first:
        scratch.append(pltpu.VMEM((PAIRS, ROWS, DH), jnp.bfloat16))
        scratch.append(pltpu.VMEM(state_shape.shape, jnp.float32))
    if last:
        scratch.append(pltpu.VMEM(state_shape.shape, jnp.float32))
    scratch.append(pltpu.SMEM((PAIRS,), jnp.int32))
    scratch.append(pltpu.SemaphoreType.DMA((len(groups) + len(PIECES) + 1,)))
    return pl.pallas_call(
        functools.partial(attend_kernel, first, last, counts, blocks),
        out_shape=out_shape,
        in_specs=[SMEM] * 3 + [ANY] * len(groups) + extra_specs,
        out_specs=jax.tree.map(lambda _: VMEM, out_shape),
        scratch_shapes=scratch,
        input_output_aliases={3 + len(groups) + len(extra) - 1: 1} if first else {},
        compiler_params=small(24),
        cost_estimate=pl.CostEstimate(
            flops=blocks * HEADS * 2 * ROWS * ROWS * 2 * DH,
            bytes_accessed=blocks * ROWS * CHUNK * DH * 2,
            transcendentals=blocks * HEADS * ROWS * ROWS,
        ),
        name="attend",
    )(place, table, plan, *groups, *extra)


def shift(n, by):
    return [(i, (i + by) % n) for i in range(n)]


def z_place(ring):
    ring %= 8
    return (ring % 2) * 4 + ring // 2


def z_shift(by):
    return [(z_place(i), z_place(i + by)) for i in range(8)]


def plan_of(blocks):
    return jnp.array([list(row) for row in zip(*blocks)], jnp.int32)


def program(teacher_query, teacher_key, student_query, student_key, pair_table):
    head = lax.axis_index("head")
    table = pair_table.T
    place = jnp.stack([head, lax.axis_index("kv_0"), lax.axis_index("kv_1")])[None]

    along_x = lambda a, by: lax.ppermute(a, "kv_1", shift(4, by))
    along_z = lambda a, by: lax.ppermute(a, ("head", "kv_0"), z_shift(by))
    other_side = [(0, 1), (1, 0)]

    ring = {0: split_heads(teacher_key[0], student_key[0])}
    *chosen, count = queries_for_other(place, table, teacher_query[0])
    ring[1] = along_z(ring[0], 1)
    ring[7] = along_z(ring[0], -1)
    pieces = [lax.ppermute(piece, "head", other_side) for piece in chosen[:-1]]
    more = lax.cond(
        count[0, 0] > SENT,
        lambda q: lax.ppermute(q, "head", other_side),
        lambda q: q,
        chosen[-1],
    )
    more, ring[1], ring[7] = lax.optimization_barrier((more, ring[1], ring[7]))
    rows = prepare(place, table, teacher_query[0], student_query[0])
    mine = chunks_of(place, ring, (0,))
    near_a = along_x(mine, 1)
    near_b = along_x(mine, -1)
    near_c = along_x(near_a[:OTHER], 1)
    near_d = along_x(near_b[OTHER:], -1)
    for step in range(2, 5):
        ring[step] = along_z(ring[step - 1], 1)
        if step < 4:
            ring[8 - step] = along_z(ring[9 - step], -1)

    rest_13 = chunks_of(place, ring, (1, 3))
    left_13 = along_x(rest_13, 1)
    right_13 = along_x(rest_13, -1)
    rest_2 = chunks_of(place, ring, (2,))
    left_2 = along_x(rest_2, 1)
    right_2 = along_x(rest_2, -1)
    state, rows = attend(
        place,
        table,
        plan_of([(0, 0), (0, -1), (0, 1), (0, 2), (1, 0), (3, 0), (2, 0)]),
        [mine, near_a, near_b, near_c, near_d, rest_13, rest_2],
        rows,
        queries=(*pieces, more),
    )
    left_13, right_13, left_2, right_2, state = lax.optimization_barrier(
        (left_13, right_13, left_2, right_2, state)
    )
    far_1 = along_x(left_13[:CHUNK], 1)
    far_3 = along_x(right_13[CHUNK:], -1)
    far_2 = along_x(left_2, 1)
    state = attend(
        place,
        table,
        plan_of([(1, -1), (3, -1), (1, 1), (3, 1), (2, -1), (2, 1)]),
        [left_13, right_13, left_2, right_2],
        rows,
        state=state,
    )
    everyone = ("dp_0", "dp_1", "kv_0", "kv_1")
    devices = lax.axis_size(everyone)
    kl, sums = attend(
        place,
        table,
        plan_of([(1, 2), (3, 2), (2, 2)]),
        [far_1, far_3, far_2],
        rows,
        state=state,
        copies_out=devices,
    )
    terms = lax.all_to_all(sums, everyone, 0, 0, tiled=True)
    head_loss = jnp.sum(terms, axis=0)[:STUDENTS] / (devices * ROWS)
    return (kl[None], head_loss)


def solution(mesh):
    split = Mesh(
        mesh.devices.reshape(4, 2, mesh.shape["head"], 4, 4),
        ("dp_0", "dp_1", "head", "kv_0", "kv_1"),
    )
    in_specs = (P(DP, KV, "head"), P(DP, KV, "head"), P(DP, KV, "head"), P(DP, KV, "head"), P())
    out_specs = (P(DP, "head", KV), P("head"))
    return jax.shard_map(
        program, mesh=split, in_specs=in_specs, out_specs=out_specs, check_vma=False
    )
```

```python
import functools
import math

import jax
import jax.numpy as jnp
from jax import lax
from jax.experimental import pallas as pl
from jax.experimental.pallas import tpu as pltpu
from jax.sharding import Mesh
from jax.sharding import PartitionSpec as P


HT = 28
KVT = 4
DH = 128
ROWS = 256
PAIRS = 14
STUDENTS = 7
HEADS = PAIRS + STUDENTS
GROUP = HT // KVT
KV = ("kv_0", "kv_1")
DP = ("dp_0", "dp_1")
LANE = 128
SUB = 8
MASKED = -1e30
LARGE = 2.0**100
LN2 = math.log(2.0)
KAPPA = 1.0 / (LN2 * math.sqrt(DH))
STATE = 3 * PAIRS + 2 * STUDENTS
TL, TC, SM, SL = PAIRS, 2 * PAIRS, 3 * PAIRS, 3 * PAIRS + STUDENTS
OWN = 3
OTHER = 2
CHUNK = OWN + OTHER
PIECES = (2, 2, 5)
SENT = sum(PIECES)
MIB = 1024 * 1024
SMEM = pl.BlockSpec(memory_space=pltpu.SMEM)
VMEM = pl.BlockSpec(memory_space=pltpu.VMEM)
ANY = pl.BlockSpec(memory_space=pl.ANY)
HBM = pl.BlockSpec(memory_space=pltpu.HBM)


def heads_of(n):
    return jax.ShapeDtypeStruct((n, ROWS, DH), jnp.bfloat16)


def small(limit):
    return pltpu.CompilerParams(vmem_limit_bytes=limit * MIB)


def run_all(copies):
    for c in copies:
        c.start()
    for c in copies:
        c.wait()


def split_kernel(teacher, student, out, sems):
    run_all(
        [
            pltpu.make_async_copy(teacher.at[:, pl.ds(0, DH)], out.at[0], sems.at[0]),
            pltpu.make_async_copy(teacher.at[:, pl.ds(DH, DH)], out.at[1], sems.at[1]),
            pltpu.make_async_copy(student, out.at[2], sems.at[2]),
        ]
    )


def split_heads(teacher, student):
    return pl.pallas_call(
        split_kernel,
        out_shape=heads_of(OWN),
        in_specs=[HBM, HBM],
        out_specs=VMEM,
        scratch_shapes=[pltpu.SemaphoreType.DMA((3,))],
        compiler_params=small(2),
        name="split_heads",
    )(teacher, student)


def queries_kernel(place, table, query, *refs):
    pieces, (count, sent, sems) = refs[:-3], refs[-3:]
    head = place[0, 0]
    theirs = (1 - head) * STUDENTS

    def each(act):
        rank = jnp.int32(0)
        for p in range(PAIRS):
            teacher = table[p % 2, theirs + p // 2]
            mine = lax.div(teacher, PAIRS) == head
            lanes = pl.ds(pl.multiple_of(lax.rem(teacher, PAIRS) * DH, DH), DH)

            @pl.when(mine)
            def _():
                act(pltpu.make_async_copy(query.at[:, lanes], sent.at[rank], sems.at[p]))

            rank = rank + mine.astype(jnp.int32)
        return rank

    count[0, 0] = each(lambda c: c.start())
    each(lambda c: c.wait())
    rank = 0
    for piece in pieces:
        piece[...] = sent[rank : rank + piece.shape[0]]
        rank += piece.shape[0]


def queries_for_other(place, table, query):
    return pl.pallas_call(
        queries_kernel,
        out_shape=(
            *(heads_of(n) for n in (*PIECES, PAIRS - SENT)),
            jax.ShapeDtypeStruct((1, 1), jnp.int32),
        ),
        in_specs=[SMEM, SMEM, ANY],
        out_specs=(*[VMEM] * (len(PIECES) + 1), SMEM),
        scratch_shapes=[
            pltpu.VMEM((PAIRS, ROWS, DH), jnp.bfloat16),
            pltpu.SemaphoreType.DMA((PAIRS,)),
        ],
        compiler_params=small(4),
        name="queries_for_other",
    )(place, table, query)


def chunks_kernel(place, *refs):
    ring, out = refs[:-1], refs[-1]
    for head in range(2):

        @pl.when(place[0, 0] == head)
        def _():
            for n in range(len(ring) // 3):
                own, other = ring[3 * n], ring[3 * n + 1 + head]
                out[CHUNK * n : CHUNK * n + OWN] = own[...]
                out[CHUNK * n + OWN : CHUNK * (n + 1)] = other[:OTHER]


def chunks_of(place, ring, chunks):
    parts = [ring[o % 8] for m in chunks for o in (2 * m, 2 * m - 1, 2 * m + 1)]
    return pl.pallas_call(
        chunks_kernel,
        out_shape=heads_of(CHUNK * len(chunks)),
        in_specs=[SMEM] + [VMEM] * len(parts),
        out_specs=VMEM,
        compiler_params=small(4),
        name="chunks_of",
    )(place, *parts)


def scaled(q):
    q = q.astype(jnp.float32) * KAPPA
    high = q.astype(jnp.bfloat16)
    low = (q - high.astype(jnp.float32)).astype(jnp.bfloat16)
    return jnp.concatenate([high, low], axis=1)


def prepare_kernel(place, table, own, student, rows):
    head = place[0, 0]
    for s in range(STUDENTS):
        rows[PAIRS + s] = scaled(student[:, s * DH : (s + 1) * DH])
    for p in range(PAIRS):
        teacher = table[p % 2, head * STUDENTS + p // 2]
        lanes = pl.ds(pl.multiple_of(lax.rem(teacher, PAIRS) * DH, DH), DH)

        @pl.when(lax.div(teacher, PAIRS) == head)
        def _():
            rows[p] = scaled(own[:, lanes])


def prepare(place, table, own, student):
    return pl.pallas_call(
        prepare_kernel,
        out_shape=jax.ShapeDtypeStruct((HEADS, ROWS, 2 * DH), jnp.bfloat16),
        in_specs=[SMEM, SMEM, VMEM, VMEM],
        out_specs=VMEM,
        compiler_params=small(8),
        cost_estimate=pl.CostEstimate(
            flops=HEADS * ROWS * DH * 64, bytes_accessed=HEADS * ROWS * DH * 6, transcendentals=0
        ),
        name="prepare",
    )(place, table, own, student)


def fill_received(place, table, received, rows):
    head = place[0, 0]
    rank = jnp.int32(0)
    for p in range(PAIRS):
        mine = lax.div(table[p % 2, head * STUDENTS + p // 2], PAIRS) == head

        @pl.when(jnp.logical_not(mine))
        def _():
            rows[p] = scaled(received[rank])

        rank = rank + 1 - mine.astype(jnp.int32)


def attend_kernel(first, last, counts, blocks, place, table, plan, *refs):
    refs = list(refs)
    take = lambda n: [refs.pop(0) for _ in range(n)]
    groups = take(len(counts))
    if first:
        pieces = take(len(PIECES) + 1)
        take(1)
        state, rows = take(2)
    else:
        rows, before = take(2)
        if last:
            out, sums = take(2)
        else:
            (state,) = take(1)
    (keys,) = take(1)
    if first:
        received, entry = take(2)
    if last:
        (state,) = take(1)
    offsets = refs[0]
    if first:
        sems = refs[1]
    head, z_hi, x = place[0, 0], place[0, 1], place[0, 2]
    row_block = z_hi * 4 + x

    if first:
        inputs = []
        rank = 0
        for n, piece in enumerate(pieces):
            length = piece.shape[0]
            inputs.append(
                pltpu.make_async_copy(
                    piece, received.at[pl.ds(rank, length)], sems.at[n]
                )
            )
            rank += length
        for c in inputs:
            c.start()
        for c in inputs:
            c.wait()
        fill_received(place, table, received, rows)
    else:
        entry = before
        state[...] = before[...]

    for p in range(PAIRS):
        kv_head = lax.div(table[p % 2, head * STUDENTS + p // 2], GROUP)
        side = jnp.where(lax.div(kv_head, 2) == head, 0, OWN)
        offsets[p] = side + lax.rem(kv_head, 2)

    def place_keys(i):
        at = 0
        for g, n in enumerate(counts):
            if n % CHUNK == 0:
                lo = at // CHUNK

                @pl.when(jnp.logical_and(i >= lo, i < lo + n // CHUNK))
                def _():
                    keys[...] = groups[g][pl.ds((i - lo) * CHUNK, CHUNK)]

            else:
                inside = at % CHUNK

                @pl.when(i == at // CHUNK)
                def _():
                    keys[inside : inside + n] = groups[g][...]

            at += n

    def product(k, p):
        return lax.dot_general(
            jnp.concatenate([k, k], axis=1),
            rows[p],
            (((1,), (1,)), ((), ())),
            preferred_element_type=jnp.float32,
        )

    def folded(a):
        return a.reshape(ROWS // SUB, SUB, ROWS)

    def own_block():
        key_pos = lax.broadcasted_iota(jnp.int32, (ROWS, ROWS), 0)
        row_pos = lax.broadcasted_iota(jnp.int32, (ROWS, ROWS), 1)
        mask = key_pos <= row_pos

        def begin(logits, m_index, l_index):
            logits = jnp.where(mask, logits, MASKED)
            top = jnp.max(logits, axis=0, keepdims=True)
            weights = folded(jnp.exp2(logits - top))
            state[m_index] = jnp.broadcast_to(top, (SUB, ROWS))
            state[l_index] = jnp.sum(weights, axis=0)
            return weights

        for s in range(STUDENTS):
            zs = product(keys[2], PAIRS + s)
            begin(zs, SM + s, SL + s)
            for c in range(2):
                p = 2 * s + c
                zt = product(keys[offsets[p]], p)
                weights = begin(zt, p, TL + p)
                state[TC + p] = jnp.sum(weights * folded(zt - zs), axis=0)

    def block():
        def add(logits, m_index, l_index):
            weights = jnp.exp2(folded(logits) - state[m_index][None])
            state[l_index] = state[l_index] + jnp.sum(weights, axis=0)
            return weights

        student_keys = keys[2]
        for s in range(STUDENTS):
            zs = product(student_keys, PAIRS + s)
            add(zs, SM + s, SL + s)
            for c in range(2):
                p = 2 * s + c
                zt = product(keys[offsets[p]], p)
                weights = add(zt, p, TL + p)
                state[TC + p] = state[TC + p] + jnp.sum(weights * folded(zt - zs), axis=0)

    def exact_block():
        def add(logits, m_index, l_index):
            logits = folded(logits)
            old = state[m_index]
            new = jnp.maximum(old, jnp.max(logits, axis=0))
            weights = jnp.exp2(logits - new[None])
            rescale = jnp.exp2(old - new)
            state[m_index] = new
            state[l_index] = state[l_index] * rescale + jnp.sum(weights, axis=0)
            return weights, rescale

        def student(s, carry):
            zs = product(keys[2], PAIRS + s)
            add(zs, SM + s, SL + s)
            for c in range(2):
                p = 2 * s + c
                zt = product(keys[offsets[p]], p)
                weights, rescale = add(zt, p, TL + p)
                cross = jnp.sum(weights * folded(zt - zs), axis=0)
                state[TC + p] = state[TC + p] * rescale + cross
            return carry

        lax.fori_loop(0, STUDENTS, student, 0)

    def visible(i):
        chunk = lax.bitwise_and(z_hi - plan[0, i], 3)
        return chunk * 4 + lax.bitwise_and(x + plan[1, i], 3) < row_block

    def step(i, carry):
        @pl.when(visible(i))
        def _():
            place_keys(i)
            block()

        return carry

    def exact_step(i, carry):
        @pl.when(visible(i))
        def _():
            place_keys(i)
            exact_block()

        return carry

    if first:
        keys[...] = groups[0][...]
        own_block()
        entry[...] = state[...]
    lax.fori_loop(int(first), blocks, step, 0)

    largest = jnp.maximum(
        jnp.max(state[TL : TL + PAIRS]), jnp.max(state[SL : SL + STUDENTS])
    )

    @pl.when(largest > LARGE)
    def _():
        state[...] = entry[...]
        lax.fori_loop(int(first), blocks, exact_step, 0)

    if not last:
        return

    def merged(m8, l8):
        top = jnp.max(m8, axis=0, keepdims=True)
        factor = jnp.exp2(m8 - top)
        total = jnp.sum(l8 * factor, axis=0, keepdims=True)
        return factor, total, LN2 * top + jnp.log(total)

    lane = lax.broadcasted_iota(jnp.int32, (1, LANE), 1)
    line = jnp.zeros((1, LANE), jnp.float32)
    for s in range(STUDENTS):
        _, _, s_lse = merged(state[SM + s], state[SL + s])
        value = 2.0 * s_lse
        for c in range(2):
            p = 2 * s + c
            factor, total, t_lse = merged(state[p], state[TL + p])
            cross = jnp.sum(state[TC + p] * factor, axis=0, keepdims=True)
            value = value + (LN2 * cross / total - t_lse)
        out[s : s + 1, :] = value
        line = jnp.where(lane == s, jnp.sum(value, axis=1, keepdims=True), line)
    sums[...] = jnp.broadcast_to(line, sums.shape)


def attend(place, table, plan, groups, rows, queries=None, state=None, copies_out=0):
    first = queries is not None
    last = copies_out > 0
    counts = tuple(g.shape[0] for g in groups)
    blocks = plan.shape[1]
    state_shape = jax.ShapeDtypeStruct((STATE, SUB, ROWS), jnp.float32)
    rows_shape = jax.ShapeDtypeStruct((HEADS, ROWS, 2 * DH), jnp.bfloat16)
    if first:
        extra, out_shape = [*queries, rows], (state_shape, rows_shape)
    elif last:
        extra = [rows, state]
        out_shape = (
            jax.ShapeDtypeStruct((STUDENTS, ROWS), jnp.float32),
            jax.ShapeDtypeStruct((copies_out, LANE), jnp.float32),
        )
    else:
        extra, out_shape = [rows, state], state_shape
    extra_specs = [ANY] * (len(PIECES) + 1) + [VMEM] if first else [VMEM, VMEM]
    scratch = [pltpu.VMEM((CHUNK, ROWS, DH), jnp.bfloat16)]
    if first:
        scratch.append(pltpu.VMEM((PAIRS, ROWS, DH), jnp.bfloat16))
        scratch.append(pltpu.VMEM(state_shape.shape, jnp.float32))
    if last:
        scratch.append(pltpu.VMEM(state_shape.shape, jnp.float32))
    scratch.append(pltpu.SMEM((PAIRS,), jnp.int32))
    if first:
        scratch.append(pltpu.SemaphoreType.DMA((len(PIECES) + 1,)))
    return pl.pallas_call(
        functools.partial(attend_kernel, first, last, counts, blocks),
        out_shape=out_shape,
        in_specs=[SMEM] * 3 + [VMEM] * len(groups) + extra_specs,
        out_specs=jax.tree.map(lambda _: VMEM, out_shape),
        scratch_shapes=scratch,
        input_output_aliases={3 + len(groups) + len(extra) - 1: 1} if first else {},
        compiler_params=small(24),
        cost_estimate=pl.CostEstimate(
            flops=blocks * HEADS * 2 * ROWS * ROWS * 2 * DH,
            bytes_accessed=blocks * ROWS * CHUNK * DH * 2,
            transcendentals=blocks * HEADS * ROWS * ROWS,
        ),
        name="attend",
    )(place, table, plan, *groups, *extra)


def z_place(ring):
    ring %= 8
    return (ring % 2) * 4 + ring // 2


def plan_of(blocks):
    return jnp.array([list(row) for row in zip(*blocks)], jnp.int32)


def program(teacher_query, teacher_key, student_query, student_key, pair_table):
    head = lax.axis_index("head")
    table = pair_table.T
    place = jnp.stack([head, lax.axis_index("kv_0"), lax.axis_index("kv_1")])[None]

    def along_x(a, by, chunks, sources=range(4)):
        pairs = [(c * 4 + i, c * 4 + (i + by) % 4) for c in chunks for i in sources]
        return lax.ppermute(a, KV, pairs)

    def along_z(a, by, sources):
        pairs = [(z_place(i), z_place(i + by)) for i in sources]
        return lax.ppermute(a, ("head", "kv_0"), pairs)

    other_side = [(0, 1), (1, 0)]

    ring = {0: split_heads(teacher_key[0], student_key[0])}
    *chosen, count = queries_for_other(place, table, teacher_query[0])
    ring[1] = along_z(ring[0], 1, range(7))
    ring[7] = along_z(ring[0], -1, (0, 1, 2, 3, 5, 7))
    pieces = [lax.ppermute(piece, "head", other_side) for piece in chosen[:-1]]
    more = lax.cond(
        count[0, 0] > SENT,
        lambda q: lax.ppermute(q, "head", other_side),
        lambda q: q,
        chosen[-1],
    )
    more, ring[1], ring[7] = lax.optimization_barrier((more, ring[1], ring[7]))
    rows = prepare(place, table, teacher_query[0], student_query[0])
    mine = chunks_of(place, ring, (0,))
    near_a = along_x(mine, 1, range(4), (0, 1, 2))
    near_b = along_x(mine, -1, range(4), (0, 1))
    near_c = along_x(near_a[:OTHER], 1, range(4), (1, 2))
    near_d = along_x(near_b[OTHER:], -1, range(4), (3, 0))
    for step in range(2, 5):
        ring[step] = along_z(ring[step - 1], 1, range(step - 1, 7))
        if step < 4:
            ring[8 - step] = along_z(ring[9 - step], -1, (7, 0, 1 if step == 2 else 6))

    rest_13 = chunks_of(place, ring, (1, 3))
    left_13 = along_x(rest_13, 1, (1, 2, 3))
    right_13 = along_x(rest_13, -1, (1, 2, 3))
    rest_2 = chunks_of(place, ring, (2,))
    left_2 = along_x(rest_2, 1, (2, 3))
    right_2 = along_x(rest_2, -1, (2, 3))
    state, rows = attend(
        place,
        table,
        plan_of([(0, 0), (0, -1), (0, 1), (0, 2), (1, 0), (3, 0), (2, 0)]),
        [mine, near_a, near_b, near_c, near_d, rest_13, rest_2],
        rows,
        queries=(*pieces, more),
    )
    left_13, right_13, state = lax.optimization_barrier((left_13, right_13, state))
    cut_1 = left_13[:CHUNK]
    cut_3 = right_13[CHUNK:]
    far_1 = along_x(cut_1, 1, (1, 2, 3))
    far_3 = along_x(cut_3, -1, (3,))
    left_2, right_2, state = lax.optimization_barrier((left_2, right_2, state))
    far_2 = along_x(left_2, 1, (2, 3))
    state = attend(
        place,
        table,
        plan_of([(1, -1), (3, -1), (1, 1), (3, 1), (2, -1), (2, 1)]),
        [left_13, right_13, left_2, right_2],
        rows,
        state=state,
    )
    everyone = ("dp_0", "dp_1", "kv_0", "kv_1")
    devices = lax.axis_size(everyone)
    kl, sums = attend(
        place,
        table,
        plan_of([(1, 2), (3, 2), (2, 2)]),
        [far_1, far_3, far_2],
        rows,
        state=state,
        copies_out=devices,
    )
    terms = lax.all_to_all(sums, everyone, 0, 0, tiled=True)
    head_loss = jnp.sum(terms, axis=0)[:STUDENTS] / (devices * ROWS)
    return (kl[None], head_loss)


def solution(mesh):
    split = Mesh(
        mesh.devices.reshape(4, 2, mesh.shape["head"], 4, 4),
        ("dp_0", "dp_1", "head", "kv_0", "kv_1"),
    )
    in_specs = (P(DP, KV, "head"), P(DP, KV, "head"), P(DP, KV, "head"), P(DP, KV, "head"), P())
    out_specs = (P(DP, "head", KV), P("head"))
    return jax.shard_map(
        program, mesh=split, in_specs=in_specs, out_specs=out_specs, check_vma=False
    )
```

```python
import functools
import math

import jax
import jax.numpy as jnp
from jax import lax
from jax.experimental import pallas as pl
from jax.experimental.pallas import tpu as pltpu
from jax.sharding import Mesh
from jax.sharding import PartitionSpec as P


HT = 28
KVT = 4
DH = 128
ROWS = 256
PAIRS = 14
STUDENTS = 7
HEADS = PAIRS + STUDENTS
GROUP = HT // KVT
KV = ("kv_0", "kv_1")
DP = ("dp_0", "dp_1")
LANE = 128
SUB = 8
MASKED = -1e30
LARGE = 2.0**100
LN2 = math.log(2.0)
KAPPA = 1.0 / (LN2 * math.sqrt(DH))
STATE = 3 * PAIRS + 2 * STUDENTS
TL, TC, SM, SL = PAIRS, 2 * PAIRS, 3 * PAIRS, 3 * PAIRS + STUDENTS
OWN = 3
OTHER = 2
CHUNK = OWN + OTHER
PIECES = (4, 5)
SENT = sum(PIECES)
MIB = 1024 * 1024
SMEM = pl.BlockSpec(memory_space=pltpu.SMEM)
VMEM = pl.BlockSpec(memory_space=pltpu.VMEM)
ANY = pl.BlockSpec(memory_space=pl.ANY)
HBM = pl.BlockSpec(memory_space=pltpu.HBM)


def heads_of(n):
    return jax.ShapeDtypeStruct((n, ROWS, DH), jnp.bfloat16)


def small(limit):
    return pltpu.CompilerParams(vmem_limit_bytes=limit * MIB)


def run_all(copies):
    for c in copies:
        c.start()
    for c in copies:
        c.wait()


def split_kernel(teacher, student, out, sems):
    run_all(
        [
            pltpu.make_async_copy(teacher.at[:, pl.ds(0, DH)], out.at[0], sems.at[0]),
            pltpu.make_async_copy(teacher.at[:, pl.ds(DH, DH)], out.at[1], sems.at[1]),
            pltpu.make_async_copy(student, out.at[2], sems.at[2]),
        ]
    )


def split_heads(teacher, student):
    return pl.pallas_call(
        split_kernel,
        out_shape=heads_of(OWN),
        in_specs=[HBM, HBM],
        out_specs=VMEM,
        scratch_shapes=[pltpu.SemaphoreType.DMA((3,))],
        compiler_params=small(2),
        name="split_heads",
    )(teacher, student)


def queries_kernel(place, table, query, *refs):
    pieces, (count, sent, sems) = refs[:-3], refs[-3:]
    head = place[0, 0]
    theirs = (1 - head) * STUDENTS

    def each(act):
        rank = jnp.int32(0)
        for p in range(PAIRS):
            teacher = table[p % 2, theirs + p // 2]
            mine = lax.div(teacher, PAIRS) == head
            lanes = pl.ds(pl.multiple_of(lax.rem(teacher, PAIRS) * DH, DH), DH)

            @pl.when(mine)
            def _():
                act(pltpu.make_async_copy(query.at[:, lanes], sent.at[rank], sems.at[p]))

            rank = rank + mine.astype(jnp.int32)
        return rank

    count[0, 0] = each(lambda c: c.start())
    each(lambda c: c.wait())
    rank = 0
    for piece in pieces:
        piece[...] = sent[rank : rank + piece.shape[0]]
        rank += piece.shape[0]


def queries_for_other(place, table, query):
    return pl.pallas_call(
        queries_kernel,
        out_shape=(
            *(heads_of(n) for n in (*PIECES, PAIRS - SENT)),
            jax.ShapeDtypeStruct((1, 1), jnp.int32),
        ),
        in_specs=[SMEM, SMEM, ANY],
        out_specs=(*[VMEM] * (len(PIECES) + 1), SMEM),
        scratch_shapes=[
            pltpu.VMEM((PAIRS, ROWS, DH), jnp.bfloat16),
            pltpu.SemaphoreType.DMA((PAIRS,)),
        ],
        compiler_params=small(4),
        name="queries_for_other",
    )(place, table, query)


def chunks_kernel(place, *refs):
    ring, out = refs[:-1], refs[-1]
    for head in range(2):

        @pl.when(place[0, 0] == head)
        def _():
            for n in range(len(ring) // 3):
                own, other = ring[3 * n], ring[3 * n + 1 + head]
                out[CHUNK * n : CHUNK * n + OWN] = own[...]
                out[CHUNK * n + OWN : CHUNK * (n + 1)] = other[:OTHER]


def chunks_of(place, ring, chunks):
    parts = [ring[o % 8] for m in chunks for o in (2 * m, 2 * m - 1, 2 * m + 1)]
    return pl.pallas_call(
        chunks_kernel,
        out_shape=heads_of(CHUNK * len(chunks)),
        in_specs=[SMEM] + [VMEM] * len(parts),
        out_specs=VMEM,
        compiler_params=small(4),
        name="chunks_of",
    )(place, *parts)


def scaled(q):
    q = q.astype(jnp.float32) * KAPPA
    high = q.astype(jnp.bfloat16)
    low = (q - high.astype(jnp.float32)).astype(jnp.bfloat16)
    return jnp.concatenate([high, low], axis=1)


def prepare_kernel(place, table, own, student, rows):
    head = place[0, 0]
    for s in range(STUDENTS):
        rows[PAIRS + s] = scaled(student[:, s * DH : (s + 1) * DH])
    for p in range(PAIRS):
        teacher = table[p % 2, head * STUDENTS + p // 2]
        lanes = pl.ds(pl.multiple_of(lax.rem(teacher, PAIRS) * DH, DH), DH)

        @pl.when(lax.div(teacher, PAIRS) == head)
        def _():
            rows[p] = scaled(own[:, lanes])


def prepare(place, table, own, student):
    return pl.pallas_call(
        prepare_kernel,
        out_shape=jax.ShapeDtypeStruct((HEADS, ROWS, 2 * DH), jnp.bfloat16),
        in_specs=[SMEM, SMEM, VMEM, VMEM],
        out_specs=VMEM,
        compiler_params=small(8),
        cost_estimate=pl.CostEstimate(
            flops=HEADS * ROWS * DH * 64, bytes_accessed=HEADS * ROWS * DH * 6, transcendentals=0
        ),
        name="prepare",
    )(place, table, own, student)


def fill_received(place, table, received, rows):
    head = place[0, 0]
    rank = jnp.int32(0)
    for p in range(PAIRS):
        mine = lax.div(table[p % 2, head * STUDENTS + p // 2], PAIRS) == head

        @pl.when(jnp.logical_not(mine))
        def _():
            rows[p] = scaled(received[rank])

        rank = rank + 1 - mine.astype(jnp.int32)


def attend_kernel(first, last, counts, blocks, place, table, plan, *refs):
    refs = list(refs)
    take = lambda n: [refs.pop(0) for _ in range(n)]
    groups = take(len(counts))
    if first:
        pieces = take(len(PIECES) + 1)
        take(1)
        state, rows = take(2)
    else:
        rows, before = take(2)
        if last:
            out, sums = take(2)
        else:
            (state,) = take(1)
    (keys,) = take(1)
    if first:
        received, entry = take(2)
    if last:
        (state,) = take(1)
    offsets = refs[0]
    if first:
        sems = refs[1]
    head, z_hi, x = place[0, 0], place[0, 1], place[0, 2]
    row_block = z_hi * 4 + x

    if first:
        inputs = []
        rank = 0
        for n, piece in enumerate(pieces):
            length = piece.shape[0]
            inputs.append(
                pltpu.make_async_copy(
                    piece, received.at[pl.ds(rank, length)], sems.at[n]
                )
            )
            rank += length
        for c in inputs:
            c.start()
        for c in inputs:
            c.wait()
        fill_received(place, table, received, rows)
    else:
        entry = before
        state[...] = before[...]

    for p in range(PAIRS):
        kv_head = lax.div(table[p % 2, head * STUDENTS + p // 2], GROUP)
        side = jnp.where(lax.div(kv_head, 2) == head, 0, OWN)
        offsets[p] = side + lax.rem(kv_head, 2)

    def place_keys(i):
        at = 0
        for g, n in enumerate(counts):
            if n % CHUNK == 0:
                lo = at // CHUNK

                @pl.when(jnp.logical_and(i >= lo, i < lo + n // CHUNK))
                def _():
                    keys[...] = groups[g][pl.ds((i - lo) * CHUNK, CHUNK)]

            else:
                inside = at % CHUNK

                @pl.when(i == at // CHUNK)
                def _():
                    keys[inside : inside + n] = groups[g][...]

            at += n

    def product(k, p):
        return lax.dot_general(
            jnp.concatenate([k, k], axis=1),
            rows[p],
            (((1,), (1,)), ((), ())),
            preferred_element_type=jnp.float32,
        )

    def folded(a):
        return a.reshape(ROWS // SUB, SUB, ROWS)

    def own_block():
        key_pos = lax.broadcasted_iota(jnp.int32, (ROWS, ROWS), 0)
        row_pos = lax.broadcasted_iota(jnp.int32, (ROWS, ROWS), 1)
        mask = key_pos <= row_pos

        def begin(logits, m_index, l_index):
            logits = jnp.where(mask, logits, MASKED)
            top = jnp.max(logits, axis=0, keepdims=True)
            weights = folded(jnp.exp2(logits - top))
            state[m_index] = jnp.broadcast_to(top, (SUB, ROWS))
            state[l_index] = jnp.sum(weights, axis=0)
            return weights

        for s in range(STUDENTS):
            zs = product(keys[2], PAIRS + s)
            begin(zs, SM + s, SL + s)
            for c in range(2):
                p = 2 * s + c
                zt = product(keys[offsets[p]], p)
                weights = begin(zt, p, TL + p)
                state[TC + p] = jnp.sum(weights * folded(zt - zs), axis=0)

    def block():
        def add(logits, m_index, l_index):
            weights = jnp.exp2(folded(logits) - state[m_index][None])
            state[l_index] = state[l_index] + jnp.sum(weights, axis=0)
            return weights

        student_keys = keys[2]
        for s in range(STUDENTS):
            zs = product(student_keys, PAIRS + s)
            add(zs, SM + s, SL + s)
            for c in range(2):
                p = 2 * s + c
                zt = product(keys[offsets[p]], p)
                weights = add(zt, p, TL + p)
                state[TC + p] = state[TC + p] + jnp.sum(weights * folded(zt - zs), axis=0)

    def exact_block():
        def add(logits, m_index, l_index):
            logits = folded(logits)
            old = state[m_index]
            new = jnp.maximum(old, jnp.max(logits, axis=0))
            weights = jnp.exp2(logits - new[None])
            rescale = jnp.exp2(old - new)
            state[m_index] = new
            state[l_index] = state[l_index] * rescale + jnp.sum(weights, axis=0)
            return weights, rescale

        def student(s, carry):
            zs = product(keys[2], PAIRS + s)
            add(zs, SM + s, SL + s)
            for c in range(2):
                p = 2 * s + c
                zt = product(keys[offsets[p]], p)
                weights, rescale = add(zt, p, TL + p)
                cross = jnp.sum(weights * folded(zt - zs), axis=0)
                state[TC + p] = state[TC + p] * rescale + cross
            return carry

        lax.fori_loop(0, STUDENTS, student, 0)

    def visible(i):
        chunk = lax.bitwise_and(z_hi - plan[0, i], 3)
        return chunk * 4 + lax.bitwise_and(x + plan[1, i], 3) < row_block

    def step(i, carry):
        @pl.when(visible(i))
        def _():
            place_keys(i)
            block()

        return carry

    def exact_step(i, carry):
        @pl.when(visible(i))
        def _():
            place_keys(i)
            exact_block()

        return carry

    if first:
        keys[...] = groups[0][...]
        own_block()
        entry[...] = state[...]
    lax.fori_loop(int(first), blocks, step, 0)

    largest = jnp.maximum(
        jnp.max(state[TL : TL + PAIRS]), jnp.max(state[SL : SL + STUDENTS])
    )

    @pl.when(largest > LARGE)
    def _():
        state[...] = entry[...]
        lax.fori_loop(int(first), blocks, exact_step, 0)

    if not last:
        return

    def merged(m8, l8):
        top = jnp.max(m8, axis=0, keepdims=True)
        factor = jnp.exp2(m8 - top)
        total = jnp.sum(l8 * factor, axis=0, keepdims=True)
        return factor, total, LN2 * top + jnp.log(total)

    lane = lax.broadcasted_iota(jnp.int32, (1, LANE), 1)
    line = jnp.zeros((1, LANE), jnp.float32)
    for s in range(STUDENTS):
        _, _, s_lse = merged(state[SM + s], state[SL + s])
        value = 2.0 * s_lse
        for c in range(2):
            p = 2 * s + c
            factor, total, t_lse = merged(state[p], state[TL + p])
            cross = jnp.sum(state[TC + p] * factor, axis=0, keepdims=True)
            value = value + (LN2 * cross / total - t_lse)
        out[s : s + 1, :] = value
        line = jnp.where(lane == s, jnp.sum(value, axis=1, keepdims=True), line)
    sums[...] = jnp.broadcast_to(line, sums.shape)


def attend(place, table, plan, groups, rows, queries=None, state=None, copies_out=0):
    first = queries is not None
    last = copies_out > 0
    counts = tuple(g.shape[0] for g in groups)
    blocks = plan.shape[1]
    state_shape = jax.ShapeDtypeStruct((STATE, SUB, ROWS), jnp.float32)
    rows_shape = jax.ShapeDtypeStruct((HEADS, ROWS, 2 * DH), jnp.bfloat16)
    if first:
        extra, out_shape = [*queries, rows], (state_shape, rows_shape)
    elif last:
        extra = [rows, state]
        out_shape = (
            jax.ShapeDtypeStruct((STUDENTS, ROWS), jnp.float32),
            jax.ShapeDtypeStruct((copies_out, LANE), jnp.float32),
        )
    else:
        extra, out_shape = [rows, state], state_shape
    extra_specs = [ANY] * (len(PIECES) + 1) + [VMEM] if first else [VMEM, VMEM]
    scratch = [pltpu.VMEM((CHUNK, ROWS, DH), jnp.bfloat16)]
    if first:
        scratch.append(pltpu.VMEM((PAIRS, ROWS, DH), jnp.bfloat16))
        scratch.append(pltpu.VMEM(state_shape.shape, jnp.float32))
    if last:
        scratch.append(pltpu.VMEM(state_shape.shape, jnp.float32))
    scratch.append(pltpu.SMEM((PAIRS,), jnp.int32))
    if first:
        scratch.append(pltpu.SemaphoreType.DMA((len(PIECES) + 1,)))
    return pl.pallas_call(
        functools.partial(attend_kernel, first, last, counts, blocks),
        out_shape=out_shape,
        in_specs=[SMEM] * 3 + [VMEM] * len(groups) + extra_specs,
        out_specs=jax.tree.map(lambda _: VMEM, out_shape),
        scratch_shapes=scratch,
        input_output_aliases={3 + len(groups) + len(extra) - 1: 1} if first else {},
        compiler_params=small(24),
        cost_estimate=pl.CostEstimate(
            flops=blocks * HEADS * 2 * ROWS * ROWS * 2 * DH,
            bytes_accessed=blocks * ROWS * CHUNK * DH * 2,
            transcendentals=blocks * HEADS * ROWS * ROWS,
        ),
        name="attend",
    )(place, table, plan, *groups, *extra)


def shift(n, by):
    return [(i, (i + by) % n) for i in range(n)]


def z_place(ring):
    ring %= 8
    return (ring % 2) * 4 + ring // 2


def z_shift(by):
    return [(z_place(i), z_place(i + by)) for i in range(8)]


def plan_of(blocks):
    return jnp.array([list(row) for row in zip(*blocks)], jnp.int32)


def program(teacher_query, teacher_key, student_query, student_key, pair_table):
    head = lax.axis_index("head")
    table = pair_table.T
    place = jnp.stack([head, lax.axis_index("kv_0"), lax.axis_index("kv_1")])[None]

    along_x = lambda a, by: lax.ppermute(a, "kv_1", shift(4, by))
    along_z = lambda a, by: lax.ppermute(a, ("head", "kv_0"), z_shift(by))
    other_side = [(0, 1), (1, 0)]

    ring = {0: split_heads(teacher_key[0], student_key[0])}
    *chosen, count = queries_for_other(place, table, teacher_query[0])
    ring[1] = along_z(ring[0], 1)
    ring[7] = along_z(ring[0], -1)
    pieces = [lax.ppermute(piece, "head", other_side) for piece in chosen[:-1]]
    more = lax.cond(
        count[0, 0] > SENT,
        lambda q: lax.ppermute(q, "head", other_side),
        lambda q: q,
        chosen[-1],
    )
    more, ring[1], ring[7] = lax.optimization_barrier((more, ring[1], ring[7]))
    rows = prepare(place, table, teacher_query[0], student_query[0])
    mine = chunks_of(place, ring, (0,))
    near_a = along_x(mine, 1)
    near_b = along_x(mine, -1)
    near_c = along_x(near_a[:OTHER], 1)
    near_d = along_x(near_b[OTHER:], -1)
    for step in range(2, 5):
        ring[step] = along_z(ring[step - 1], 1)
        if step < 4:
            ring[8 - step] = along_z(ring[9 - step], -1)

    rest_13 = chunks_of(place, ring, (1, 3))
    left_13 = along_x(rest_13, 1)
    right_13 = along_x(rest_13, -1)
    rest_2 = chunks_of(place, ring, (2,))
    left_2 = along_x(rest_2, 1)
    right_2 = along_x(rest_2, -1)
    state, rows = attend(
        place,
        table,
        plan_of([(0, 0), (0, -1), (0, 1), (0, 2), (1, 0), (3, 0), (2, 0)]),
        [mine, near_a, near_b, near_c, near_d, rest_13, rest_2],
        rows,
        queries=(*pieces, more),
    )
    left_13, right_13, state = lax.optimization_barrier((left_13, right_13, state))
    cut_1 = left_13[:CHUNK]
    cut_3 = right_13[CHUNK:]
    far_1 = along_x(cut_1, 1)
    far_3 = along_x(cut_3, -1)
    left_2, right_2, state = lax.optimization_barrier((left_2, right_2, state))
    far_2 = along_x(left_2, 1)
    state = attend(
        place,
        table,
        plan_of([(1, -1), (3, -1), (1, 1), (3, 1), (2, -1), (2, 1)]),
        [left_13, right_13, left_2, right_2],
        rows,
        state=state,
    )
    everyone = ("dp_0", "dp_1", "kv_0", "kv_1")
    devices = lax.axis_size(everyone)
    kl, sums = attend(
        place,
        table,
        plan_of([(1, 2), (3, 2), (2, 2)]),
        [far_1, far_3, far_2],
        rows,
        state=state,
        copies_out=devices,
    )
    terms = lax.all_to_all(sums, everyone, 0, 0, tiled=True)
    head_loss = jnp.sum(terms, axis=0)[:STUDENTS] / (devices * ROWS)
    return (kl[None], head_loss)


def solution(mesh):
    split = Mesh(
        mesh.devices.reshape(4, 2, mesh.shape["head"], 4, 4),
        ("dp_0", "dp_1", "head", "kv_0", "kv_1"),
    )
    in_specs = (P(DP, KV, "head"), P(DP, KV, "head"), P(DP, KV, "head"), P(DP, KV, "head"), P())
    out_specs = (P(DP, "head", KV), P("head"))
    return jax.shard_map(
        program, mesh=split, in_specs=in_specs, out_specs=out_specs, check_vma=False
    )
```

```python
import functools
import math

import jax
import jax.numpy as jnp
from jax import lax
from jax.experimental import pallas as pl
from jax.experimental.pallas import tpu as pltpu
from jax.sharding import Mesh
from jax.sharding import PartitionSpec as P


HT = 28
KVT = 4
DH = 128
ROWS = 256
PAIRS = 14
STUDENTS = 7
HEADS = PAIRS + STUDENTS
GROUP = HT // KVT
KV = ("kv_0", "kv_1")
DP = ("dp_0", "dp_1")
LANE = 128
SUB = 8
MASKED = -1e30
LARGE = 2.0**100
LN2 = math.log(2.0)
KAPPA = 1.0 / (LN2 * math.sqrt(DH))
STATE = 3 * PAIRS + 2 * STUDENTS
TL, TC, SM, SL = PAIRS, 2 * PAIRS, 3 * PAIRS, 3 * PAIRS + STUDENTS
OWN = 3
OTHER = 2
CHUNK = OWN + OTHER
PIECES = (4, 5)
SENT = sum(PIECES)
MIB = 1024 * 1024
SMEM = pl.BlockSpec(memory_space=pltpu.SMEM)
VMEM = pl.BlockSpec(memory_space=pltpu.VMEM)
ANY = pl.BlockSpec(memory_space=pl.ANY)
HBM = pl.BlockSpec(memory_space=pltpu.HBM)


def heads_of(n):
    return jax.ShapeDtypeStruct((n, ROWS, DH), jnp.bfloat16)


def small(limit):
    return pltpu.CompilerParams(vmem_limit_bytes=limit * MIB)


def run_all(copies):
    for c in copies:
        c.start()
    for c in copies:
        c.wait()


def split_kernel(teacher, student, out, sems):
    run_all(
        [
            pltpu.make_async_copy(teacher.at[:, pl.ds(0, DH)], out.at[0], sems.at[0]),
            pltpu.make_async_copy(teacher.at[:, pl.ds(DH, DH)], out.at[1], sems.at[1]),
            pltpu.make_async_copy(student, out.at[2], sems.at[2]),
        ]
    )


def split_heads(teacher, student):
    return pl.pallas_call(
        split_kernel,
        out_shape=heads_of(OWN),
        in_specs=[HBM, HBM],
        out_specs=VMEM,
        scratch_shapes=[pltpu.SemaphoreType.DMA((3,))],
        compiler_params=small(2),
        name="split_heads",
    )(teacher, student)


def queries_kernel(place, table, query, *refs):
    pieces, (count, sent, sems) = refs[:-3], refs[-3:]
    head = place[0, 0]
    theirs = (1 - head) * STUDENTS

    def each(act):
        rank = jnp.int32(0)
        for p in range(PAIRS):
            teacher = table[p % 2, theirs + p // 2]
            mine = lax.div(teacher, PAIRS) == head
            lanes = pl.ds(pl.multiple_of(lax.rem(teacher, PAIRS) * DH, DH), DH)

            @pl.when(mine)
            def _():
                act(pltpu.make_async_copy(query.at[:, lanes], sent.at[rank], sems.at[p]))

            rank = rank + mine.astype(jnp.int32)
        return rank

    count[0, 0] = each(lambda c: c.start())
    each(lambda c: c.wait())
    rank = 0
    for piece in pieces:
        piece[...] = sent[rank : rank + piece.shape[0]]
        rank += piece.shape[0]


def queries_for_other(place, table, query):
    return pl.pallas_call(
        queries_kernel,
        out_shape=(
            *(heads_of(n) for n in (*PIECES, PAIRS - SENT)),
            jax.ShapeDtypeStruct((1, 1), jnp.int32),
        ),
        in_specs=[SMEM, SMEM, ANY],
        out_specs=(*[VMEM] * (len(PIECES) + 1), SMEM),
        scratch_shapes=[
            pltpu.VMEM((PAIRS, ROWS, DH), jnp.bfloat16),
            pltpu.SemaphoreType.DMA((PAIRS,)),
        ],
        compiler_params=small(4),
        name="queries_for_other",
    )(place, table, query)


def chunks_kernel(place, *refs):
    ring, out = refs[:-1], refs[-1]
    for head in range(2):

        @pl.when(place[0, 0] == head)
        def _():
            for n in range(len(ring) // 3):
                own, other = ring[3 * n], ring[3 * n + 1 + head]
                out[CHUNK * n : CHUNK * n + OWN] = own[...]
                out[CHUNK * n + OWN : CHUNK * (n + 1)] = other[:OTHER]


def chunks_of(place, ring, chunks):
    parts = [ring[o % 8] for m in chunks for o in (2 * m, 2 * m - 1, 2 * m + 1)]
    return pl.pallas_call(
        chunks_kernel,
        out_shape=heads_of(CHUNK * len(chunks)),
        in_specs=[SMEM] + [VMEM] * len(parts),
        out_specs=VMEM,
        compiler_params=small(4),
        name="chunks_of",
    )(place, *parts)


def scaled(q):
    q = q.astype(jnp.float32) * KAPPA
    high = q.astype(jnp.bfloat16)
    low = (q - high.astype(jnp.float32)).astype(jnp.bfloat16)
    return jnp.concatenate([high, low], axis=1)


def prepare_kernel(place, table, own, student, rows):
    head = place[0, 0]
    for s in range(STUDENTS):
        rows[PAIRS + s] = scaled(student[:, s * DH : (s + 1) * DH])
    for p in range(PAIRS):
        teacher = table[p % 2, head * STUDENTS + p // 2]
        lanes = pl.ds(pl.multiple_of(lax.rem(teacher, PAIRS) * DH, DH), DH)

        @pl.when(lax.div(teacher, PAIRS) == head)
        def _():
            rows[p] = scaled(own[:, lanes])


def prepare(place, table, own, student):
    return pl.pallas_call(
        prepare_kernel,
        out_shape=jax.ShapeDtypeStruct((HEADS, ROWS, 2 * DH), jnp.bfloat16),
        in_specs=[SMEM, SMEM, VMEM, VMEM],
        out_specs=VMEM,
        compiler_params=small(8),
        cost_estimate=pl.CostEstimate(
            flops=HEADS * ROWS * DH * 64, bytes_accessed=HEADS * ROWS * DH * 6, transcendentals=0
        ),
        name="prepare",
    )(place, table, own, student)


def fill_received(place, table, received, rows):
    head = place[0, 0]
    rank = jnp.int32(0)
    for p in range(PAIRS):
        mine = lax.div(table[p % 2, head * STUDENTS + p // 2], PAIRS) == head

        @pl.when(jnp.logical_not(mine))
        def _():
            rows[p] = scaled(received[rank])

        rank = rank + 1 - mine.astype(jnp.int32)


def attend_kernel(first, last, counts, blocks, place, table, plan, *refs):
    refs = list(refs)
    take = lambda n: [refs.pop(0) for _ in range(n)]
    groups = take(len(counts))
    if first:
        pieces = take(len(PIECES) + 1)
        take(1)
        state, rows = take(2)
    else:
        rows, before = take(2)
        if last:
            out, sums = take(2)
        else:
            (state,) = take(1)
    (keys,) = take(1)
    if first:
        received, entry = take(2)
    if last:
        (state,) = take(1)
    offsets = refs[0]
    if first:
        sems = refs[1]
    head, z_hi, x = place[0, 0], place[0, 1], place[0, 2]
    row_block = z_hi * 4 + x

    if first:
        inputs = []
        rank = 0
        for n, piece in enumerate(pieces):
            length = piece.shape[0]
            inputs.append(
                pltpu.make_async_copy(
                    piece, received.at[pl.ds(rank, length)], sems.at[n]
                )
            )
            rank += length
        for c in inputs:
            c.start()
        for c in inputs:
            c.wait()
        fill_received(place, table, received, rows)
    else:
        entry = before
        state[...] = before[...]

    for p in range(PAIRS):
        kv_head = lax.div(table[p % 2, head * STUDENTS + p // 2], GROUP)
        side = jnp.where(lax.div(kv_head, 2) == head, 0, OWN)
        offsets[p] = side + lax.rem(kv_head, 2)

    def place_keys(i):
        at = 0
        for g, n in enumerate(counts):
            if n % CHUNK == 0:
                lo = at // CHUNK

                @pl.when(jnp.logical_and(i >= lo, i < lo + n // CHUNK))
                def _():
                    keys[...] = groups[g][pl.ds((i - lo) * CHUNK, CHUNK)]

            else:
                inside = at % CHUNK

                @pl.when(i == at // CHUNK)
                def _():
                    keys[inside : inside + n] = groups[g][...]

            at += n

    def product(k, p):
        return lax.dot_general(
            jnp.concatenate([k, k], axis=1),
            rows[p],
            (((1,), (1,)), ((), ())),
            preferred_element_type=jnp.float32,
        )

    def folded(a):
        return a.reshape(ROWS // SUB, SUB, ROWS)

    def own_block():
        key_pos = lax.broadcasted_iota(jnp.int32, (ROWS, ROWS), 0)
        row_pos = lax.broadcasted_iota(jnp.int32, (ROWS, ROWS), 1)
        mask = key_pos <= row_pos

        def begin(logits, m_index, l_index):
            logits = jnp.where(mask, logits, MASKED)
            top = jnp.max(logits, axis=0, keepdims=True)
            weights = folded(jnp.exp2(logits - top))
            state[m_index] = jnp.broadcast_to(top, (SUB, ROWS))
            state[l_index] = jnp.sum(weights, axis=0)
            return weights

        for s in range(STUDENTS):
            zs = product(keys[2], PAIRS + s)
            begin(zs, SM + s, SL + s)
            for c in range(2):
                p = 2 * s + c
                zt = product(keys[offsets[p]], p)
                weights = begin(zt, p, TL + p)
                state[TC + p] = jnp.sum(weights * folded(zt - zs), axis=0)

    def block():
        def add(logits, m_index, l_index):
            weights = jnp.exp2(folded(logits) - state[m_index][None])
            state[l_index] = state[l_index] + jnp.sum(weights, axis=0)
            return weights

        student_keys = keys[2]
        for s in range(STUDENTS):
            zs = product(student_keys, PAIRS + s)
            add(zs, SM + s, SL + s)
            for c in range(2):
                p = 2 * s + c
                zt = product(keys[offsets[p]], p)
                weights = add(zt, p, TL + p)
                state[TC + p] = state[TC + p] + jnp.sum(weights * folded(zt - zs), axis=0)

    def exact_block():
        def add(logits, m_index, l_index):
            logits = folded(logits)
            old = state[m_index]
            new = jnp.maximum(old, jnp.max(logits, axis=0))
            weights = jnp.exp2(logits - new[None])
            rescale = jnp.exp2(old - new)
            state[m_index] = new
            state[l_index] = state[l_index] * rescale + jnp.sum(weights, axis=0)
            return weights, rescale

        def student(s, carry):
            zs = product(keys[2], PAIRS + s)
            add(zs, SM + s, SL + s)
            for c in range(2):
                p = 2 * s + c
                zt = product(keys[offsets[p]], p)
                weights, rescale = add(zt, p, TL + p)
                cross = jnp.sum(weights * folded(zt - zs), axis=0)
                state[TC + p] = state[TC + p] * rescale + cross
            return carry

        lax.fori_loop(0, STUDENTS, student, 0)

    def visible(i):
        chunk = lax.bitwise_and(z_hi - plan[0, i], 3)
        return chunk * 4 + lax.bitwise_and(x + plan[1, i], 3) < row_block

    def step(i, carry):
        @pl.when(visible(i))
        def _():
            place_keys(i)
            block()

        return carry

    def exact_step(i, carry):
        @pl.when(visible(i))
        def _():
            place_keys(i)
            exact_block()

        return carry

    if first:
        keys[...] = groups[0][...]
        own_block()
        entry[...] = state[...]
    lax.fori_loop(int(first), blocks, step, 0)

    largest = jnp.maximum(
        jnp.max(state[TL : TL + PAIRS]), jnp.max(state[SL : SL + STUDENTS])
    )

    @pl.when(largest > LARGE)
    def _():
        state[...] = entry[...]
        lax.fori_loop(int(first), blocks, exact_step, 0)

    if not last:
        return

    def merged(m8, l8):
        top = jnp.max(m8, axis=0, keepdims=True)
        factor = jnp.exp2(m8 - top)
        total = jnp.sum(l8 * factor, axis=0, keepdims=True)
        return factor, total, LN2 * top + jnp.log(total)

    lane = lax.broadcasted_iota(jnp.int32, (1, LANE), 1)
    line = jnp.zeros((1, LANE), jnp.float32)
    for s in range(STUDENTS):
        _, _, s_lse = merged(state[SM + s], state[SL + s])
        value = 2.0 * s_lse
        for c in range(2):
            p = 2 * s + c
            factor, total, t_lse = merged(state[p], state[TL + p])
            cross = jnp.sum(state[TC + p] * factor, axis=0, keepdims=True)
            value = value + (LN2 * cross / total - t_lse)
        out[s : s + 1, :] = value
        line = jnp.where(lane == s, jnp.sum(value, axis=1, keepdims=True), line)
    sums[...] = jnp.broadcast_to(line, sums.shape)


def attend(place, table, plan, groups, rows, queries=None, state=None, copies_out=0):
    first = queries is not None
    last = copies_out > 0
    counts = tuple(g.shape[0] for g in groups)
    blocks = plan.shape[1]
    state_shape = jax.ShapeDtypeStruct((STATE, SUB, ROWS), jnp.float32)
    rows_shape = jax.ShapeDtypeStruct((HEADS, ROWS, 2 * DH), jnp.bfloat16)
    if first:
        extra, out_shape = [*queries, rows], (state_shape, rows_shape)
    elif last:
        extra = [rows, state]
        out_shape = (
            jax.ShapeDtypeStruct((STUDENTS, ROWS), jnp.float32),
            jax.ShapeDtypeStruct((copies_out, LANE), jnp.float32),
        )
    else:
        extra, out_shape = [rows, state], state_shape
    extra_specs = [ANY] * (len(PIECES) + 1) + [VMEM] if first else [VMEM, VMEM]
    scratch = [pltpu.VMEM((CHUNK, ROWS, DH), jnp.bfloat16)]
    if first:
        scratch.append(pltpu.VMEM((PAIRS, ROWS, DH), jnp.bfloat16))
        scratch.append(pltpu.VMEM(state_shape.shape, jnp.float32))
    if last:
        scratch.append(pltpu.VMEM(state_shape.shape, jnp.float32))
    scratch.append(pltpu.SMEM((PAIRS,), jnp.int32))
    if first:
        scratch.append(pltpu.SemaphoreType.DMA((len(PIECES) + 1,)))
    return pl.pallas_call(
        functools.partial(attend_kernel, first, last, counts, blocks),
        out_shape=out_shape,
        in_specs=[SMEM] * 3 + [VMEM] * len(groups) + extra_specs,
        out_specs=jax.tree.map(lambda _: VMEM, out_shape),
        scratch_shapes=scratch,
        input_output_aliases={3 + len(groups) + len(extra) - 1: 1} if first else {},
        compiler_params=small(24),
        cost_estimate=pl.CostEstimate(
            flops=blocks * HEADS * 2 * ROWS * ROWS * 2 * DH,
            bytes_accessed=blocks * ROWS * CHUNK * DH * 2,
            transcendentals=blocks * HEADS * ROWS * ROWS,
        ),
        name="attend",
    )(place, table, plan, *groups, *extra)


def shift(n, by):
    return [(i, (i + by) % n) for i in range(n)]


def z_place(ring):
    ring %= 8
    return (ring % 2) * 4 + ring // 2


def z_shift(by):
    return [(z_place(i), z_place(i + by)) for i in range(8)]


def plan_of(blocks):
    return jnp.array([list(row) for row in zip(*blocks)], jnp.int32)


def program(teacher_query, teacher_key, student_query, student_key, pair_table):
    head = lax.axis_index("head")
    table = pair_table.T
    place = jnp.stack([head, lax.axis_index("kv_0"), lax.axis_index("kv_1")])[None]

    along_x = lambda a, by: lax.ppermute(a, "kv_1", shift(4, by))
    along_z = lambda a, by: lax.ppermute(a, ("head", "kv_0"), z_shift(by))
    other_side = [(0, 1), (1, 0)]

    ring = {0: split_heads(teacher_key[0], student_key[0])}
    *chosen, count = queries_for_other(place, table, teacher_query[0])
    ring[1] = along_z(ring[0], 1)
    ring[7] = along_z(ring[0], -1)
    pieces = [lax.ppermute(piece, "head", other_side) for piece in chosen[:-1]]
    more = lax.cond(
        count[0, 0] > SENT,
        lambda q: lax.ppermute(q, "head", other_side),
        lambda q: q,
        chosen[-1],
    )
    more, ring[1], ring[7] = lax.optimization_barrier((more, ring[1], ring[7]))
    rows = prepare(place, table, teacher_query[0], student_query[0])
    mine = chunks_of(place, ring, (0,))
    near_a = along_x(mine, 1)
    near_b = along_x(mine, -1)
    near_c = along_x(near_a, 1)
    for step in range(2, 5):
        ring[step] = along_z(ring[step - 1], 1)
        if step < 4:
            ring[8 - step] = along_z(ring[9 - step], -1)

    rest_13 = chunks_of(place, ring, (1, 3))
    left_13 = along_x(rest_13, 1)
    right_13 = along_x(rest_13, -1)
    rest_2 = chunks_of(place, ring, (2,))
    left_2 = along_x(rest_2, 1)
    right_2 = along_x(rest_2, -1)
    state, rows = attend(
        place,
        table,
        plan_of([(0, 0), (0, -1), (0, 1), (0, 2), (1, 0), (3, 0), (2, 0)]),
        [mine, near_a, near_b, near_c, rest_13, rest_2],
        rows,
        queries=(*pieces, more),
    )
    left_13, right_13, state = lax.optimization_barrier((left_13, right_13, state))
    cut_1 = left_13[:CHUNK]
    cut_3 = right_13[CHUNK:]
    far_1 = along_x(cut_1, 1)
    far_3 = along_x(cut_3, -1)
    left_2, right_2, state = lax.optimization_barrier((left_2, right_2, state))
    far_2 = along_x(left_2, 1)
    state = attend(
        place,
        table,
        plan_of([(1, -1), (3, -1), (1, 1), (3, 1), (2, -1), (2, 1)]),
        [left_13, right_13, left_2, right_2],
        rows,
        state=state,
    )
    everyone = ("dp_0", "dp_1", "kv_0", "kv_1")
    devices = lax.axis_size(everyone)
    kl, sums = attend(
        place,
        table,
        plan_of([(1, 2), (3, 2), (2, 2)]),
        [far_1, far_3, far_2],
        rows,
        state=state,
        copies_out=devices,
    )
    terms = lax.all_to_all(sums, everyone, 0, 0, tiled=True)
    head_loss = jnp.sum(terms, axis=0)[:STUDENTS] / (devices * ROWS)
    return (kl[None], head_loss)


def solution(mesh):
    split = Mesh(
        mesh.devices.reshape(4, 2, mesh.shape["head"], 4, 4),
        ("dp_0", "dp_1", "head", "kv_0", "kv_1"),
    )
    in_specs = (P(DP, KV, "head"), P(DP, KV, "head"), P(DP, KV, "head"), P(DP, KV, "head"), P())
    out_specs = (P(DP, "head", KV), P("head"))
    return jax.shard_map(
        program, mesh=split, in_specs=in_specs, out_specs=out_specs, check_vma=False
    )
```

```python
import functools
import math

import jax
import jax.numpy as jnp
from jax import lax
from jax.experimental import pallas as pl
from jax.experimental.pallas import tpu as pltpu
from jax.sharding import Mesh
from jax.sharding import PartitionSpec as P


HT = 28
KVT = 4
DH = 128
ROWS = 256
PAIRS = 14
STUDENTS = 7
HEADS = PAIRS + STUDENTS
GROUP = HT // KVT
KV = ("kv_0", "kv_1")
DP = ("dp_0", "dp_1")
LANE = 128
SUB = 8
MASKED = -1e30
LARGE = 2.0**100
LN2 = math.log(2.0)
KAPPA = 1.0 / (LN2 * math.sqrt(DH))
STATE = 3 * PAIRS + 2 * STUDENTS
TL, TC, SM, SL = PAIRS, 2 * PAIRS, 3 * PAIRS, 3 * PAIRS + STUDENTS
OWN = 3
OTHER = 2
CHUNK = OWN + OTHER
PIECES = (4, 5)
SENT = sum(PIECES)
MIB = 1024 * 1024
SMEM = pl.BlockSpec(memory_space=pltpu.SMEM)
VMEM = pl.BlockSpec(memory_space=pltpu.VMEM)
ANY = pl.BlockSpec(memory_space=pl.ANY)
HBM = pl.BlockSpec(memory_space=pltpu.HBM)


def heads_of(n):
    return jax.ShapeDtypeStruct((n, ROWS, DH), jnp.bfloat16)


def small(limit):
    return pltpu.CompilerParams(vmem_limit_bytes=limit * MIB)


def run_all(copies):
    for c in copies:
        c.start()
    for c in copies:
        c.wait()


def split_kernel(teacher, student, out, sems):
    run_all(
        [
            pltpu.make_async_copy(teacher.at[:, pl.ds(0, DH)], out.at[0], sems.at[0]),
            pltpu.make_async_copy(teacher.at[:, pl.ds(DH, DH)], out.at[1], sems.at[1]),
            pltpu.make_async_copy(student, out.at[2], sems.at[2]),
        ]
    )


def split_heads(teacher, student):
    return pl.pallas_call(
        split_kernel,
        out_shape=heads_of(OWN),
        in_specs=[HBM, HBM],
        out_specs=VMEM,
        scratch_shapes=[pltpu.SemaphoreType.DMA((3,))],
        compiler_params=small(2),
        name="split_heads",
    )(teacher, student)


def queries_kernel(place, table, query, *refs):
    pieces, (count, sent, sems) = refs[:-3], refs[-3:]
    head = place[0, 0]
    theirs = (1 - head) * STUDENTS

    def each(act):
        rank = jnp.int32(0)
        for p in range(PAIRS):
            teacher = table[p % 2, theirs + p // 2]
            mine = lax.div(teacher, PAIRS) == head
            lanes = pl.ds(pl.multiple_of(lax.rem(teacher, PAIRS) * DH, DH), DH)

            @pl.when(mine)
            def _():
                act(pltpu.make_async_copy(query.at[:, lanes], sent.at[rank], sems.at[p]))

            rank = rank + mine.astype(jnp.int32)
        return rank

    count[0, 0] = each(lambda c: c.start())
    each(lambda c: c.wait())
    rank = 0
    for piece in pieces:
        piece[...] = sent[rank : rank + piece.shape[0]]
        rank += piece.shape[0]


def queries_for_other(place, table, query):
    return pl.pallas_call(
        queries_kernel,
        out_shape=(
            *(heads_of(n) for n in (*PIECES, PAIRS - SENT)),
            jax.ShapeDtypeStruct((1, 1), jnp.int32),
        ),
        in_specs=[SMEM, SMEM, ANY],
        out_specs=(*[VMEM] * (len(PIECES) + 1), SMEM),
        scratch_shapes=[
            pltpu.VMEM((PAIRS, ROWS, DH), jnp.bfloat16),
            pltpu.SemaphoreType.DMA((PAIRS,)),
        ],
        compiler_params=small(4),
        name="queries_for_other",
    )(place, table, query)


def chunks_kernel(place, *refs):
    ring, out = refs[:-1], refs[-1]
    for head in range(2):

        @pl.when(place[0, 0] == head)
        def _():
            for n in range(len(ring) // 3):
                own, other = ring[3 * n], ring[3 * n + 1 + head]
                out[CHUNK * n : CHUNK * n + OWN] = own[...]
                out[CHUNK * n + OWN : CHUNK * (n + 1)] = other[:OTHER]


def chunks_of(place, ring, chunks):
    parts = [ring[o % 8] for m in chunks for o in (2 * m, 2 * m - 1, 2 * m + 1)]
    return pl.pallas_call(
        chunks_kernel,
        out_shape=heads_of(CHUNK * len(chunks)),
        in_specs=[SMEM] + [VMEM] * len(parts),
        out_specs=VMEM,
        compiler_params=small(4),
        name="chunks_of",
    )(place, *parts)


def scaled(q):
    q = q.astype(jnp.float32) * KAPPA
    high = q.astype(jnp.bfloat16)
    low = (q - high.astype(jnp.float32)).astype(jnp.bfloat16)
    return jnp.concatenate([high, low], axis=1)


def prepare_kernel(place, table, own, student, rows):
    head = place[0, 0]
    for s in range(STUDENTS):
        rows[PAIRS + s] = scaled(student[:, s * DH : (s + 1) * DH])
    for p in range(PAIRS):
        teacher = table[p % 2, head * STUDENTS + p // 2]
        lanes = pl.ds(pl.multiple_of(lax.rem(teacher, PAIRS) * DH, DH), DH)

        @pl.when(lax.div(teacher, PAIRS) == head)
        def _():
            rows[p] = scaled(own[:, lanes])


def prepare(place, table, own, student):
    return pl.pallas_call(
        prepare_kernel,
        out_shape=jax.ShapeDtypeStruct((HEADS, ROWS, 2 * DH), jnp.bfloat16),
        in_specs=[SMEM, SMEM, VMEM, VMEM],
        out_specs=VMEM,
        compiler_params=small(8),
        cost_estimate=pl.CostEstimate(
            flops=HEADS * ROWS * DH * 64, bytes_accessed=HEADS * ROWS * DH * 6, transcendentals=0
        ),
        name="prepare",
    )(place, table, own, student)


def fill_received(place, table, received, rows):
    head = place[0, 0]
    rank = jnp.int32(0)
    for p in range(PAIRS):
        mine = lax.div(table[p % 2, head * STUDENTS + p // 2], PAIRS) == head

        @pl.when(jnp.logical_not(mine))
        def _():
            rows[p] = scaled(received[rank])

        rank = rank + 1 - mine.astype(jnp.int32)


def attend_kernel(first, last, counts, blocks, place, table, plan, *refs):
    refs = list(refs)
    take = lambda n: [refs.pop(0) for _ in range(n)]
    groups = take(len(counts))
    if first:
        pieces = take(len(PIECES) + 1)
        take(1)
        state, rows = take(2)
    else:
        rows, before = take(2)
        if last:
            out, sums = take(2)
        else:
            (state,) = take(1)
    (keys,) = take(1)
    if first:
        received, entry = take(2)
    if last:
        (state,) = take(1)
    offsets = refs[0]
    if first:
        sems = refs[1]
    head, z_hi, x = place[0, 0], place[0, 1], place[0, 2]
    row_block = z_hi * 4 + x

    if first:
        inputs = []
        rank = 0
        for n, piece in enumerate(pieces):
            length = piece.shape[0]
            inputs.append(
                pltpu.make_async_copy(
                    piece, received.at[pl.ds(rank, length)], sems.at[n]
                )
            )
            rank += length
        for c in inputs:
            c.start()
        for c in inputs:
            c.wait()
        fill_received(place, table, received, rows)
    else:
        entry = before
        state[...] = before[...]

    for p in range(PAIRS):
        kv_head = lax.div(table[p % 2, head * STUDENTS + p // 2], GROUP)
        side = jnp.where(lax.div(kv_head, 2) == head, 0, OWN)
        offsets[p] = side + lax.rem(kv_head, 2)

    def place_keys(i):
        at = 0
        for g, n in enumerate(counts):
            if n % CHUNK == 0:
                lo = at // CHUNK

                @pl.when(jnp.logical_and(i >= lo, i < lo + n // CHUNK))
                def _():
                    keys[...] = groups[g][pl.ds((i - lo) * CHUNK, CHUNK)]

            else:
                inside = at % CHUNK

                @pl.when(i == at // CHUNK)
                def _():
                    keys[inside : inside + n] = groups[g][...]

            at += n

    def product(k, p):
        return lax.dot_general(
            jnp.concatenate([k, k], axis=1),
            rows[p],
            (((1,), (1,)), ((), ())),
            preferred_element_type=jnp.float32,
        )

    def folded(a):
        return a.reshape(ROWS // SUB, SUB, ROWS)

    def own_block():
        key_pos = lax.broadcasted_iota(jnp.int32, (ROWS, ROWS), 0)
        row_pos = lax.broadcasted_iota(jnp.int32, (ROWS, ROWS), 1)
        mask = key_pos <= row_pos

        def begin(logits, m_index, l_index):
            logits = jnp.where(mask, logits, MASKED)
            top = jnp.max(logits, axis=0, keepdims=True)
            weights = folded(jnp.exp2(logits - top))
            state[m_index] = jnp.broadcast_to(top, (SUB, ROWS))
            state[l_index] = jnp.sum(weights, axis=0)
            return weights

        for s in range(STUDENTS):
            zs = product(keys[2], PAIRS + s)
            begin(zs, SM + s, SL + s)
            for c in range(2):
                p = 2 * s + c
                zt = product(keys[offsets[p]], p)
                weights = begin(zt, p, TL + p)
                state[TC + p] = jnp.sum(weights * folded(zt - zs), axis=0)

    def block():
        def add(logits, m_index, l_index):
            weights = jnp.exp2(folded(logits) - state[m_index][None])
            state[l_index] = state[l_index] + jnp.sum(weights, axis=0)
            return weights

        student_keys = keys[2]
        for s in range(STUDENTS):
            zs = product(student_keys, PAIRS + s)
            add(zs, SM + s, SL + s)
            for c in range(2):
                p = 2 * s + c
                zt = product(keys[offsets[p]], p)
                weights = add(zt, p, TL + p)
                state[TC + p] = state[TC + p] + jnp.sum(weights * folded(zt - zs), axis=0)

    def exact_block():
        def add(logits, m_index, l_index):
            logits = folded(logits)
            old = state[m_index]
            new = jnp.maximum(old, jnp.max(logits, axis=0))
            weights = jnp.exp2(logits - new[None])
            rescale = jnp.exp2(old - new)
            state[m_index] = new
            state[l_index] = state[l_index] * rescale + jnp.sum(weights, axis=0)
            return weights, rescale

        def student(s, carry):
            zs = product(keys[2], PAIRS + s)
            add(zs, SM + s, SL + s)
            for c in range(2):
                p = 2 * s + c
                zt = product(keys[offsets[p]], p)
                weights, rescale = add(zt, p, TL + p)
                cross = jnp.sum(weights * folded(zt - zs), axis=0)
                state[TC + p] = state[TC + p] * rescale + cross
            return carry

        lax.fori_loop(0, STUDENTS, student, 0)

    def visible(i):
        chunk = lax.bitwise_and(z_hi - plan[0, i], 3)
        return chunk * 4 + lax.bitwise_and(x + plan[1, i], 3) < row_block

    def step(i, carry):
        @pl.when(visible(i))
        def _():
            place_keys(i)
            block()

        return carry

    def exact_step(i, carry):
        @pl.when(visible(i))
        def _():
            place_keys(i)
            exact_block()

        return carry

    if first:
        keys[...] = groups[0][...]
        own_block()
        entry[...] = state[...]
    lax.fori_loop(int(first), blocks, step, 0)

    largest = jnp.maximum(
        jnp.max(state[TL : TL + PAIRS]), jnp.max(state[SL : SL + STUDENTS])
    )

    @pl.when(largest > LARGE)
    def _():
        state[...] = entry[...]
        lax.fori_loop(int(first), blocks, exact_step, 0)

    if not last:
        return

    def merged(m8, l8):
        top = jnp.max(m8, axis=0, keepdims=True)
        factor = jnp.exp2(m8 - top)
        total = jnp.sum(l8 * factor, axis=0, keepdims=True)
        return factor, total, LN2 * top + jnp.log(total)

    lane = lax.broadcasted_iota(jnp.int32, (1, LANE), 1)
    line = jnp.zeros((1, LANE), jnp.float32)
    for s in range(STUDENTS):
        _, _, s_lse = merged(state[SM + s], state[SL + s])
        value = 2.0 * s_lse
        for c in range(2):
            p = 2 * s + c
            factor, total, t_lse = merged(state[p], state[TL + p])
            cross = jnp.sum(state[TC + p] * factor, axis=0, keepdims=True)
            value = value + (LN2 * cross / total - t_lse)
        out[s : s + 1, :] = value
        line = jnp.where(lane == s, jnp.sum(value, axis=1, keepdims=True), line)
    sums[...] = jnp.broadcast_to(line, sums.shape)


def attend(place, table, plan, groups, rows, queries=None, state=None, copies_out=0):
    first = queries is not None
    last = copies_out > 0
    counts = tuple(g.shape[0] for g in groups)
    blocks = plan.shape[1]
    state_shape = jax.ShapeDtypeStruct((STATE, SUB, ROWS), jnp.float32)
    rows_shape = jax.ShapeDtypeStruct((HEADS, ROWS, 2 * DH), jnp.bfloat16)
    if first:
        extra, out_shape = [*queries, rows], (state_shape, rows_shape)
    elif last:
        extra = [rows, state]
        out_shape = (
            jax.ShapeDtypeStruct((STUDENTS, ROWS), jnp.float32),
            jax.ShapeDtypeStruct((copies_out, LANE), jnp.float32),
        )
    else:
        extra, out_shape = [rows, state], state_shape
    extra_specs = [ANY] * (len(PIECES) + 1) + [VMEM] if first else [VMEM, VMEM]
    scratch = [pltpu.VMEM((CHUNK, ROWS, DH), jnp.bfloat16)]
    if first:
        scratch.append(pltpu.VMEM((PAIRS, ROWS, DH), jnp.bfloat16))
        scratch.append(pltpu.VMEM(state_shape.shape, jnp.float32))
    if last:
        scratch.append(pltpu.VMEM(state_shape.shape, jnp.float32))
    scratch.append(pltpu.SMEM((PAIRS,), jnp.int32))
    if first:
        scratch.append(pltpu.SemaphoreType.DMA((len(PIECES) + 1,)))
    return pl.pallas_call(
        functools.partial(attend_kernel, first, last, counts, blocks),
        out_shape=out_shape,
        in_specs=[SMEM] * 3 + [VMEM] * len(groups) + extra_specs,
        out_specs=jax.tree.map(lambda _: VMEM, out_shape),
        scratch_shapes=scratch,
        input_output_aliases={3 + len(groups) + len(extra) - 1: 1} if first else {},
        compiler_params=small(24),
        cost_estimate=pl.CostEstimate(
            flops=blocks * HEADS * 2 * ROWS * ROWS * 2 * DH,
            bytes_accessed=blocks * ROWS * CHUNK * DH * 2,
            transcendentals=blocks * HEADS * ROWS * ROWS,
        ),
        name="attend",
    )(place, table, plan, *groups, *extra)


def shift(n, by):
    return [(i, (i + by) % n) for i in range(n)]


def z_place(ring):
    ring %= 8
    return (ring % 2) * 4 + ring // 2


def z_shift(by):
    return [(z_place(i), z_place(i + by)) for i in range(8)]


def plan_of(blocks):
    return jnp.array([list(row) for row in zip(*blocks)], jnp.int32)


def program(teacher_query, teacher_key, student_query, student_key, pair_table):
    head = lax.axis_index("head")
    table = pair_table.T
    place = jnp.stack([head, lax.axis_index("kv_0"), lax.axis_index("kv_1")])[None]

    along_x = lambda a, by: lax.ppermute(a, "kv_1", shift(4, by))
    along_z = lambda a, by: lax.ppermute(a, ("head", "kv_0"), z_shift(by))
    other_side = [(0, 1), (1, 0)]

    ring = {0: split_heads(teacher_key[0], student_key[0])}
    *chosen, count = queries_for_other(place, table, teacher_query[0])
    ring[1] = along_z(ring[0], 1)
    ring[7] = along_z(ring[0], -1)
    pieces = [lax.ppermute(piece, "head", other_side) for piece in chosen[:-1]]
    more = lax.cond(
        count[0, 0] > SENT,
        lambda q: lax.ppermute(q, "head", other_side),
        lambda q: q,
        chosen[-1],
    )
    more, ring[1], ring[7] = lax.optimization_barrier((more, ring[1], ring[7]))
    rows = prepare(place, table, teacher_query[0], student_query[0])
    mine = chunks_of(place, ring, (0,))
    near_a = along_x(mine, 1)
    near_b = along_x(mine, -1)
    near_c = along_x(near_a[:OTHER], 1)
    near_d = along_x(near_b[OTHER:], -1)
    for step in range(2, 5):
        ring[step] = along_z(ring[step - 1], 1)
        if step < 4:
            ring[8 - step] = along_z(ring[9 - step], -1)

    rest_13 = chunks_of(place, ring, (1, 3))
    left_13 = along_x(rest_13, 1)
    right_13 = along_x(rest_13, -1)
    rest_2 = chunks_of(place, ring, (2,))
    left_2 = along_x(rest_2, 1)
    right_2 = along_x(rest_2, -1)
    state, rows = attend(
        place,
        table,
        plan_of([(0, 0), (0, -1), (0, 1), (0, 2), (1, 0), (3, 0)]),
        [mine, near_a, near_b, near_c, near_d, rest_13],
        rows,
        queries=(*pieces, more),
    )
    left_13, right_13, state = lax.optimization_barrier((left_13, right_13, state))
    cut_1 = left_13[:CHUNK]
    cut_3 = right_13[CHUNK:]
    far_1 = along_x(cut_1, 1)
    far_3 = along_x(cut_3, -1)
    left_2, right_2, state = lax.optimization_barrier((left_2, right_2, state))
    far_2 = along_x(left_2, 1)
    state = attend(
        place,
        table,
        plan_of([(1, -1), (3, -1), (1, 1), (3, 1), (2, -1), (2, 1), (2, 0)]),
        [left_13, right_13, left_2, right_2, rest_2],
        rows,
        state=state,
    )
    everyone = ("dp_0", "dp_1", "kv_0", "kv_1")
    devices = lax.axis_size(everyone)
    kl, sums = attend(
        place,
        table,
        plan_of([(1, 2), (3, 2), (2, 2)]),
        [far_1, far_3, far_2],
        rows,
        state=state,
        copies_out=devices,
    )
    terms = lax.all_to_all(sums, everyone, 0, 0, tiled=True)
    head_loss = jnp.sum(terms, axis=0)[:STUDENTS] / (devices * ROWS)
    return (kl[None], head_loss)


def solution(mesh):
    split = Mesh(
        mesh.devices.reshape(4, 2, mesh.shape["head"], 4, 4),
        ("dp_0", "dp_1", "head", "kv_0", "kv_1"),
    )
    in_specs = (P(DP, KV, "head"), P(DP, KV, "head"), P(DP, KV, "head"), P(DP, KV, "head"), P())
    out_specs = (P(DP, "head", KV), P("head"))
    return jax.shard_map(
        program, mesh=split, in_specs=in_specs, out_specs=out_specs, check_vma=False
    )
```

```python
import functools
import math

import jax
import jax.numpy as jnp
from jax import lax
from jax.experimental import pallas as pl
from jax.experimental.pallas import tpu as pltpu
from jax.sharding import Mesh
from jax.sharding import PartitionSpec as P


HT = 28
KVT = 4
DH = 128
ROWS = 256
PAIRS = 14
STUDENTS = 7
HEADS = PAIRS + STUDENTS
GROUP = HT // KVT
KV = ("kv_0", "kv_1")
DP = ("dp_0", "dp_1")
LANE = 128
SUB = 8
MASKED = -1e30
LARGE = 2.0**100
LN2 = math.log(2.0)
KAPPA = 1.0 / (LN2 * math.sqrt(DH))
STATE = 3 * PAIRS + 2 * STUDENTS
TL, TC, SM, SL = PAIRS, 2 * PAIRS, 3 * PAIRS, 3 * PAIRS + STUDENTS
OWN = 3
OTHER = 2
CHUNK = OWN + OTHER
PIECES = (4, 5)
SENT = sum(PIECES)
MIB = 1024 * 1024
SMEM = pl.BlockSpec(memory_space=pltpu.SMEM)
VMEM = pl.BlockSpec(memory_space=pltpu.VMEM)
ANY = pl.BlockSpec(memory_space=pl.ANY)
HBM = pl.BlockSpec(memory_space=pltpu.HBM)


def heads_of(n):
    return jax.ShapeDtypeStruct((n, ROWS, DH), jnp.bfloat16)


def small(limit):
    return pltpu.CompilerParams(vmem_limit_bytes=limit * MIB)


def run_all(copies):
    for c in copies:
        c.start()
    for c in copies:
        c.wait()


def split_kernel(teacher, student, out, sems):
    run_all(
        [
            pltpu.make_async_copy(teacher.at[:, pl.ds(0, DH)], out.at[0], sems.at[0]),
            pltpu.make_async_copy(teacher.at[:, pl.ds(DH, DH)], out.at[1], sems.at[1]),
            pltpu.make_async_copy(student, out.at[2], sems.at[2]),
        ]
    )


def split_heads(teacher, student):
    return pl.pallas_call(
        split_kernel,
        out_shape=heads_of(OWN),
        in_specs=[HBM, HBM],
        out_specs=VMEM,
        scratch_shapes=[pltpu.SemaphoreType.DMA((3,))],
        compiler_params=small(2),
        name="split_heads",
    )(teacher, student)


def queries_kernel(place, table, query, *refs):
    pieces, (count, sent, sems) = refs[:-3], refs[-3:]
    head = place[0, 0]
    theirs = (1 - head) * STUDENTS

    def each(act):
        rank = jnp.int32(0)
        for p in range(PAIRS):
            teacher = table[p % 2, theirs + p // 2]
            mine = lax.div(teacher, PAIRS) == head
            lanes = pl.ds(pl.multiple_of(lax.rem(teacher, PAIRS) * DH, DH), DH)

            @pl.when(mine)
            def _():
                act(pltpu.make_async_copy(query.at[:, lanes], sent.at[rank], sems.at[p]))

            rank = rank + mine.astype(jnp.int32)
        return rank

    count[0, 0] = each(lambda c: c.start())
    each(lambda c: c.wait())
    rank = 0
    for piece in pieces:
        piece[...] = sent[rank : rank + piece.shape[0]]
        rank += piece.shape[0]


def queries_for_other(place, table, query):
    return pl.pallas_call(
        queries_kernel,
        out_shape=(
            *(heads_of(n) for n in (*PIECES, PAIRS - SENT)),
            jax.ShapeDtypeStruct((1, 1), jnp.int32),
        ),
        in_specs=[SMEM, SMEM, ANY],
        out_specs=(*[VMEM] * (len(PIECES) + 1), SMEM),
        scratch_shapes=[
            pltpu.VMEM((PAIRS, ROWS, DH), jnp.bfloat16),
            pltpu.SemaphoreType.DMA((PAIRS,)),
        ],
        compiler_params=small(4),
        name="queries_for_other",
    )(place, table, query)


def chunks_kernel(place, *refs):
    ring, out = refs[:-1], refs[-1]
    for head in range(2):

        @pl.when(place[0, 0] == head)
        def _():
            for n in range(len(ring) // 3):
                own, other = ring[3 * n], ring[3 * n + 1 + head]
                out[CHUNK * n : CHUNK * n + OWN] = own[...]
                out[CHUNK * n + OWN : CHUNK * (n + 1)] = other[:OTHER]


def chunks_of(place, ring, chunks):
    parts = [ring[o % 8] for m in chunks for o in (2 * m, 2 * m - 1, 2 * m + 1)]
    return pl.pallas_call(
        chunks_kernel,
        out_shape=heads_of(CHUNK * len(chunks)),
        in_specs=[SMEM] + [VMEM] * len(parts),
        out_specs=VMEM,
        compiler_params=small(4),
        name="chunks_of",
    )(place, *parts)


def scaled(q):
    q = q.astype(jnp.float32) * KAPPA
    high = q.astype(jnp.bfloat16)
    low = (q - high.astype(jnp.float32)).astype(jnp.bfloat16)
    return jnp.concatenate([high, low], axis=1)


def prepare_kernel(place, table, own, student, rows):
    head = place[0, 0]
    for s in range(STUDENTS):
        rows[PAIRS + s] = scaled(student[:, s * DH : (s + 1) * DH])
    for p in range(PAIRS):
        teacher = table[p % 2, head * STUDENTS + p // 2]
        lanes = pl.ds(pl.multiple_of(lax.rem(teacher, PAIRS) * DH, DH), DH)

        @pl.when(lax.div(teacher, PAIRS) == head)
        def _():
            rows[p] = scaled(own[:, lanes])


def prepare(place, table, own, student):
    return pl.pallas_call(
        prepare_kernel,
        out_shape=jax.ShapeDtypeStruct((HEADS, ROWS, 2 * DH), jnp.bfloat16),
        in_specs=[SMEM, SMEM, VMEM, VMEM],
        out_specs=VMEM,
        compiler_params=small(8),
        cost_estimate=pl.CostEstimate(
            flops=HEADS * ROWS * DH * 64, bytes_accessed=HEADS * ROWS * DH * 6, transcendentals=0
        ),
        name="prepare",
    )(place, table, own, student)


def fill_received(place, table, received, rows):
    head = place[0, 0]
    rank = jnp.int32(0)
    for p in range(PAIRS):
        mine = lax.div(table[p % 2, head * STUDENTS + p // 2], PAIRS) == head

        @pl.when(jnp.logical_not(mine))
        def _():
            rows[p] = scaled(received[rank])

        rank = rank + 1 - mine.astype(jnp.int32)


def attend_kernel(first, last, counts, blocks, place, table, plan, *refs):
    refs = list(refs)
    take = lambda n: [refs.pop(0) for _ in range(n)]
    groups = take(len(counts))
    if first:
        pieces = take(len(PIECES) + 1)
        take(1)
        state, rows = take(2)
    else:
        rows, before = take(2)
        if last:
            out, sums = take(2)
        else:
            (state,) = take(1)
    (keys,) = take(1)
    if first:
        received, entry = take(2)
    if last:
        (state,) = take(1)
    offsets = refs[0]
    if first:
        sems = refs[1]
    head, z_hi, x = place[0, 0], place[0, 1], place[0, 2]
    row_block = z_hi * 4 + x

    if first:
        inputs = []
        rank = 0
        for n, piece in enumerate(pieces):
            length = piece.shape[0]
            inputs.append(
                pltpu.make_async_copy(
                    piece, received.at[pl.ds(rank, length)], sems.at[n]
                )
            )
            rank += length
        for c in inputs:
            c.start()
        for c in inputs:
            c.wait()
        fill_received(place, table, received, rows)
    else:
        entry = before
        state[...] = before[...]

    for p in range(PAIRS):
        kv_head = lax.div(table[p % 2, head * STUDENTS + p // 2], GROUP)
        side = jnp.where(lax.div(kv_head, 2) == head, 0, OWN)
        offsets[p] = side + lax.rem(kv_head, 2)

    def place_keys(i):
        at = 0
        for g, n in enumerate(counts):
            if n % CHUNK == 0:
                lo = at // CHUNK

                @pl.when(jnp.logical_and(i >= lo, i < lo + n // CHUNK))
                def _():
                    keys[...] = groups[g][pl.ds((i - lo) * CHUNK, CHUNK)]

            else:
                inside = at % CHUNK

                @pl.when(i == at // CHUNK)
                def _():
                    keys[inside : inside + n] = groups[g][...]

            at += n

    def product(k, p):
        return lax.dot_general(
            jnp.concatenate([k, k], axis=1),
            rows[p],
            (((1,), (1,)), ((), ())),
            preferred_element_type=jnp.float32,
        )

    def folded(a):
        return a.reshape(ROWS // SUB, SUB, ROWS)

    def own_block():
        key_pos = lax.broadcasted_iota(jnp.int32, (ROWS, ROWS), 0)
        row_pos = lax.broadcasted_iota(jnp.int32, (ROWS, ROWS), 1)
        mask = key_pos <= row_pos

        def begin(logits, m_index, l_index):
            logits = jnp.where(mask, logits, MASKED)
            top = jnp.max(logits, axis=0, keepdims=True)
            weights = folded(jnp.exp2(logits - top))
            state[m_index] = jnp.broadcast_to(top, (SUB, ROWS))
            state[l_index] = jnp.sum(weights, axis=0)
            return weights

        for s in range(STUDENTS):
            zs = product(keys[2], PAIRS + s)
            begin(zs, SM + s, SL + s)
            for c in range(2):
                p = 2 * s + c
                zt = product(keys[offsets[p]], p)
                weights = begin(zt, p, TL + p)
                state[TC + p] = jnp.sum(weights * folded(zt - zs), axis=0)

    def block():
        def add(logits, m_index, l_index):
            weights = jnp.exp2(folded(logits) - state[m_index][None])
            state[l_index] = state[l_index] + jnp.sum(weights, axis=0)
            return weights

        student_keys = keys[2]
        for s in range(STUDENTS):
            zs = product(student_keys, PAIRS + s)
            add(zs, SM + s, SL + s)
            for c in range(2):
                p = 2 * s + c
                zt = product(keys[offsets[p]], p)
                weights = add(zt, p, TL + p)
                state[TC + p] = state[TC + p] + jnp.sum(weights * folded(zt - zs), axis=0)

    def exact_block():
        def add(logits, m_index, l_index):
            logits = folded(logits)
            old = state[m_index]
            new = jnp.maximum(old, jnp.max(logits, axis=0))
            weights = jnp.exp2(logits - new[None])
            rescale = jnp.exp2(old - new)
            state[m_index] = new
            state[l_index] = state[l_index] * rescale + jnp.sum(weights, axis=0)
            return weights, rescale

        def student(s, carry):
            zs = product(keys[2], PAIRS + s)
            add(zs, SM + s, SL + s)
            for c in range(2):
                p = 2 * s + c
                zt = product(keys[offsets[p]], p)
                weights, rescale = add(zt, p, TL + p)
                cross = jnp.sum(weights * folded(zt - zs), axis=0)
                state[TC + p] = state[TC + p] * rescale + cross
            return carry

        lax.fori_loop(0, STUDENTS, student, 0)

    def visible(i):
        chunk = lax.bitwise_and(z_hi - plan[0, i], 3)
        return chunk * 4 + lax.bitwise_and(x + plan[1, i], 3) < row_block

    def step(i, carry):
        @pl.when(visible(i))
        def _():
            place_keys(i)
            block()

        return carry

    def exact_step(i, carry):
        @pl.when(visible(i))
        def _():
            place_keys(i)
            exact_block()

        return carry

    if first:
        keys[...] = groups[0][...]
        own_block()
        entry[...] = state[...]
    lax.fori_loop(int(first), blocks, step, 0)

    largest = jnp.maximum(
        jnp.max(state[TL : TL + PAIRS]), jnp.max(state[SL : SL + STUDENTS])
    )

    @pl.when(largest > LARGE)
    def _():
        state[...] = entry[...]
        lax.fori_loop(int(first), blocks, exact_step, 0)

    if not last:
        return

    def merged(m8, l8):
        top = jnp.max(m8, axis=0, keepdims=True)
        factor = jnp.exp2(m8 - top)
        total = jnp.sum(l8 * factor, axis=0, keepdims=True)
        return factor, total, LN2 * top + jnp.log(total)

    lane = lax.broadcasted_iota(jnp.int32, (1, LANE), 1)
    line = jnp.zeros((1, LANE), jnp.float32)
    for s in range(STUDENTS):
        _, _, s_lse = merged(state[SM + s], state[SL + s])
        value = 2.0 * s_lse
        for c in range(2):
            p = 2 * s + c
            factor, total, t_lse = merged(state[p], state[TL + p])
            cross = jnp.sum(state[TC + p] * factor, axis=0, keepdims=True)
            value = value + (LN2 * cross / total - t_lse)
        out[s : s + 1, :] = value
        line = jnp.where(lane == s, jnp.sum(value, axis=1, keepdims=True), line)
    sums[...] = jnp.broadcast_to(line, sums.shape)


def attend(place, table, plan, groups, rows, queries=None, state=None, copies_out=0):
    first = queries is not None
    last = copies_out > 0
    counts = tuple(g.shape[0] for g in groups)
    blocks = plan.shape[1]
    state_shape = jax.ShapeDtypeStruct((STATE, SUB, ROWS), jnp.float32)
    rows_shape = jax.ShapeDtypeStruct((HEADS, ROWS, 2 * DH), jnp.bfloat16)
    if first:
        extra, out_shape = [*queries, rows], (state_shape, rows_shape)
    elif last:
        extra = [rows, state]
        out_shape = (
            jax.ShapeDtypeStruct((STUDENTS, ROWS), jnp.float32),
            jax.ShapeDtypeStruct((copies_out, LANE), jnp.float32),
        )
    else:
        extra, out_shape = [rows, state], state_shape
    extra_specs = [ANY] * (len(PIECES) + 1) + [VMEM] if first else [VMEM, VMEM]
    scratch = [pltpu.VMEM((CHUNK, ROWS, DH), jnp.bfloat16)]
    if first:
        scratch.append(pltpu.VMEM((PAIRS, ROWS, DH), jnp.bfloat16))
        scratch.append(pltpu.VMEM(state_shape.shape, jnp.float32))
    if last:
        scratch.append(pltpu.VMEM(state_shape.shape, jnp.float32))
    scratch.append(pltpu.SMEM((PAIRS,), jnp.int32))
    if first:
        scratch.append(pltpu.SemaphoreType.DMA((len(PIECES) + 1,)))
    return pl.pallas_call(
        functools.partial(attend_kernel, first, last, counts, blocks),
        out_shape=out_shape,
        in_specs=[SMEM] * 3 + [VMEM] * len(groups) + extra_specs,
        out_specs=jax.tree.map(lambda _: VMEM, out_shape),
        scratch_shapes=scratch,
        input_output_aliases={3 + len(groups) + len(extra) - 1: 1} if first else {},
        compiler_params=small(24),
        cost_estimate=pl.CostEstimate(
            flops=blocks * HEADS * 2 * ROWS * ROWS * 2 * DH,
            bytes_accessed=blocks * ROWS * CHUNK * DH * 2,
            transcendentals=blocks * HEADS * ROWS * ROWS,
        ),
        name="attend",
    )(place, table, plan, *groups, *extra)


def shift(n, by):
    return [(i, (i + by) % n) for i in range(n)]


def z_place(ring):
    ring %= 8
    return (ring % 2) * 4 + ring // 2


def z_shift(by):
    return [(z_place(i), z_place(i + by)) for i in range(8)]


def plan_of(blocks):
    return jnp.array([list(row) for row in zip(*blocks)], jnp.int32)


def program(teacher_query, teacher_key, student_query, student_key, pair_table):
    head = lax.axis_index("head")
    table = pair_table.T
    place = jnp.stack([head, lax.axis_index("kv_0"), lax.axis_index("kv_1")])[None]

    along_x = lambda a, by: lax.ppermute(a, "kv_1", shift(4, by))
    along_z = lambda a, by: lax.ppermute(a, ("head", "kv_0"), z_shift(by))
    other_side = [(0, 1), (1, 0)]

    ring = {0: split_heads(teacher_key[0], student_key[0])}
    *chosen, count = queries_for_other(place, table, teacher_query[0])
    ring[1] = along_z(ring[0], 1)
    ring[7] = along_z(ring[0], -1)
    pieces = [lax.ppermute(piece, "head", other_side) for piece in chosen[:-1]]
    more = lax.cond(
        count[0, 0] > SENT,
        lambda q: lax.ppermute(q, "head", other_side),
        lambda q: q,
        chosen[-1],
    )
    more, ring[1], ring[7] = lax.optimization_barrier((more, ring[1], ring[7]))
    rows = prepare(place, table, teacher_query[0], student_query[0])
    mine = chunks_of(place, ring, (0,))
    near_a = along_x(mine, 1)
    near_b = along_x(mine, -1)
    near_c = along_x(near_a[:OTHER], 1)
    near_d = along_x(near_b[OTHER:], -1)
    for step in range(2, 5):
        ring[step] = along_z(ring[step - 1], 1)
        if step < 4:
            ring[8 - step] = along_z(ring[9 - step], -1)

    rest_13 = chunks_of(place, ring, (1, 3))
    left_13 = along_x(rest_13, 1)
    right_13 = along_x(rest_13, -1)
    rest_2 = chunks_of(place, ring, (2,))
    left_2 = along_x(rest_2, 1)
    right_2 = along_x(rest_2, -1)
    state, rows = attend(
        place,
        table,
        plan_of([(0, 0), (0, -1), (0, 1), (0, 2), (1, 0), (3, 0), (2, 0)]),
        [mine, near_a, near_b, near_c, near_d, rest_13, rest_2],
        rows,
        queries=(*pieces, more),
    )
    left_13, right_13, state = lax.optimization_barrier((left_13, right_13, state))
    cut_1 = left_13[:CHUNK]
    cut_3 = right_13[CHUNK:]
    far_1 = along_x(cut_1, 1)
    far_3 = along_x(cut_3, -1)
    left_2, right_2, state = lax.optimization_barrier((left_2, right_2, state))
    far_2a = along_x(left_2[:OTHER], 1)
    far_2b = along_x(right_2[OTHER:], -1)
    state = attend(
        place,
        table,
        plan_of([(1, -1), (3, -1), (1, 1), (3, 1), (2, -1), (2, 1)]),
        [left_13, right_13, left_2, right_2],
        rows,
        state=state,
    )
    everyone = ("dp_0", "dp_1", "kv_0", "kv_1")
    devices = lax.axis_size(everyone)
    kl, sums = attend(
        place,
        table,
        plan_of([(1, 2), (3, 2), (2, 2)]),
        [far_1, far_3, far_2a, far_2b],
        rows,
        state=state,
        copies_out=devices,
    )
    terms = lax.all_to_all(sums, everyone, 0, 0, tiled=True)
    head_loss = jnp.sum(terms, axis=0)[:STUDENTS] / (devices * ROWS)
    return (kl[None], head_loss)


def solution(mesh):
    split = Mesh(
        mesh.devices.reshape(4, 2, mesh.shape["head"], 4, 4),
        ("dp_0", "dp_1", "head", "kv_0", "kv_1"),
    )
    in_specs = (P(DP, KV, "head"), P(DP, KV, "head"), P(DP, KV, "head"), P(DP, KV, "head"), P())
    out_specs = (P(DP, "head", KV), P("head"))
    return jax.shard_map(
        program, mesh=split, in_specs=in_specs, out_specs=out_specs, check_vma=False
    )
```

```python
import functools
import math

import jax
import jax.numpy as jnp
from jax import lax
from jax.experimental import pallas as pl
from jax.experimental.pallas import tpu as pltpu
from jax.sharding import Mesh
from jax.sharding import PartitionSpec as P


HT = 28
KVT = 4
DH = 128
ROWS = 256
PAIRS = 14
STUDENTS = 7
HEADS = PAIRS + STUDENTS
GROUP = HT // KVT
KV = ("kv_0", "kv_1")
DP = ("dp_0", "dp_1")
LANE = 128
SUB = 8
MASKED = -1e30
LARGE = 2.0**100
LN2 = math.log(2.0)
KAPPA = 1.0 / (LN2 * math.sqrt(DH))
STATE = 3 * PAIRS + 2 * STUDENTS
TL, TC, SM, SL = PAIRS, 2 * PAIRS, 3 * PAIRS, 3 * PAIRS + STUDENTS
OWN = 3
OTHER = 2
CHUNK = OWN + OTHER
PIECES = (4, 5)
SENT = sum(PIECES)
MIB = 1024 * 1024
SMEM = pl.BlockSpec(memory_space=pltpu.SMEM)
VMEM = pl.BlockSpec(memory_space=pltpu.VMEM)
ANY = pl.BlockSpec(memory_space=pl.ANY)
HBM = pl.BlockSpec(memory_space=pltpu.HBM)


def heads_of(n):
    return jax.ShapeDtypeStruct((n, ROWS, DH), jnp.bfloat16)


def small(limit):
    return pltpu.CompilerParams(vmem_limit_bytes=limit * MIB)


def run_all(copies):
    for c in copies:
        c.start()
    for c in copies:
        c.wait()


def split_kernel(teacher, student, out, sems):
    run_all(
        [
            pltpu.make_async_copy(teacher.at[:, pl.ds(0, DH)], out.at[0], sems.at[0]),
            pltpu.make_async_copy(teacher.at[:, pl.ds(DH, DH)], out.at[1], sems.at[1]),
            pltpu.make_async_copy(student, out.at[2], sems.at[2]),
        ]
    )


def split_heads(teacher, student):
    return pl.pallas_call(
        split_kernel,
        out_shape=heads_of(OWN),
        in_specs=[HBM, HBM],
        out_specs=VMEM,
        scratch_shapes=[pltpu.SemaphoreType.DMA((3,))],
        compiler_params=small(2),
        name="split_heads",
    )(teacher, student)


def queries_kernel(place, table, query, *refs):
    pieces, (count, sent, sems) = refs[:-3], refs[-3:]
    head = place[0, 0]
    theirs = (1 - head) * STUDENTS

    def each(act):
        rank = jnp.int32(0)
        for p in range(PAIRS):
            teacher = table[p % 2, theirs + p // 2]
            mine = lax.div(teacher, PAIRS) == head
            lanes = pl.ds(pl.multiple_of(lax.rem(teacher, PAIRS) * DH, DH), DH)

            @pl.when(mine)
            def _():
                act(pltpu.make_async_copy(query.at[:, lanes], sent.at[rank], sems.at[p]))

            rank = rank + mine.astype(jnp.int32)
        return rank

    count[0, 0] = each(lambda c: c.start())
    each(lambda c: c.wait())
    rank = 0
    for piece in pieces:
        piece[...] = sent[rank : rank + piece.shape[0]]
        rank += piece.shape[0]


def queries_for_other(place, table, query):
    return pl.pallas_call(
        queries_kernel,
        out_shape=(
            *(heads_of(n) for n in (*PIECES, PAIRS - SENT)),
            jax.ShapeDtypeStruct((1, 1), jnp.int32),
        ),
        in_specs=[SMEM, SMEM, ANY],
        out_specs=(*[VMEM] * (len(PIECES) + 1), SMEM),
        scratch_shapes=[
            pltpu.VMEM((PAIRS, ROWS, DH), jnp.bfloat16),
            pltpu.SemaphoreType.DMA((PAIRS,)),
        ],
        compiler_params=small(4),
        name="queries_for_other",
    )(place, table, query)


def chunks_kernel(place, *refs):
    ring, out = refs[:-1], refs[-1]
    for head in range(2):

        @pl.when(place[0, 0] == head)
        def _():
            for n in range(len(ring) // 3):
                own, other = ring[3 * n], ring[3 * n + 1 + head]
                out[CHUNK * n : CHUNK * n + OWN] = own[...]
                out[CHUNK * n + OWN : CHUNK * (n + 1)] = other[:OTHER]


def chunks_of(place, ring, chunks):
    parts = [ring[o % 8] for m in chunks for o in (2 * m, 2 * m - 1, 2 * m + 1)]
    return pl.pallas_call(
        chunks_kernel,
        out_shape=heads_of(CHUNK * len(chunks)),
        in_specs=[SMEM] + [VMEM] * len(parts),
        out_specs=VMEM,
        compiler_params=small(4),
        name="chunks_of",
    )(place, *parts)


def scaled(q):
    q = q.astype(jnp.float32) * KAPPA
    high = q.astype(jnp.bfloat16)
    low = (q - high.astype(jnp.float32)).astype(jnp.bfloat16)
    return jnp.concatenate([high, low], axis=1)


def prepare_kernel(place, table, own, student, rows):
    head = place[0, 0]
    for s in range(STUDENTS):
        rows[PAIRS + s] = scaled(student[:, s * DH : (s + 1) * DH])
    for p in range(PAIRS):
        teacher = table[p % 2, head * STUDENTS + p // 2]
        lanes = pl.ds(pl.multiple_of(lax.rem(teacher, PAIRS) * DH, DH), DH)

        @pl.when(lax.div(teacher, PAIRS) == head)
        def _():
            rows[p] = scaled(own[:, lanes])


def prepare(place, table, own, student):
    return pl.pallas_call(
        prepare_kernel,
        out_shape=jax.ShapeDtypeStruct((HEADS, ROWS, 2 * DH), jnp.bfloat16),
        in_specs=[SMEM, SMEM, VMEM, VMEM],
        out_specs=VMEM,
        compiler_params=small(8),
        cost_estimate=pl.CostEstimate(
            flops=HEADS * ROWS * DH * 64, bytes_accessed=HEADS * ROWS * DH * 6, transcendentals=0
        ),
        name="prepare",
    )(place, table, own, student)


def fill_received(place, table, received, rows):
    head = place[0, 0]
    rank = jnp.int32(0)
    for p in range(PAIRS):
        mine = lax.div(table[p % 2, head * STUDENTS + p // 2], PAIRS) == head

        @pl.when(jnp.logical_not(mine))
        def _():
            rows[p] = scaled(received[rank])

        rank = rank + 1 - mine.astype(jnp.int32)


def attend_kernel(first, last, counts, blocks, place, table, plan, *refs):
    refs = list(refs)
    take = lambda n: [refs.pop(0) for _ in range(n)]
    groups = take(len(counts))
    if first:
        pieces = take(len(PIECES) + 1)
        take(1)
        state, rows = take(2)
    else:
        rows, before = take(2)
        if last:
            out, sums = take(2)
        else:
            (state,) = take(1)
    (keys,) = take(1)
    if first:
        received, entry = take(2)
    if last:
        (state,) = take(1)
    offsets = refs[0]
    if first:
        sems = refs[1]
    head, z_hi, x = place[0, 0], place[0, 1], place[0, 2]
    row_block = z_hi * 4 + x

    if first:
        inputs = []
        rank = 0
        for n, piece in enumerate(pieces):
            length = piece.shape[0]
            inputs.append(
                pltpu.make_async_copy(
                    piece, received.at[pl.ds(rank, length)], sems.at[n]
                )
            )
            rank += length
        for c in inputs:
            c.start()
        for c in inputs:
            c.wait()
        fill_received(place, table, received, rows)
    else:
        entry = before
        state[...] = before[...]

    for p in range(PAIRS):
        kv_head = lax.div(table[p % 2, head * STUDENTS + p // 2], GROUP)
        side = jnp.where(lax.div(kv_head, 2) == head, 0, OWN)
        offsets[p] = side + lax.rem(kv_head, 2)

    def place_keys(i):
        at = 0
        for g, n in enumerate(counts):
            if n % CHUNK == 0:
                lo = at // CHUNK

                @pl.when(jnp.logical_and(i >= lo, i < lo + n // CHUNK))
                def _():
                    keys[...] = groups[g][pl.ds((i - lo) * CHUNK, CHUNK)]

            else:
                inside = at % CHUNK

                @pl.when(i == at // CHUNK)
                def _():
                    keys[inside : inside + n] = groups[g][...]

            at += n

    def product(k, p):
        return lax.dot_general(
            jnp.concatenate([k, k], axis=1),
            rows[p],
            (((1,), (1,)), ((), ())),
            preferred_element_type=jnp.float32,
        )

    def folded(a):
        return a.reshape(ROWS // SUB, SUB, ROWS)

    def own_block():
        key_pos = lax.broadcasted_iota(jnp.int32, (ROWS, ROWS), 0)
        row_pos = lax.broadcasted_iota(jnp.int32, (ROWS, ROWS), 1)
        mask = key_pos <= row_pos

        def begin(logits, m_index, l_index):
            logits = jnp.where(mask, logits, MASKED)
            top = jnp.max(logits, axis=0, keepdims=True)
            weights = folded(jnp.exp2(logits - top))
            state[m_index] = jnp.broadcast_to(top, (SUB, ROWS))
            state[l_index] = jnp.sum(weights, axis=0)
            return weights

        for s in range(STUDENTS):
            zs = product(keys[2], PAIRS + s)
            begin(zs, SM + s, SL + s)
            for c in range(2):
                p = 2 * s + c
                zt = product(keys[offsets[p]], p)
                weights = begin(zt, p, TL + p)
                state[TC + p] = jnp.sum(weights * folded(zt - zs), axis=0)

    def block():
        def add(logits, m_index, l_index):
            weights = jnp.exp2(folded(logits) - state[m_index][None])
            state[l_index] = state[l_index] + jnp.sum(weights, axis=0)
            return weights

        student_keys = keys[2]
        for s in range(STUDENTS):
            zs = product(student_keys, PAIRS + s)
            add(zs, SM + s, SL + s)
            for c in range(2):
                p = 2 * s + c
                zt = product(keys[offsets[p]], p)
                weights = add(zt, p, TL + p)
                state[TC + p] = state[TC + p] + jnp.sum(weights * folded(zt - zs), axis=0)

    def exact_block():
        def add(logits, m_index, l_index):
            logits = folded(logits)
            old = state[m_index]
            new = jnp.maximum(old, jnp.max(logits, axis=0))
            weights = jnp.exp2(logits - new[None])
            rescale = jnp.exp2(old - new)
            state[m_index] = new
            state[l_index] = state[l_index] * rescale + jnp.sum(weights, axis=0)
            return weights, rescale

        def student(s, carry):
            zs = product(keys[2], PAIRS + s)
            add(zs, SM + s, SL + s)
            for c in range(2):
                p = 2 * s + c
                zt = product(keys[offsets[p]], p)
                weights, rescale = add(zt, p, TL + p)
                cross = jnp.sum(weights * folded(zt - zs), axis=0)
                state[TC + p] = state[TC + p] * rescale + cross
            return carry

        lax.fori_loop(0, STUDENTS, student, 0)

    def visible(i):
        chunk = lax.bitwise_and(z_hi - plan[0, i], 3)
        return chunk * 4 + lax.bitwise_and(x + plan[1, i], 3) < row_block

    def step(i, carry):
        @pl.when(visible(i))
        def _():
            place_keys(i)
            block()

        return carry

    def exact_step(i, carry):
        @pl.when(visible(i))
        def _():
            place_keys(i)
            exact_block()

        return carry

    if first:
        keys[...] = groups[0][...]
        own_block()
        entry[...] = state[...]
    lax.fori_loop(int(first), blocks, step, 0)

    largest = jnp.maximum(
        jnp.max(state[TL : TL + PAIRS]), jnp.max(state[SL : SL + STUDENTS])
    )

    @pl.when(largest > LARGE)
    def _():
        state[...] = entry[...]
        lax.fori_loop(int(first), blocks, exact_step, 0)

        def settle(m_index, *sums):
            old = state[m_index]
            top = jnp.broadcast_to(jnp.max(old, axis=0, keepdims=True), old.shape)
            for index in sums:
                state[index] = state[index] * jnp.exp2(old - top)
            state[m_index] = top

        for p in range(PAIRS):
            settle(p, TL + p, TC + p)
        for s in range(STUDENTS):
            settle(SM + s, SL + s)

    if not last:
        return

    def merged(m_index, l_index):
        total = jnp.sum(state[l_index], axis=0, keepdims=True)
        return total, LN2 * state[m_index][:1] + jnp.log(total)

    lane = lax.broadcasted_iota(jnp.int32, (1, LANE), 1)
    line = jnp.zeros((1, LANE), jnp.float32)
    for s in range(STUDENTS):
        _, s_lse = merged(SM + s, SL + s)
        value = 2.0 * s_lse
        for c in range(2):
            p = 2 * s + c
            total, t_lse = merged(p, TL + p)
            cross = jnp.sum(state[TC + p], axis=0, keepdims=True)
            value = value + (LN2 * cross / total - t_lse)
        out[s : s + 1, :] = value
        line = jnp.where(lane == s, jnp.sum(value, axis=1, keepdims=True), line)
    sums[...] = jnp.broadcast_to(line, sums.shape)


def attend(place, table, plan, groups, rows, queries=None, state=None, copies_out=0):
    first = queries is not None
    last = copies_out > 0
    counts = tuple(g.shape[0] for g in groups)
    blocks = plan.shape[1]
    state_shape = jax.ShapeDtypeStruct((STATE, SUB, ROWS), jnp.float32)
    rows_shape = jax.ShapeDtypeStruct((HEADS, ROWS, 2 * DH), jnp.bfloat16)
    if first:
        extra, out_shape = [*queries, rows], (state_shape, rows_shape)
    elif last:
        extra = [rows, state]
        out_shape = (
            jax.ShapeDtypeStruct((STUDENTS, ROWS), jnp.float32),
            jax.ShapeDtypeStruct((copies_out, LANE), jnp.float32),
        )
    else:
        extra, out_shape = [rows, state], state_shape
    extra_specs = [ANY] * (len(PIECES) + 1) + [VMEM] if first else [VMEM, VMEM]
    scratch = [pltpu.VMEM((CHUNK, ROWS, DH), jnp.bfloat16)]
    if first:
        scratch.append(pltpu.VMEM((PAIRS, ROWS, DH), jnp.bfloat16))
        scratch.append(pltpu.VMEM(state_shape.shape, jnp.float32))
    if last:
        scratch.append(pltpu.VMEM(state_shape.shape, jnp.float32))
    scratch.append(pltpu.SMEM((PAIRS,), jnp.int32))
    if first:
        scratch.append(pltpu.SemaphoreType.DMA((len(PIECES) + 1,)))
    return pl.pallas_call(
        functools.partial(attend_kernel, first, last, counts, blocks),
        out_shape=out_shape,
        in_specs=[SMEM] * 3 + [VMEM] * len(groups) + extra_specs,
        out_specs=jax.tree.map(lambda _: VMEM, out_shape),
        scratch_shapes=scratch,
        input_output_aliases={3 + len(groups) + len(extra) - 1: 1} if first else {},
        compiler_params=small(24),
        cost_estimate=pl.CostEstimate(
            flops=blocks * HEADS * 2 * ROWS * ROWS * 2 * DH,
            bytes_accessed=blocks * ROWS * CHUNK * DH * 2,
            transcendentals=blocks * HEADS * ROWS * ROWS,
        ),
        name="attend",
    )(place, table, plan, *groups, *extra)


def shift(n, by):
    return [(i, (i + by) % n) for i in range(n)]


def z_place(ring):
    ring %= 8
    return (ring % 2) * 4 + ring // 2


def z_shift(by):
    return [(z_place(i), z_place(i + by)) for i in range(8)]


def plan_of(blocks):
    return jnp.array([list(row) for row in zip(*blocks)], jnp.int32)


def program(teacher_query, teacher_key, student_query, student_key, pair_table):
    head = lax.axis_index("head")
    table = pair_table.T
    place = jnp.stack([head, lax.axis_index("kv_0"), lax.axis_index("kv_1")])[None]

    along_x = lambda a, by: lax.ppermute(a, "kv_1", shift(4, by))
    along_z = lambda a, by: lax.ppermute(a, ("head", "kv_0"), z_shift(by))
    other_side = [(0, 1), (1, 0)]

    ring = {0: split_heads(teacher_key[0], student_key[0])}
    *chosen, count = queries_for_other(place, table, teacher_query[0])
    ring[1] = along_z(ring[0], 1)
    ring[7] = along_z(ring[0], -1)
    pieces = [lax.ppermute(piece, "head", other_side) for piece in chosen[:-1]]
    more = lax.cond(
        count[0, 0] > SENT,
        lambda q: lax.ppermute(q, "head", other_side),
        lambda q: q,
        chosen[-1],
    )
    more, ring[1], ring[7] = lax.optimization_barrier((more, ring[1], ring[7]))
    rows = prepare(place, table, teacher_query[0], student_query[0])
    mine = chunks_of(place, ring, (0,))
    near_a = along_x(mine, 1)
    near_b = along_x(mine, -1)
    near_c = along_x(near_a[:OTHER], 1)
    near_d = along_x(near_b[OTHER:], -1)
    for step in range(2, 5):
        ring[step] = along_z(ring[step - 1], 1)
        if step < 4:
            ring[8 - step] = along_z(ring[9 - step], -1)

    rest_13 = chunks_of(place, ring, (1, 3))
    left_13 = along_x(rest_13, 1)
    right_13 = along_x(rest_13, -1)
    rest_2 = chunks_of(place, ring, (2,))
    left_2 = along_x(rest_2, 1)
    right_2 = along_x(rest_2, -1)
    state, rows = attend(
        place,
        table,
        plan_of([(0, 0), (0, -1), (0, 1), (0, 2), (1, 0), (3, 0), (2, 0)]),
        [mine, near_a, near_b, near_c, near_d, rest_13, rest_2],
        rows,
        queries=(*pieces, more),
    )
    left_13, right_13, state = lax.optimization_barrier((left_13, right_13, state))
    cut_1 = left_13[:CHUNK]
    cut_3 = right_13[CHUNK:]
    far_1 = along_x(cut_1, 1)
    far_3 = along_x(cut_3, -1)
    left_2, right_2, state = lax.optimization_barrier((left_2, right_2, state))
    far_2a = along_x(left_2[:OTHER], 1)
    far_2b = along_x(right_2[OTHER:], -1)
    state = attend(
        place,
        table,
        plan_of([(1, -1), (3, -1), (1, 1), (3, 1), (2, -1), (2, 1)]),
        [left_13, right_13, left_2, right_2],
        rows,
        state=state,
    )
    everyone = ("dp_0", "dp_1", "kv_0", "kv_1")
    devices = lax.axis_size(everyone)
    kl, sums = attend(
        place,
        table,
        plan_of([(1, 2), (3, 2), (2, 2)]),
        [far_1, far_3, far_2a, far_2b],
        rows,
        state=state,
        copies_out=devices,
    )
    terms = lax.all_to_all(sums, everyone, 0, 0, tiled=True)
    head_loss = jnp.sum(terms, axis=0)[:STUDENTS] / (devices * ROWS)
    return (kl[None], head_loss)


def solution(mesh):
    split = Mesh(
        mesh.devices.reshape(4, 2, mesh.shape["head"], 4, 4),
        ("dp_0", "dp_1", "head", "kv_0", "kv_1"),
    )
    in_specs = (P(DP, KV, "head"), P(DP, KV, "head"), P(DP, KV, "head"), P(DP, KV, "head"), P())
    out_specs = (P(DP, "head", KV), P("head"))
    return jax.shard_map(
        program, mesh=split, in_specs=in_specs, out_specs=out_specs, check_vma=False
    )
```
